8 devices in a mesh: data: 1 (over z), col: 2 (over y), row: 4 (over x, core).
Axes of the slice: x: 2, y: 2, z: 1, core: 2. Of those that a mesh axis runs over, the one named last changes fastest.
Arguments:
- tokens: bfloat16 [4096, 2048], P(('data', 'row'), 'col')
- w_qkv: bfloat16 [2048, 2560], P('row', 'col')
- w_out: bfloat16 [2048, 2048], P('row', 'col')
- doc_ids: int32 [4096], P(('data', 'row'))
Outputs:
- output: bfloat16 [4096, 2048], P(('data', 'row'), 'col')
All inputs are finite; a program needn't handle non-finite values.
Results may differ from the reference program's by a relative error of at most 0.00401571.
Values are sent between devices in bfloat16 or wider.
A program may use at most 1 GiB of HBM per device.

```python
import jax
import jax.numpy as jnp
from jax import lax

HIDDEN = 2048
N_HEADS = 16
KV_HEADS = 2
HEAD_DIM = 128
SEQ_LEN = 4096
N_DOCS = 2

GROUP_RATIO = N_HEADS // KV_HEADS
QKV_COLS = HIDDEN + 2 * KV_HEADS * HEAD_DIM


def block_size(row_count, score_width):
    q_blk = row_count
    while q_blk % 16 == 0 and q_blk * score_width > 4194304:
        q_blk = q_blk // 2
    return q_blk


def setup_inputs(seed: int = 0, part: int = 0) -> dict:
    base_key = jax.random.key(seed)
    key_qkv, key_out, key_part = jax.random.split(base_key, 3)
    part_key = jax.random.fold_in(key_part, part)
    key_tok, key_doc = jax.random.split(part_key)
    tokens = jax.random.normal(key_tok, (SEQ_LEN, HIDDEN), jnp.float32).astype(jnp.bfloat16)
    w_qkv = (jax.random.normal(key_qkv, (HIDDEN, QKV_COLS), jnp.float32) * HIDDEN ** -0.5).astype(jnp.bfloat16)
    w_out = (jax.random.normal(key_out, (HIDDEN, HIDDEN), jnp.float32) * HIDDEN ** -0.5).astype(jnp.bfloat16)
    doc_cuts = jax.random.randint(key_doc, (N_DOCS - 1,), 1, SEQ_LEN, dtype=jnp.int32)
    positions = jnp.arange(SEQ_LEN, dtype=jnp.int32)
    doc_ids = jnp.sum((positions[:, None] >= doc_cuts[None, :]).astype(jnp.int32), axis=1)
    return {"tokens": tokens, "w_qkv": w_qkv, "w_out": w_out, "doc_ids": doc_ids}


def reference(tokens, w_qkv, w_out, doc_ids):
    qkv_rows = jnp.dot(tokens, w_qkv, preferred_element_type=jnp.float32).astype(jnp.bfloat16)
    qkv_rows = qkv_rows.reshape(SEQ_LEN, KV_HEADS, GROUP_RATIO + 2, HEAD_DIM)
    key_rows = qkv_rows[:, :, GROUP_RATIO, :].astype(jnp.float32)
    value_rows = qkv_rows[:, :, GROUP_RATIO + 1, :].astype(jnp.float32)
    q_blk = block_size(SEQ_LEN, N_HEADS * SEQ_LEN)
    n_steps = SEQ_LEN // q_blk
    q_steps = qkv_rows[:, :, :GROUP_RATIO, :].reshape(n_steps, q_blk, KV_HEADS, GROUP_RATIO, HEAD_DIM)
    score_scale = HEAD_DIM ** -0.5

    def attend(block_in):
        q_part, seg_part = block_in
        scores = jnp.einsum("qgrd,kgd->qgrk", q_part.astype(jnp.float32), key_rows) * score_scale
        same_doc = seg_part[:, None, None, None] == doc_ids[None, None, None, :]
        scores = jnp.where(same_doc, scores, -jnp.inf)
        weights = jax.nn.softmax(scores, axis=-1).astype(jnp.bfloat16)
        context = jnp.einsum("qgrk,kgd->qgrd", weights.astype(jnp.float32), value_rows)
        return context.astype(jnp.bfloat16)

    context = lax.map(attend, (q_steps, doc_ids.reshape(n_steps, q_blk)))
    context = context.reshape(SEQ_LEN, HIDDEN)
    return jnp.dot(context, w_out, preferred_element_type=jnp.float32).astype(jnp.bfloat16)
```

```python
import functools
import math

import jax
import jax.numpy as jnp
from jax import lax
from jax.experimental import pallas as pl
from jax.experimental.pallas import tpu as pltpu
from jax.sharding import PartitionSpec as P

HEAD_DIM = 128
MESH = pl.DeviceIdType.MESH

ROWS = 1024
HID = 1024
SEQ = 4096
HEADS = 8
QKV = 1280
SHARD = 512
QB = 256
KC = 512
CHUNK = 256
N_CHUNK = ROWS // CHUNK
W_PIECES = 4
W_ROWS = SHARD // W_PIECES
TILES = HEADS * (ROWS // QB)
CORE, XP, DIAG = 0, 1, 2
EXP_SCALE = math.log2(math.e) / math.sqrt(HEAD_DIM)
NT = (((1,), (1,)), ((), ()))


def kernel(
    tok_hbm, w_hbm, wo_hbm, doc_hbm, out_hbm,
    tok_own, tok_peer, w_buf, wo_buf, doc_buf, kcol, bias, q_buf, k_buf, vt_buf, s0, s1, ctx_own, ctx_peer, out_buf,
    loc_sem, tok_send, tok_recv, wx_send, wx_recv, wc_send, wc_recv, wf_send, wf_recv,
    ox_send, ox_recv, oc_send, oc_recv, of_send, of_recv, doc_send, doc_recv, kv_send, kv_recv, ctx_send, ctx_recv, out_sem,
):
    d, y, r = lax.axis_index("data"), lax.axis_index("col"), lax.axis_index("row")
    x, core = r // 2, r % 2
    row_of = {CORE: x * 2 + (1 - core), XP: (1 - x) * 2 + core, DIAG: (1 - x) * 2 + (1 - core)}
    y_peer = (d, 1 - y, r)
    peer = {k: (d, y, v) for k, v in row_of.items()}

    barrier = pltpu.get_barrier_semaphore()
    for p in (y_peer, peer[CORE], peer[XP], peer[DIAG]):
        pl.semaphore_signal(barrier, inc=1, device_id=p, device_id_type=MESH)
    pl.semaphore_wait(barrier, 4)

    def rcopy(src, dst, ssem, rsem, dev):
        return pltpu.make_async_remote_copy(
            src_ref=src, dst_ref=dst, send_sem=ssem, recv_sem=rsem, device_id=dev, device_id_type=MESH
        )

    def shard_rows(row, piece=0, size=SHARD):
        return pl.ds(pl.multiple_of(row * SHARD + piece * size, size), size)

    tok_copies = []
    for c in range(N_CHUNK):
        rows = pl.ds(c * CHUNK, CHUNK)
        cp = rcopy(tok_hbm.at[rows], tok_peer.at[rows], tok_send.at[c], tok_recv.at[c], y_peer)
        cp.start()
        tok_copies.append(cp)
    doc_copies = []
    for k in (CORE, XP, DIAG):
        cp = rcopy(doc_hbm, doc_buf.at[r], doc_send.at[k], doc_recv.at[k], peer[k])
        cp.start()
        doc_copies.append(cp)
    wx_copies = []
    for p in range(W_PIECES):
        cp = rcopy(
            w_hbm.at[pl.ds(p * W_ROWS, W_ROWS)], w_buf.at[shard_rows(r, p, W_ROWS)], wx_send.at[p], wx_recv.at[p], peer[XP]
        )
        cp.start()
        wx_copies.append(cp)
    wc_copy = rcopy(w_hbm, w_buf.at[shard_rows(r)], wc_send, wc_recv, peer[CORE])
    wc_copy.start()
    oc_copy = rcopy(wo_hbm, wo_buf.at[shard_rows(r)], oc_send, oc_recv, peer[CORE])
    oc_copy.start()
    doc_local = pltpu.make_async_copy(doc_hbm, doc_buf.at[r], loc_sem.at[0])
    doc_local.start()
    w_local = pltpu.make_async_copy(w_hbm, w_buf.at[shard_rows(r)], loc_sem.at[1])
    w_local.start()
    tok_local = pltpu.make_async_copy(tok_hbm, tok_own, loc_sem.at[2])
    tok_local.start()
    wo_local = pltpu.make_async_copy(wo_hbm, wo_buf.at[shard_rows(r)], loc_sem.at[3])
    wo_local.start()

    doc_local.wait()
    for cp in doc_copies:
        cp.wait_recv()

    def spread(i, carry):
        line = doc_buf[i // 8, pl.ds(i % 8, 1), :]
        kcol[pl.ds(pl.multiple_of(i * 128, 128), 128), :] = jnp.transpose(jnp.broadcast_to(line, (128, 128)))
        return carry

    lax.fori_loop(0, SEQ // 128, spread, 0)

    def mask_tile(i, carry):
        lanes = pl.ds(pl.multiple_of((i // 16) * 128, 128), 128)
        keys = pl.ds(pl.multiple_of((i % 16) * 256, 256), 256)
        line = doc_buf[r, pl.ds(i // 16, 1), :]
        bias[keys, lanes] = jnp.where(kcol[keys, :] == line, 0.0, -jnp.inf)
        return carry

    lax.fori_loop(0, 8 * 16, mask_tile, 0)

    wf_copies = []
    for p in range(W_PIECES):
        wx_copies[p].wait_recv()
        rows = shard_rows(row_of[XP], p, W_ROWS)
        cp = rcopy(w_buf.at[rows], w_buf.at[rows], wf_send.at[p], wf_recv.at[p], peer[CORE])
        cp.start()
        wf_copies.append(cp)
    w_local.wait()
    tok_local.wait()
    wc_copy.wait_recv()
    for cp in wf_copies:
        cp.wait_recv()

    own_half = pl.ds(pl.multiple_of(y * HID, HID), HID)
    peer_half = pl.ds(pl.multiple_of((1 - y) * HID, HID), HID)

    def project(rows, cols):
        return jnp.dot(tok_own[rows, :], w_buf[own_half, cols], preferred_element_type=jnp.float32) + jnp.dot(
            tok_peer[rows, :], w_buf[peer_half, cols], preferred_element_type=jnp.float32
        )

    kv_copies = []
    for c in range(N_CHUNK):
        rows = pl.ds(c * CHUNK, CHUNK)
        tok_copies[c].wait_recv()
        kv = project(rows, pl.ds(HID, 2 * HEAD_DIM)).astype(jnp.bfloat16)
        krows = pl.ds(pl.multiple_of(r * ROWS + c * CHUNK, CHUNK), CHUNK)
        k_buf[krows, :] = kv[:, :HEAD_DIM]
        vt_buf[:, krows] = jnp.transpose(kv[:, HEAD_DIM:])
        for k in (DIAG, XP, CORE):
            cp = rcopy(k_buf.at[krows], k_buf.at[krows], kv_send.at[c, k, 0], kv_recv.at[c, k, 0], peer[k])
            cp.start()
            kv_copies.append(cp)
            cp = rcopy(vt_buf.at[:, krows], vt_buf.at[:, krows], kv_send.at[c, k, 1], kv_recv.at[c, k, 1], peer[k])
            cp.start()
            kv_copies.append(cp)

        def q_tile(n, carry):
            cols = pl.ds(pl.multiple_of(n * 256, 256), 256)
            q_buf[rows, cols] = project(rows, cols).astype(jnp.bfloat16)
            return carry

        lax.fori_loop(0, HID // 256, q_tile, 0)

    for cp in kv_copies:
        cp.wait_recv()

    ox_copy = rcopy(wo_hbm, wo_buf.at[shard_rows(r)], ox_send, ox_recv, peer[XP])
    ox_copy.start()

    def tile_of(i):
        return (
            pl.ds(pl.multiple_of((i // HEADS) * QB, QB), QB),
            pl.ds(pl.multiple_of((i % HEADS) * HEAD_DIM, HEAD_DIM), HEAD_DIM),
        )

    def score_step(i, s_ref, j, mx):
        rows, cols = tile_of(i)
        keys = pl.ds(j * KC, KC)
        s = lax.dot_general(k_buf[keys, :], q_buf[rows, cols], NT, preferred_element_type=jnp.float32)
        s = s + bias[keys, rows]
        s_ref[keys, :] = s
        top = jnp.max(s.reshape(KC // 8, 8, QB), axis=0)
        return top if mx is None else jnp.maximum(mx, top)

    def value_step(s_ref, j, m_scaled, total, acc):
        keys = pl.ds(j * KC, KC)
        p = jnp.exp2(s_ref[keys, :] * EXP_SCALE - m_scaled)
        part = jnp.sum(p.reshape(KC // 8, 8, QB), axis=0)
        o = jnp.dot(vt_buf[:, keys], p.astype(jnp.bfloat16), preferred_element_type=jnp.float32)
        return (part, o) if total is None else (total + part, acc + o)

    def ctx_copy(i):
        rows, cols = tile_of(i)
        return rcopy(ctx_own.at[rows, cols], ctx_peer.at[rows, cols], ctx_send.at[i], ctx_recv.at[i], y_peer)

    def tile(i, s_ref, mx, nxt, s_next):
        m_scaled = jnp.max(mx, axis=0, keepdims=True) * EXP_SCALE
        total, acc, mx_next = None, None, None
        for j in range(SEQ // KC):
            mx_next = score_step(nxt, s_next, j, mx_next)
            total, acc = value_step(s_ref, j, m_scaled, total, acc)
        o = acc * (1.0 / jnp.sum(total, axis=0, keepdims=True))
        rows, cols = tile_of(i)
        ctx_own[rows, cols] = jnp.transpose(o).astype(jnp.bfloat16)
        ctx_copy(i).start()
        return mx_next

    def two_tiles(t, mx):
        i = t * 2
        mx = tile(i, s0, mx, i + 1, s1)
        return tile(i + 1, s1, mx, jnp.minimum(i + 2, TILES - 1), s0)

    mx = None
    for j in range(SEQ // KC):
        mx = score_step(0, s0, j, mx)

    def project_out(b):
        rows = pl.ds(pl.multiple_of(b * QB, QB), QB)

        def wait_piece(h, carry):
            ctx_copy(b * HEADS + h).wait_recv()
            return carry

        lax.fori_loop(0, HEADS, wait_piece, 0)

        def out_tile(n, carry):
            cols = pl.ds(pl.multiple_of(n * 256, 256), 256)
            o = jnp.dot(ctx_own[rows, :], wo_buf[own_half, cols], preferred_element_type=jnp.float32) + jnp.dot(
                ctx_peer[rows, :], wo_buf[peer_half, cols], preferred_element_type=jnp.float32
            )
            out_buf[rows, cols] = o.astype(jnp.bfloat16)
            return carry

        lax.fori_loop(0, HID // 256, out_tile, 0)
        pltpu.make_async_copy(out_buf.at[rows], out_hbm.at[rows], out_sem.at[b]).start()

    n_blocks = ROWS // QB
    per_block = HEADS // 2
    mx = lax.fori_loop(0, 3 * per_block, two_tiles, mx)
    ox_copy.wait_recv()
    rows = shard_rows(row_of[XP])
    of_copy = rcopy(wo_buf.at[rows], wo_buf.at[rows], of_send, of_recv, peer[CORE])
    of_copy.start()
    mx = lax.fori_loop(3 * per_block, 4 * per_block, two_tiles, mx)
    wo_local.wait()
    oc_copy.wait_recv()
    of_copy.wait_recv()
    for b in range(n_blocks):
        project_out(b)

    for b in range(n_blocks):
        rows = pl.ds(b * QB, QB)
        pltpu.make_async_copy(out_buf.at[rows], out_hbm.at[rows], out_sem.at[b]).wait()
    for cp in (*tok_copies, *doc_copies, *wx_copies, wc_copy, oc_copy, *wf_copies, *kv_copies, ox_copy, of_copy):
        cp.wait_send()

    def wait_sent(i, carry):
        ctx_copy(i).wait_send()
        return carry

    lax.fori_loop(0, TILES, wait_sent, 0)


def solution(mesh):
    def local_block(tokens, w_qkv, w_out, doc_ids):
        bf16, f32 = jnp.bfloat16, jnp.float32
        dma = pltpu.SemaphoreType.DMA
        any_spec = pl.BlockSpec(memory_space=pl.ANY)
        return pl.pallas_call(
            kernel,
            out_shape=jax.ShapeDtypeStruct(tokens.shape, bf16),
            in_specs=[any_spec] * 4,
            out_specs=any_spec,
            scratch_shapes=[
                pltpu.VMEM((ROWS, HID), bf16),
                pltpu.VMEM((ROWS, HID), bf16),
                pltpu.VMEM((2 * HID, QKV), bf16),
                pltpu.VMEM((2 * HID, HID), bf16),
                pltpu.VMEM((4, 8, 128), jnp.int32),
                pltpu.VMEM((SEQ, 128), jnp.int32),
                pltpu.VMEM((SEQ, ROWS), f32),
                pltpu.VMEM((ROWS, HID), bf16),
                pltpu.VMEM((SEQ, HEAD_DIM), bf16),
                pltpu.VMEM((HEAD_DIM, SEQ), bf16),
                pltpu.VMEM((SEQ, QB), f32),
                pltpu.VMEM((SEQ, QB), f32),
                pltpu.VMEM((ROWS, HID), bf16),
                pltpu.VMEM((ROWS, HID), bf16),
                pltpu.VMEM((ROWS, HID), bf16),
                dma((4,)),
                dma((N_CHUNK,)),
                dma((N_CHUNK,)),
                dma((W_PIECES,)),
                dma((W_PIECES,)),
                dma,
                dma,
                dma((W_PIECES,)),
                dma((W_PIECES,)),
                dma,
                dma,
                dma,
                dma,
                dma,
                dma,
                dma((3,)),
                dma((3,)),
                dma((N_CHUNK, 3, 2)),
                dma((N_CHUNK, 3, 2)),
                dma((TILES,)),
                dma((TILES,)),
                dma((ROWS // QB,)),
            ],
            compiler_params=pltpu.CompilerParams(
                collective_id=0, has_side_effects=True, vmem_limit_bytes=67043328
            ),
        )(tokens, w_qkv, w_out, doc_ids.reshape(8, 128))

    row_spec = P(("data", "row"), "col")
    weight_spec = P("row", "col")
    return jax.shard_map(
        local_block,
        mesh=mesh,
        in_specs=(row_spec, weight_spec, weight_spec, P(("data", "row"))),
        out_specs=row_spec,
        check_vma=False,
    )
```

```python
import itertools
import math

import jax
import jax.numpy as jnp
from jax import lax
from jax.experimental import pallas as pl
from jax.experimental.pallas import tpu as pltpu
from jax.sharding import PartitionSpec as P

HEAD_DIM = 128
MESH = pl.DeviceIdType.MESH

ROWS = 1024
HID = 1024
SEQ = 4096
HEADS = 8
QKV = 1280
SHARD = 512
QB = 256
KC = 512
N_STEP = SEQ // KC
CHUNK = 256
N_CHUNK = ROWS // CHUNK
W_PIECES = 4
W_ROWS = SHARD // W_PIECES
N_BLOCK = ROWS // QB
TILES = HEADS * N_BLOCK
N_SEM = 64
CORE, XP, DIAG = 0, 1, 2
EXP_SCALE = math.log2(math.e) / math.sqrt(HEAD_DIM)
NT = (((1,), (1,)), ((), ()))
BF16_MAX = float(jnp.finfo(jnp.bfloat16).max)
F32_MIN = float(jnp.finfo(jnp.float32).min)


def kernel(
    tok_hbm, w_hbm, wo_hbm, doc_hbm, out_hbm,
    tok_own, tok_peer, w_buf, wo_buf, doc_buf, q_buf, qx_buf, k_buf, vt_buf, p0, p1, top_buf,
    ctx_own, ctx_peer, out_buf, loc_sem, send_sem, recv_sem, ctx_send, ctx_recv, out_sem,
):
    d, y, r = lax.axis_index("data"), lax.axis_index("col"), lax.axis_index("row")
    x, core = r // 2, r % 2
    row_of = {CORE: x * 2 + (1 - core), XP: (1 - x) * 2 + core, DIAG: (1 - x) * 2 + (1 - core)}
    y_peer = (d, 1 - y, r)
    peer = {k: (d, y, v) for k, v in row_of.items()}

    barrier = pltpu.get_barrier_semaphore()
    for p in (y_peer, peer[CORE], peer[XP], peer[DIAG]):
        pl.semaphore_signal(barrier, inc=1, device_id=p, device_id_type=MESH)
    pl.semaphore_wait(barrier, 4)

    number = itertools.count()
    sent = []

    def send(src, dst, device):
        i = next(number)
        cp = pltpu.make_async_remote_copy(
            src_ref=src, dst_ref=dst, send_sem=send_sem.at[i], recv_sem=recv_sem.at[i], device_id=device, device_id_type=MESH
        )
        cp.start()
        sent.append(cp)
        return cp

    def local(src, dst, i):
        cp = pltpu.make_async_copy(src, dst, loc_sem.at[i])
        cp.start()
        return cp

    def shard(row, piece=0, size=SHARD):
        return pl.ds(pl.multiple_of(row * SHARD + piece * size, size), size)

    kv_cols, q_cols, k_cols = pl.ds(HID, 2 * HEAD_DIM), pl.ds(0, HID), pl.ds(0, HEAD_DIM)

    tok_in = []
    for c in range(N_CHUNK):
        rows = pl.ds(c * CHUNK, CHUNK)
        tok_in.append(send(tok_hbm.at[rows], tok_peer.at[rows], y_peer))
    wkv_x = send(w_hbm.at[:, kv_cols], w_buf.at[shard(r), kv_cols], peer[XP])
    doc_in = [send(doc_hbm, doc_buf.at[r], peer[k]) for k in (CORE, XP, DIAG)]
    wq_x = [
        send(w_hbm.at[pl.ds(p * W_ROWS, W_ROWS), q_cols], w_buf.at[shard(r, p, W_ROWS), q_cols], peer[XP])
        for p in range(W_PIECES)
    ]
    w_core = send(w_hbm, w_buf.at[shard(r)], peer[CORE])
    wo_core = send(wo_hbm, wo_buf.at[shard(r)], peer[CORE])
    doc_local = local(doc_hbm, doc_buf.at[r], 0)
    w_local = local(w_hbm, w_buf.at[shard(r)], 1)
    tok_local = local(tok_hbm, tok_own, 2)
    wo_local = local(wo_hbm, wo_buf.at[shard(r)], 3)

    doc_local.wait()
    for cp in doc_in:
        cp.wait_recv()
    lane = lax.broadcasted_iota(jnp.int32, (128, 128), 1)

    def as_column(line):
        return jnp.transpose(jnp.broadcast_to(line, (128, 128)))

    def key_mask(i, carry):
        ids = as_column(doc_buf[i // 8, pl.ds(i % 8, 1), :])
        hit = jnp.where(lane < 3, 1 - ids, jnp.where(lane < 6, ids, 0))
        k_buf[pl.ds(pl.multiple_of(i * 128, 128), 128), HEAD_DIM:] = hit.astype(jnp.float32).astype(jnp.bfloat16)
        return carry

    def query_mask(i, carry):
        ids = as_column(doc_buf[r, pl.ds(i, 1), :])
        hit = jnp.where(lane < 3, ids, jnp.where(lane < 6, 1 - ids, 0))
        qx_buf[pl.ds(pl.multiple_of(i * 128, 128), 128), :] = jnp.where(hit == 1, -BF16_MAX, 0.0).astype(jnp.bfloat16)
        return carry

    lax.fori_loop(0, SEQ // 128, key_mask, 0)
    lax.fori_loop(0, ROWS // 128, query_mask, 0)

    own_half = pl.ds(pl.multiple_of(y * HID, HID), HID)
    peer_half = pl.ds(pl.multiple_of((1 - y) * HID, HID), HID)

    def project(rows, cols):
        return jnp.dot(tok_own[rows, :], w_buf[own_half, cols], preferred_element_type=jnp.float32) + jnp.dot(
            tok_peer[rows, :], w_buf[peer_half, cols], preferred_element_type=jnp.float32
        )

    def forward(ref, *index):
        return send(ref.at[index], ref.at[index], peer[CORE])

    k_in, kv_core = [], []

    def keys_of(row, c):
        return pl.ds(pl.multiple_of(row * ROWS + c * CHUNK, CHUNK), CHUNK)

    def project_kv(c):
        tok_in[c].wait_recv()
        kv = project(pl.ds(c * CHUNK, CHUNK), kv_cols).astype(jnp.bfloat16)
        keys = keys_of(r, c)
        k_buf[keys, k_cols] = kv[:, :HEAD_DIM]
        k_in.append([send(k_buf.at[keys, k_cols], k_buf.at[keys, k_cols], peer[XP])])
        vt_buf[:, keys] = jnp.transpose(kv[:, HEAD_DIM:])
        k_in[c].append(send(vt_buf.at[:, keys], vt_buf.at[:, keys], peer[XP]))
        kv_core.append(send(k_buf.at[keys, k_cols], k_buf.at[keys, k_cols], peer[CORE]))
        kv_core.append(send(vt_buf.at[:, keys], vt_buf.at[:, keys], peer[CORE]))

    def forward_kv(c):
        keys = keys_of(row_of[XP], c)
        k_in[c][0].wait_recv()
        kv_core.append(forward(k_buf, keys, k_cols))
        k_in[c][1].wait_recv()
        kv_core.append(forward(vt_buf, slice(None), keys))

    def project_q(c):
        rows = pl.ds(c * CHUNK, CHUNK)

        def q_tile(n, carry):
            cols = pl.ds(pl.multiple_of(n * 256, 256), 256)
            q_buf[rows, cols] = project(rows, cols).astype(jnp.bfloat16)
            return carry

        lax.fori_loop(0, HID // 256, q_tile, 0)

    wkv_x.wait_recv()
    wkv_f = forward(w_buf, shard(row_of[XP]), kv_cols)
    w_local.wait()
    tok_local.wait()
    w_core.wait_recv()
    wkv_f.wait_recv()
    wq_f = []

    def forward_wq(p):
        wq_x[p].wait_recv()
        wq_f.append(forward(w_buf, shard(row_of[XP], p, W_ROWS), q_cols))

    half = SHARD // 2

    def send_wo(p):
        return send(wo_hbm.at[pl.ds(p * half, half)], wo_buf.at[shard(r, p, half)], peer[XP])

    project_kv(0)
    forward_wq(0)
    forward_wq(1)
    project_kv(1)
    forward_wq(2)
    forward_wq(3)
    wo_x = [send_wo(0)]
    for cp in wq_f:
        cp.wait_recv()
    project_q(0)
    project_q(1)
    forward_kv(0)
    forward_kv(1)
    project_kv(2)
    project_q(2)
    forward_kv(2)
    project_kv(3)
    wo_x.append(send_wo(1))
    project_q(3)
    forward_kv(3)
    wo_x[0].wait_recv()
    wo_f = [forward(wo_buf, shard(row_of[XP], 0, half))]
    for cp in kv_core:
        cp.wait_recv()

    def tile_of(i):
        return (
            pl.ds(pl.multiple_of((i // HEADS) * QB, QB), QB),
            pl.ds(pl.multiple_of((i % HEADS) * HEAD_DIM, HEAD_DIM), HEAD_DIM),
        )

    def over_keys(f, a):
        return f(a.reshape(a.shape[0] // 8, 8, QB), axis=0)

    def to_keys(a):
        return jnp.concatenate([a] * (KC // 8), axis=0)

    def score_step(i, slot, p_ref, j, state):
        top, total = state
        rows, cols = tile_of(i)
        keys = pl.ds(j * KC, KC)
        k = k_buf[keys, :]
        q = jnp.concatenate([q_buf[rows, cols], qx_buf[rows, :]], axis=1)
        s = lax.dot_general(k, q, NT, preferred_element_type=jnp.float32)
        new_top = jnp.maximum(top, over_keys(jnp.max, s))
        scaled = new_top * EXP_SCALE
        top_buf[slot, j] = scaled
        p = jnp.exp2(s * EXP_SCALE - to_keys(scaled))
        p_ref[keys, :] = p
        return new_top, total * jnp.exp2(top * EXP_SCALE - scaled) + over_keys(jnp.sum, p)

    def value_step(slot, p_ref, j, lse, acc):
        keys = pl.ds(j * KC, KC)
        weights = p_ref[keys, :] * to_keys(jnp.exp2(top_buf[slot, j] - lse))
        o = jnp.dot(vt_buf[:, keys], weights.astype(jnp.bfloat16), preferred_element_type=jnp.float32)
        return o if acc is None else acc + o

    def ctx_copy(i):
        rows, cols = tile_of(i)
        return pltpu.make_async_remote_copy(
            src_ref=ctx_own.at[rows, cols], dst_ref=ctx_peer.at[rows, cols], send_sem=ctx_send.at[i], recv_sem=ctx_recv.at[i],
            device_id=y_peer, device_id_type=MESH,
        )

    empty = (jnp.full((8, QB), F32_MIN, jnp.float32), jnp.zeros((8, QB), jnp.float32))
    bufs = (p0, p1)

    def tile(i, slot, state, nxt):
        top, total = state
        best = jnp.max(top, axis=0, keepdims=True)
        whole = jnp.sum(total * jnp.exp2((top - best) * EXP_SCALE), axis=0, keepdims=True)
        lse = best * EXP_SCALE + jnp.log2(whole)
        acc, state = None, empty
        for j in range(N_STEP):
            state = score_step(nxt, 1 - slot, bufs[1 - slot], j, state)
            acc = value_step(slot, bufs[slot], j, lse, acc)
        rows, cols = tile_of(i)
        ctx_own[rows, cols] = jnp.transpose(acc).astype(jnp.bfloat16)
        return state

    def two_tiles(t, state):
        i = t * 2
        state = tile(i, 0, state, i + 1)
        state = tile(i + 1, 1, state, jnp.minimum(i + 2, TILES - 1))
        ctx_copy(i).start()
        ctx_copy(i + 1).start()
        return state

    def out_copy(b, n):
        at = (pl.ds(pl.multiple_of(b * QB, QB), QB), pl.ds(pl.multiple_of(n * 256, 256), 256))
        return pltpu.make_async_copy(out_buf.at[at], out_hbm.at[at], out_sem.at[b])

    def project_out(b):
        rows = pl.ds(pl.multiple_of(b * QB, QB), QB)

        def wait_piece(h, carry):
            ctx_copy(b * HEADS + h).wait_recv()
            return carry

        lax.fori_loop(0, HEADS, wait_piece, 0)

        def out_tile(n, carry):
            cols = pl.ds(pl.multiple_of(n * 256, 256), 256)
            o = jnp.dot(ctx_own[rows, :], wo_buf[own_half, cols], preferred_element_type=jnp.float32) + jnp.dot(
                ctx_peer[rows, :], wo_buf[peer_half, cols], preferred_element_type=jnp.float32
            )
            out_buf[rows, cols] = o.astype(jnp.bfloat16)
            return carry

        lax.fori_loop(0, HID // 256, out_tile, 0)
        out = pltpu.make_async_copy(out_buf.at[rows], out_hbm.at[rows], out_sem.at[b])
        out.start()

    state = empty
    for j in range(N_STEP):
        state = score_step(0, 0, p0, j, state)

    pairs = HEADS // 2
    state = lax.fori_loop(0, 2 * pairs, two_tiles, state)
    wo_x[1].wait_recv()
    wo_f.append(forward(wo_buf, shard(row_of[XP], 1, half)))
    wo_local.wait()
    wo_core.wait_recv()
    for cp in wo_f:
        cp.wait_recv()

    def later_block(b, state):
        project_out(b - 2)
        return lax.fori_loop(b * pairs, (b + 1) * pairs, two_tiles, state)

    lax.fori_loop(2, N_BLOCK, later_block, state)

    def last_block(b, carry):
        project_out(b)
        return carry

    lax.fori_loop(N_BLOCK - 2, N_BLOCK, last_block, 0)

    def wait_out(b, carry):
        rows = pl.ds(pl.multiple_of(b * QB, QB), QB)
        pltpu.make_async_copy(out_buf.at[rows], out_hbm.at[rows], out_sem.at[b]).wait()
        return carry

    lax.fori_loop(0, N_BLOCK, wait_out, 0)
    for cp in sent:
        cp.wait_send()

    def wait_sent(i, carry):
        ctx_copy(i).wait_send()
        return carry

    lax.fori_loop(0, TILES, wait_sent, 0)
    assert next(number) <= N_SEM


def solution(mesh):
    def local_block(tokens, w_qkv, w_out, doc_ids):
        bf16, f32 = jnp.bfloat16, jnp.float32
        dma = pltpu.SemaphoreType.DMA
        any_spec = pl.BlockSpec(memory_space=pl.ANY)
        return pl.pallas_call(
            kernel,
            out_shape=jax.ShapeDtypeStruct(tokens.shape, bf16),
            in_specs=[any_spec] * 4,
            out_specs=any_spec,
            scratch_shapes=[
                pltpu.VMEM((ROWS, HID), bf16),
                pltpu.VMEM((ROWS, HID), bf16),
                pltpu.VMEM((2 * HID, QKV), bf16),
                pltpu.VMEM((2 * HID, HID), bf16),
                pltpu.VMEM((4, 8, 128), jnp.int32),
                pltpu.VMEM((ROWS, HID), bf16),
                pltpu.VMEM((ROWS, 128), bf16),
                pltpu.VMEM((SEQ, 2 * HEAD_DIM), bf16),
                pltpu.VMEM((HEAD_DIM, SEQ), bf16),
                pltpu.VMEM((SEQ, QB), f32),
                pltpu.VMEM((SEQ, QB), f32),
                pltpu.VMEM((2, N_STEP, 8, QB), f32),
                pltpu.VMEM((ROWS, HID), bf16),
                pltpu.VMEM((ROWS, HID), bf16),
                pltpu.VMEM((ROWS, HID), bf16),
                dma((4,)),
                dma((N_SEM,)),
                dma((N_SEM,)),
                dma((TILES,)),
                dma((TILES,)),
                dma((N_BLOCK,)),
            ],
            compiler_params=pltpu.CompilerParams(
                collective_id=0, has_side_effects=True, vmem_limit_bytes=67043328
            ),
        )(tokens, w_qkv, w_out, doc_ids.reshape(8, 128))

    row_spec = P(("data", "row"), "col")
    weight_spec = P("row", "col")
    return jax.shard_map(
        local_block,
        mesh=mesh,
        in_specs=(row_spec, weight_spec, weight_spec, P(("data", "row"))),
        out_specs=row_spec,
        check_vma=False,
    )
```

```python
import itertools
import math

import jax
import jax.numpy as jnp
from jax import lax
from jax.experimental import pallas as pl
from jax.experimental.pallas import tpu as pltpu
from jax.sharding import PartitionSpec as P

HEAD_DIM = 128
MESH = pl.DeviceIdType.MESH

ROWS = 1024
HID = 1024
SEQ = 4096
HEADS = 8
QKV = 1280
SHARD = 512
QB = 256
KC = 1024
GROUP = 128
N_GROUP = KC // GROUP
N_STEP = SEQ // KC
CHUNKS = ((0, 256), (256, 256), (512, 256), (768, 128), (896, 128))
W_PIECES = 4
W_ROWS = SHARD // W_PIECES
N_BLOCK = ROWS // QB
TILES = HEADS * N_BLOCK
SLOTS = 8
N_SEM = 64
CORE, XP, DIAG = 0, 1, 2
EXP_SCALE = math.log2(math.e) / math.sqrt(HEAD_DIM)
NT = (((1,), (1,)), ((), ()))
BF16_MAX = float(jnp.finfo(jnp.bfloat16).max)
F32_MIN = float(jnp.finfo(jnp.float32).min)


def kernel(
    tok_hbm, w_hbm, wo_hbm, doc_hbm, out_hbm,
    tok_own, tok_peer, w_buf, wo_buf, doc_buf, q_buf, qx_buf, k_buf, vt_buf, p_buf, top_buf, state_buf,
    ctx_own, ctx_peer, loc_sem, send_sem, recv_sem, ctx_send, ctx_recv, out_sem,
):
    d, y, r = lax.axis_index("data"), lax.axis_index("col"), lax.axis_index("row")
    x, core = r // 2, r % 2
    row_of = {CORE: x * 2 + (1 - core), XP: (1 - x) * 2 + core, DIAG: (1 - x) * 2 + (1 - core)}
    y_peer = (d, 1 - y, r)
    peer = {k: (d, y, v) for k, v in row_of.items()}
    out_buf = tok_own

    barrier = pltpu.get_barrier_semaphore()
    for p in (y_peer, peer[CORE], peer[XP], peer[DIAG]):
        pl.semaphore_signal(barrier, inc=1, device_id=p, device_id_type=MESH)
    pl.semaphore_wait(barrier, 4)

    number = itertools.count()
    sent = []

    def send(src, dst, device):
        i = next(number)
        cp = pltpu.make_async_remote_copy(
            src_ref=src, dst_ref=dst, send_sem=send_sem.at[i], recv_sem=recv_sem.at[i], device_id=device, device_id_type=MESH
        )
        cp.start()
        sent.append(cp)
        return cp

    def local(src, dst, i):
        cp = pltpu.make_async_copy(src, dst, loc_sem.at[i])
        cp.start()
        return cp

    def shard(row, piece=0, size=SHARD):
        return pl.ds(pl.multiple_of(row * SHARD + piece * size, size), size)

    kv_cols, q_cols, k_cols = pl.ds(HID, 2 * HEAD_DIM), pl.ds(0, HID), pl.ds(0, HEAD_DIM)

    tok_in = []
    for first, size in CHUNKS:
        rows = pl.ds(first, size)
        tok_in.append(send(tok_hbm.at[rows], tok_peer.at[rows], y_peer))
    wkv_x = send(w_hbm.at[:, kv_cols], w_buf.at[shard(r), kv_cols], peer[XP])
    doc_in = [send(doc_hbm, doc_buf.at[r], peer[k]) for k in (CORE, XP, DIAG)]
    wq_x = [
        send(w_hbm.at[pl.ds(p * W_ROWS, W_ROWS), q_cols], w_buf.at[shard(r, p, W_ROWS), q_cols], peer[XP])
        for p in range(W_PIECES)
    ]
    w_core = send(w_hbm, w_buf.at[shard(r)], peer[CORE])
    wo_core = send(wo_hbm, wo_buf.at[shard(r)], peer[CORE])
    doc_local = local(doc_hbm, doc_buf.at[r], 0)
    w_local = local(w_hbm, w_buf.at[shard(r)], 1)
    tok_local = local(tok_hbm, tok_own, 2)
    wo_local = local(wo_hbm, wo_buf.at[shard(r)], 3)

    doc_local.wait()
    for cp in doc_in:
        cp.wait_recv()
    lane = lax.broadcasted_iota(jnp.int32, (128, 128), 1)

    def as_column(line):
        return jnp.transpose(jnp.broadcast_to(line, (128, 128)))

    def key_mask(place):
        def line_mask(i, carry):
            part, line, first = place(i)
            ids = as_column(doc_buf[part, pl.ds(line, 1), :])
            hit = jnp.where(lane < 3, 1 - ids, jnp.where(lane < 6, ids, 0))
            k_buf[pl.ds(pl.multiple_of(first, 128), 128), HEAD_DIM:] = hit.astype(jnp.float32).astype(jnp.bfloat16)
            return carry

        return line_mask

    def query_mask(i, carry):
        ids = as_column(doc_buf[r, pl.ds(i, 1), :])
        hit = jnp.where(lane < 3, ids, jnp.where(lane < 6, 1 - ids, 0))
        qx_buf[pl.ds(pl.multiple_of(i * 128, 128), 128), :] = jnp.where(hit == 1, -BF16_MAX, 0.0).astype(jnp.bfloat16)
        return carry

    wide = key_mask(lambda i: (i // 6, i % 6, (i % 6) // 2 * 1024 + i // 6 * 256 + i % 2 * 128))
    lax.fori_loop(0, 24, wide, 0)
    narrow = key_mask(lambda i: (i // 2, 6 + i % 2, 3072 + i % 2 * 512 + i // 2 * 128))
    lax.fori_loop(0, 8, narrow, 0)
    lax.fori_loop(0, ROWS // 128, query_mask, 0)

    own_half = pl.ds(pl.multiple_of(y * HID, HID), HID)
    peer_half = pl.ds(pl.multiple_of((1 - y) * HID, HID), HID)

    def project(rows, cols):
        return jnp.dot(tok_own[rows, :], w_buf[own_half, cols], preferred_element_type=jnp.float32) + jnp.dot(
            tok_peer[rows, :], w_buf[peer_half, cols], preferred_element_type=jnp.float32
        )

    def forward(ref, *index):
        return send(ref.at[index], ref.at[index], peer[CORE])

    k_in, kv_core = [], [[] for _ in CHUNKS]

    def keys_of(row, c):
        first, size = CHUNKS[c]
        return pl.ds(pl.multiple_of(first * 4 + row * size, size), size)

    def project_kv(c):
        tok_in[c].wait_recv()
        kv = project(pl.ds(*CHUNKS[c]), kv_cols).astype(jnp.bfloat16)
        keys = keys_of(r, c)
        k_buf[keys, k_cols] = kv[:, :HEAD_DIM]
        k_in.append([send(k_buf.at[keys, k_cols], k_buf.at[keys, k_cols], peer[XP])])
        vt_buf[:, keys] = jnp.transpose(kv[:, HEAD_DIM:])
        k_in[c].append(send(vt_buf.at[:, keys], vt_buf.at[:, keys], peer[XP]))
        kv_core[c].append(send(k_buf.at[keys, k_cols], k_buf.at[keys, k_cols], peer[CORE]))
        kv_core[c].append(send(vt_buf.at[:, keys], vt_buf.at[:, keys], peer[CORE]))

    def forward_kv(c):
        keys = keys_of(row_of[XP], c)
        k_in[c][0].wait_recv()
        kv_core[c].append(forward(k_buf, keys, k_cols))
        k_in[c][1].wait_recv()
        kv_core[c].append(forward(vt_buf, slice(None), keys))

    def wait_kv(c):
        for cp in kv_core[c]:
            cp.wait_recv()

    def project_q(c):
        rows = pl.ds(c * QB, QB)

        def q_tile(n, carry):
            cols = pl.ds(pl.multiple_of(n * 256, 256), 256)
            q_buf[rows, cols] = project(rows, cols).astype(jnp.bfloat16)
            return carry

        lax.fori_loop(0, HID // 256, q_tile, 0)

    wkv_x.wait_recv()
    wkv_f = forward(w_buf, shard(row_of[XP]), kv_cols)
    w_local.wait()
    tok_local.wait()
    w_core.wait_recv()
    wkv_f.wait_recv()
    wq_f = []

    def forward_wq(p):
        wq_x[p].wait_recv()
        wq_f.append(forward(w_buf, shard(row_of[XP], p, W_ROWS), q_cols))

    half = SHARD // 2

    def send_wo(p):
        return send(wo_hbm.at[pl.ds(p * half, half)], wo_buf.at[shard(r, p, half)], peer[XP])

    def tile_of(i):
        return (
            pl.ds(pl.multiple_of((i // HEADS) * QB, QB), QB),
            pl.ds(pl.multiple_of((i % HEADS) * HEAD_DIM, HEAD_DIM), HEAD_DIM),
        )

    def over_keys(f, a):
        return f(a.reshape(a.shape[0] // 8, 8, QB), axis=0)

    def to_keys(a):
        return jnp.concatenate([a] * (GROUP // 8), axis=0)

    def score_step(i, slot, j, state):
        top, total = state
        rows, cols = tile_of(i)
        q = jnp.concatenate([q_buf[rows, cols], qx_buf[rows, :]], axis=1)
        s = lax.dot_general(k_buf[pl.ds(j * KC, KC), :], q, NT, preferred_element_type=jnp.float32)
        for g in range(N_GROUP):
            part = s[g * GROUP : (g + 1) * GROUP]
            new_top = jnp.maximum(top, over_keys(jnp.max, part))
            scaled = new_top * EXP_SCALE
            top_buf[slot, j * N_GROUP + g] = scaled
            p = jnp.exp2(part * EXP_SCALE - to_keys(scaled))
            p_buf[slot, pl.ds(j * KC + g * GROUP, GROUP), :] = p
            total = total * jnp.exp2(top * EXP_SCALE - scaled) + over_keys(jnp.sum, p)
            top = new_top
        return top, total

    def value_step(slot, j, lse, acc):
        keys = pl.ds(j * KC, KC)
        factor = [to_keys(jnp.exp2(top_buf[slot, j * N_GROUP + g] - lse)) for g in range(N_GROUP)]
        weights = p_buf[slot, keys, :] * jnp.concatenate(factor, axis=0)
        o = jnp.dot(vt_buf[:, keys], weights.astype(jnp.bfloat16), preferred_element_type=jnp.float32)
        return o if acc is None else acc + o

    def ctx_copy(i):
        rows, cols = tile_of(i)
        return pltpu.make_async_remote_copy(
            src_ref=ctx_own.at[rows, cols], dst_ref=ctx_peer.at[rows, cols], send_sem=ctx_send.at[i], recv_sem=ctx_recv.at[i],
            device_id=y_peer, device_id_type=MESH,
        )

    empty = (jnp.full((8, QB), F32_MIN, jnp.float32), jnp.zeros((8, QB), jnp.float32))

    def load_state(slot):
        return state_buf[slot, 0], state_buf[slot, 1]

    def prefetch(*steps):
        def one(slot, carry):
            state = load_state(slot) if steps[0] else empty
            for j in steps:
                state = score_step(slot, slot, j, state)
            state_buf[slot, 0], state_buf[slot, 1] = state
            return carry

        lax.fori_loop(0, SLOTS, one, 0)

    def tile(i, slot, state, nxt=None, nxt_slot=None, nxt_state=None, nxt_steps=()):
        top, total = state
        best = jnp.max(top, axis=0, keepdims=True)
        whole = jnp.sum(total * jnp.exp2((top - best) * EXP_SCALE), axis=0, keepdims=True)
        lse = best * EXP_SCALE + jnp.log2(whole)
        acc = None
        steps = list(nxt_steps)
        for j in range(N_STEP):
            if steps:
                nxt_state = score_step(nxt, nxt_slot, steps.pop(0), nxt_state)
            acc = value_step(slot, j, lse, acc)
        rows, cols = tile_of(i)
        ctx_own[rows, cols] = jnp.transpose(acc).astype(jnp.bfloat16)
        return nxt_state

    every = range(N_STEP)

    def two_tiles(t, state):
        i = t * 2
        state = tile(i, 0, state, i + 1, 1, empty, every)
        state = tile(i + 1, 1, state, i + 2, 0, empty, every)
        ctx_copy(i).start()
        ctx_copy(i + 1).start()
        return state

    def project_out(b):
        rows = pl.ds(pl.multiple_of(b * QB, QB), QB)

        def wait_piece(h, carry):
            ctx_copy(b * HEADS + h).wait_recv()
            return carry

        lax.fori_loop(0, HEADS, wait_piece, 0)

        def out_tile(n, carry):
            cols = pl.ds(pl.multiple_of(n * 256, 256), 256)
            o = jnp.dot(ctx_own[rows, :], wo_buf[own_half, cols], preferred_element_type=jnp.float32) + jnp.dot(
                ctx_peer[rows, :], wo_buf[peer_half, cols], preferred_element_type=jnp.float32
            )
            out_buf[rows, cols] = o.astype(jnp.bfloat16)
            return carry

        lax.fori_loop(0, HID // 256, out_tile, 0)
        out = pltpu.make_async_copy(out_buf.at[rows], out_hbm.at[rows], out_sem.at[b])
        out.start()

    project_kv(0)
    forward_wq(0)
    forward_wq(1)
    project_kv(1)
    forward_wq(2)
    forward_wq(3)
    for cp in wq_f:
        cp.wait_recv()
    project_q(0)
    project_q(1)
    forward_kv(0)
    forward_kv(1)
    project_kv(2)
    project_q(2)
    for c in (0, 1):
        wait_kv(c)
    prefetch(0, 1)
    forward_kv(2)
    project_kv(3)
    wait_kv(2)
    prefetch(2)
    forward_kv(3)
    project_kv(4)
    wo_x = [send_wo(0), send_wo(1)]
    project_q(3)
    forward_kv(4)
    for c in (3, 4):
        wait_kv(c)

    last = N_STEP - 1
    state = score_step(0, 0, last, load_state(0))
    for i in range(SLOTS):
        if i + 1 < SLOTS:
            state = tile(i, i, state, i + 1, i + 1, load_state(i + 1), (last,))
        else:
            state = tile(i, i, state, i + 1, 0, empty, every)
        if i % 2:
            ctx_copy(i - 1).start()
            ctx_copy(i).start()

    pairs = HEADS // 2
    state = lax.fori_loop(pairs, 2 * pairs, two_tiles, state)
    wo_f = []
    for p in (0, 1):
        wo_x[p].wait_recv()
        wo_f.append(forward(wo_buf, shard(row_of[XP], p, half)))

    state = lax.fori_loop(2 * pairs, 3 * pairs, two_tiles, state)
    wo_local.wait()
    wo_core.wait_recv()
    for cp in wo_f:
        cp.wait_recv()
    project_out(0)
    state = lax.fori_loop(3 * pairs, 4 * pairs - 1, two_tiles, state)
    state = tile(TILES - 2, 0, state, TILES - 1, 1, empty, every)
    ctx_copy(TILES - 2).start()
    tile(TILES - 1, 1, state)
    ctx_copy(TILES - 1).start()

    def last_block(b, carry):
        project_out(b)
        return carry

    lax.fori_loop(1, N_BLOCK, last_block, 0)

    def wait_out(b, carry):
        rows = pl.ds(pl.multiple_of(b * QB, QB), QB)
        pltpu.make_async_copy(out_buf.at[rows], out_hbm.at[rows], out_sem.at[b]).wait()
        return carry

    lax.fori_loop(0, N_BLOCK, wait_out, 0)
    for cp in sent:
        cp.wait_send()

    def wait_sent(i, carry):
        ctx_copy(i).wait_send()
        return carry

    lax.fori_loop(0, TILES, wait_sent, 0)
    assert next(number) <= N_SEM


def solution(mesh):
    def local_block(tokens, w_qkv, w_out, doc_ids):
        bf16, f32 = jnp.bfloat16, jnp.float32
        dma = pltpu.SemaphoreType.DMA
        any_spec = pl.BlockSpec(memory_space=pl.ANY)
        return pl.pallas_call(
            kernel,
            out_shape=jax.ShapeDtypeStruct(tokens.shape, bf16),
            in_specs=[any_spec] * 4,
            out_specs=any_spec,
            scratch_shapes=[
                pltpu.VMEM((ROWS, HID), bf16),
                pltpu.VMEM((ROWS, HID), bf16),
                pltpu.VMEM((2 * HID, QKV), bf16),
                pltpu.VMEM((2 * HID, HID), bf16),
                pltpu.VMEM((4, 8, 128), jnp.int32),
                pltpu.VMEM((ROWS, HID), bf16),
                pltpu.VMEM((ROWS, 128), bf16),
                pltpu.VMEM((SEQ, 2 * HEAD_DIM), bf16),
                pltpu.VMEM((HEAD_DIM, SEQ), bf16),
                pltpu.VMEM((SLOTS, SEQ, QB), f32),
                pltpu.VMEM((SLOTS, SEQ // GROUP, 8, QB), f32),
                pltpu.VMEM((SLOTS, 2, 8, QB), f32),
                pltpu.VMEM((ROWS, HID), bf16),
                pltpu.VMEM((ROWS, HID), bf16),
                dma((4,)),
                dma((N_SEM,)),
                dma((N_SEM,)),
                dma((TILES,)),
                dma((TILES,)),
                dma((N_BLOCK,)),
            ],
            compiler_params=pltpu.CompilerParams(
                collective_id=0, has_side_effects=True, vmem_limit_bytes=67043328
            ),
        )(tokens, w_qkv, w_out, doc_ids.reshape(8, 128))

    row_spec = P(("data", "row"), "col")
    weight_spec = P("row", "col")
    return jax.shard_map(
        local_block,
        mesh=mesh,
        in_specs=(row_spec, weight_spec, weight_spec, P(("data", "row"))),
        out_specs=row_spec,
        check_vma=False,
    )
```

```python
import itertools
import math

import jax
import jax.numpy as jnp
from jax import lax
from jax.experimental import pallas as pl
from jax.experimental.pallas import tpu as pltpu
from jax.sharding import PartitionSpec as P

HEAD_DIM = 128
MESH = pl.DeviceIdType.MESH

ROWS = 1024
HID = 1024
SEQ = 4096
HEADS = 8
QKV = 1280
SHARD = 512
QB = 256
KC = 1024
GROUP = 128
N_GROUP = KC // GROUP
N_STEP = SEQ // KC
CHUNKS = ((0, 256), (256, 256), (512, 256), (768, 128), (896, 128))
W_PIECES = 4
W_ROWS = SHARD // W_PIECES
N_BLOCK = ROWS // QB
TILES = HEADS * N_BLOCK
SLOTS = 8
N_SEM = 64
CORE, XP, DIAG = 0, 1, 2
EXP_SCALE = math.log2(math.e) / math.sqrt(HEAD_DIM)
NT = (((1,), (1,)), ((), ()))
BF16_MAX = float(jnp.finfo(jnp.bfloat16).max)
F32_MIN = float(jnp.finfo(jnp.float32).min)


def kernel(
    tok_hbm, w_hbm, wo_hbm, doc_hbm, out_hbm,
    tok_own, tok_peer, w_buf, wo_buf, doc_buf, q_buf, qx_buf, k_buf, kx_buf, vw_buf, vn_buf, p_buf, top_buf, state_buf,
    ctx_own, ctx_peer, loc_sem, send_sem, recv_sem, ctx_send, ctx_recv, out_sem,
):
    d, y, r = lax.axis_index("data"), lax.axis_index("col"), lax.axis_index("row")
    x, core = r // 2, r % 2
    row_of = {CORE: x * 2 + (1 - core), XP: (1 - x) * 2 + core, DIAG: (1 - x) * 2 + (1 - core)}
    y_peer = (d, 1 - y, r)
    peer = {k: (d, y, v) for k, v in row_of.items()}
    out_buf = tok_own

    barrier = pltpu.get_barrier_semaphore()
    for p in (y_peer, peer[CORE], peer[XP], peer[DIAG]):
        pl.semaphore_signal(barrier, inc=1, device_id=p, device_id_type=MESH)
    pl.semaphore_wait(barrier, 4)

    number = itertools.count()
    sent = []

    def send(src, dst, device):
        i = next(number)
        cp = pltpu.make_async_remote_copy(
            src_ref=src, dst_ref=dst, send_sem=send_sem.at[i], recv_sem=recv_sem.at[i], device_id=device, device_id_type=MESH
        )
        cp.start()
        sent.append(cp)
        return cp

    def local(src, dst, i):
        cp = pltpu.make_async_copy(src, dst, loc_sem.at[i])
        cp.start()
        return cp

    def shard(row, piece=0, size=SHARD):
        return pl.ds(pl.multiple_of(row * SHARD + piece * size, size), size)

    kv_cols, q_cols = pl.ds(HID, 2 * HEAD_DIM), pl.ds(0, HID)

    tok_in = []
    for first, size in CHUNKS:
        rows = pl.ds(first, size)
        tok_in.append(send(tok_hbm.at[rows], tok_peer.at[rows], y_peer))
    wkv_x = send(w_hbm.at[:, kv_cols], w_buf.at[shard(r), kv_cols], peer[XP])
    doc_in = [send(doc_hbm, doc_buf.at[r], peer[k]) for k in (CORE, XP, DIAG)]
    wq_x = [
        send(w_hbm.at[pl.ds(p * W_ROWS, W_ROWS), q_cols], w_buf.at[shard(r, p, W_ROWS), q_cols], peer[XP])
        for p in range(W_PIECES)
    ]
    w_core = send(w_hbm, w_buf.at[shard(r)], peer[CORE])
    wo_core = send(wo_hbm, wo_buf.at[shard(r)], peer[CORE])
    doc_local = local(doc_hbm, doc_buf.at[r], 0)
    w_local = local(w_hbm, w_buf.at[shard(r)], 1)
    tok_local = local(tok_hbm, tok_own, 2)
    wo_local = local(wo_hbm, wo_buf.at[shard(r)], 3)

    doc_local.wait()
    for cp in doc_in:
        cp.wait_recv()
    lane = lax.broadcasted_iota(jnp.int32, (128, 128), 1)

    def as_column(line):
        return jnp.transpose(jnp.broadcast_to(line, (128, 128)))

    def key_mask(place):
        def line_mask(i, carry):
            part, line, first = place(i)
            ids = as_column(doc_buf[part, pl.ds(line, 1), :])
            hit = jnp.where(lane < 3, 1 - ids, jnp.where(lane < 6, ids, 0))
            kx_buf[pl.ds(pl.multiple_of(first, 128), 128), :] = hit.astype(jnp.float32).astype(jnp.bfloat16)
            return carry

        return line_mask

    def query_mask(i, carry):
        ids = as_column(doc_buf[r, pl.ds(i, 1), :])
        hit = jnp.where(lane < 3, ids, jnp.where(lane < 6, 1 - ids, 0))
        qx_buf[pl.ds(pl.multiple_of(i * 128, 128), 128), :] = jnp.where(hit == 1, -BF16_MAX, 0.0).astype(jnp.bfloat16)
        return carry

    wide = key_mask(lambda i: (i // 6, i % 6, (i % 6) // 2 * 1024 + i // 6 * 256 + i % 2 * 128))
    lax.fori_loop(0, 24, wide, 0)
    narrow = key_mask(lambda i: (i // 2, 6 + i % 2, 3072 + i % 2 * 512 + i // 2 * 128))
    lax.fori_loop(0, 8, narrow, 0)
    lax.fori_loop(0, ROWS // 128, query_mask, 0)

    own_half = pl.ds(pl.multiple_of(y * HID, HID), HID)
    peer_half = pl.ds(pl.multiple_of((1 - y) * HID, HID), HID)

    def project(rows, cols):
        return jnp.dot(tok_own[rows, :], w_buf[own_half, cols], preferred_element_type=jnp.float32) + jnp.dot(
            tok_peer[rows, :], w_buf[peer_half, cols], preferred_element_type=jnp.float32
        )

    def forward(ref, *index):
        return send(ref.at[index], ref.at[index], peer[CORE])

    k_in, kv_core = [], [[] for _ in CHUNKS]

    def keys_of(row, c):
        first, size = CHUNKS[c]
        values = vw_buf.at[c * 4 + row] if size == 256 else vn_buf.at[(c - N_STEP + 1) * 4 + row]
        return k_buf.at[pl.ds(pl.multiple_of(first * 4 + row * size, size), size)], values

    def project_kv(c):
        tok_in[c].wait_recv()
        kv = project(pl.ds(*CHUNKS[c]), kv_cols).astype(jnp.bfloat16)
        keys, values = keys_of(r, c)
        keys[...] = kv[:, :HEAD_DIM]
        k_in.append([send(keys, keys, peer[XP])])
        values[...] = jnp.transpose(kv[:, HEAD_DIM:])
        k_in[c].append(send(values, values, peer[XP]))
        kv_core[c].append(send(keys, keys, peer[CORE]))
        kv_core[c].append(send(values, values, peer[CORE]))

    def forward_kv(c):
        for ref, cp in zip(keys_of(row_of[XP], c), k_in[c]):
            cp.wait_recv()
            kv_core[c].append(send(ref, ref, peer[CORE]))

    def wait_kv(c):
        for cp in kv_core[c]:
            cp.wait_recv()

    def project_q(c):
        rows = pl.ds(c * QB, QB)

        def q_tile(n, carry):
            cols = pl.ds(pl.multiple_of(n * 256, 256), 256)
            q_buf[rows, cols] = project(rows, cols).astype(jnp.bfloat16)
            return carry

        lax.fori_loop(0, HID // 256, q_tile, 0)

    wkv_x.wait_recv()
    wkv_f = forward(w_buf, shard(row_of[XP]), kv_cols)
    w_local.wait()
    tok_local.wait()
    w_core.wait_recv()
    wkv_f.wait_recv()
    wq_f = []

    def forward_wq(p):
        wq_x[p].wait_recv()
        wq_f.append(forward(w_buf, shard(row_of[XP], p, W_ROWS), q_cols))

    half = SHARD // 2

    def send_wo(p):
        return send(wo_hbm.at[pl.ds(p * half, half)], wo_buf.at[shard(r, p, half)], peer[XP])

    def tile_of(i):
        return (
            pl.ds(pl.multiple_of((i // HEADS) * QB, QB), QB),
            pl.ds(pl.multiple_of((i % HEADS) * HEAD_DIM, HEAD_DIM), HEAD_DIM),
        )

    def over_keys(f, a):
        return f(a.reshape(a.shape[0] // 8, 8, QB), axis=0)

    def to_keys(a):
        return jnp.concatenate([a] * (GROUP // 8), axis=0)

    def score_step(i, slot, j, state):
        top, total = state
        rows, cols = tile_of(i)
        q = jnp.concatenate([q_buf[rows, cols], qx_buf[rows, :]], axis=1)
        k = jnp.concatenate([k_buf[pl.ds(j * KC, KC), :], kx_buf[pl.ds(j * KC, KC), :]], axis=1)
        s = lax.dot_general(k, q, NT, preferred_element_type=jnp.float32)
        for g in range(N_GROUP):
            part = s[g * GROUP : (g + 1) * GROUP]
            new_top = jnp.maximum(top, over_keys(jnp.max, part))
            scaled = new_top * EXP_SCALE
            top_buf[slot, j * N_GROUP + g] = scaled
            p = jnp.exp2(part * EXP_SCALE - to_keys(scaled))
            p_buf[slot, pl.ds(j * KC + g * GROUP, GROUP), :] = p
            total = total * jnp.exp2(top * EXP_SCALE - scaled) + over_keys(jnp.sum, p)
            top = new_top
        return top, total

    def value_step(slot, j, lse, acc):
        keys = pl.ds(j * KC, KC)
        factor = [to_keys(jnp.exp2(top_buf[slot, j * N_GROUP + g] - lse)) for g in range(N_GROUP)]
        weights = p_buf[slot, keys, :] * jnp.concatenate(factor, axis=0)
        parts = [vw_buf[j * 4 + i] for i in range(4)] if j + 1 < N_STEP else [vn_buf[i] for i in range(8)]
        o = jnp.dot(jnp.concatenate(parts, axis=1), weights.astype(jnp.bfloat16), preferred_element_type=jnp.float32)
        return o if acc is None else acc + o

    def ctx_copy(i):
        return pltpu.make_async_remote_copy(
            src_ref=ctx_own.at[i], dst_ref=ctx_peer.at[i], send_sem=ctx_send.at[i], recv_sem=ctx_recv.at[i],
            device_id=y_peer, device_id_type=MESH,
        )

    empty = (jnp.full((8, QB), F32_MIN, jnp.float32), jnp.zeros((8, QB), jnp.float32))

    def load_state(slot):
        return state_buf[slot, 0], state_buf[slot, 1]

    def prefetch(*steps):
        def one(slot, carry):
            state = load_state(slot) if steps[0] else empty
            for j in steps:
                state = score_step(slot, slot, j, state)
            state_buf[slot, 0], state_buf[slot, 1] = state
            return carry

        lax.fori_loop(0, SLOTS, one, 0)

    def tile(i, slot, state, nxt=None, nxt_slot=None, nxt_state=None, nxt_steps=()):
        top, total = state
        best = jnp.max(top, axis=0, keepdims=True)
        whole = jnp.sum(total * jnp.exp2((top - best) * EXP_SCALE), axis=0, keepdims=True)
        lse = best * EXP_SCALE + jnp.log2(whole)
        acc = None
        steps = list(nxt_steps)
        for j in range(N_STEP):
            if steps:
                nxt_state = score_step(nxt, nxt_slot, steps.pop(0), nxt_state)
            acc = value_step(slot, j, lse, acc)
        ctx_own[i] = jnp.transpose(acc).astype(jnp.bfloat16)
        return nxt_state

    every = range(N_STEP)

    def two_tiles(t, state):
        i = t * 2
        state = tile(i, 0, state, i + 1, 1, empty, every)
        state = tile(i + 1, 1, state, i + 2, 0, empty, every)
        ctx_copy(i).start()
        ctx_copy(i + 1).start()
        return state

    def project_out(b):
        rows = pl.ds(pl.multiple_of(b * QB, QB), QB)

        def wait_piece(h, carry):
            ctx_copy(b * HEADS + h).wait_recv()
            return carry

        lax.fori_loop(0, HEADS, wait_piece, 0)

        def out_tile(n, carry):
            cols = pl.ds(pl.multiple_of(n * 256, 256), 256)
            own, other = (jnp.concatenate([ref[b * HEADS + h] for h in range(HEADS)], axis=1) for ref in (ctx_own, ctx_peer))
            o = jnp.dot(own, wo_buf[own_half, cols], preferred_element_type=jnp.float32) + jnp.dot(
                other, wo_buf[peer_half, cols], preferred_element_type=jnp.float32
            )
            out_buf[rows, cols] = o.astype(jnp.bfloat16)
            return carry

        lax.fori_loop(0, HID // 256, out_tile, 0)
        out = pltpu.make_async_copy(out_buf.at[rows], out_hbm.at[rows], out_sem.at[b])
        out.start()

    project_kv(0)
    forward_wq(0)
    forward_wq(1)
    project_kv(1)
    forward_wq(2)
    forward_wq(3)
    for cp in wq_f:
        cp.wait_recv()
    project_q(0)
    project_q(1)
    forward_kv(0)
    forward_kv(1)
    project_kv(2)
    project_q(2)
    for c in (0, 1):
        wait_kv(c)
    prefetch(0, 1)
    forward_kv(2)
    project_kv(3)
    wait_kv(2)
    prefetch(2)
    forward_kv(3)
    project_kv(4)
    wo_x = [send_wo(0), send_wo(1)]
    project_q(3)
    forward_kv(4)
    for c in (3, 4):
        wait_kv(c)

    last = N_STEP - 1
    state = score_step(0, 0, last, load_state(0))
    for i in range(SLOTS):
        if i + 1 < SLOTS:
            state = tile(i, i, state, i + 1, i + 1, load_state(i + 1), (last,))
        else:
            state = tile(i, i, state, i + 1, 0, empty, every)
        if i % 2:
            ctx_copy(i - 1).start()
            ctx_copy(i).start()

    pairs = HEADS // 2
    state = lax.fori_loop(pairs, 2 * pairs, two_tiles, state)
    wo_f = []

    def forward_wo(p):
        wo_x[p].wait_recv()
        wo_f.append(forward(wo_buf, shard(row_of[XP], p, half)))

    forward_wo(0)
    state = lax.fori_loop(2 * pairs, 3 * pairs, two_tiles, state)
    forward_wo(1)
    state = lax.fori_loop(3 * pairs, 4 * pairs - 1, two_tiles, state)
    state = tile(TILES - 2, 0, state, TILES - 1, 1, empty, every)
    ctx_copy(TILES - 2).start()
    tile(TILES - 1, 1, state)
    ctx_copy(TILES - 1).start()

    wo_local.wait()
    wo_core.wait_recv()
    for cp in wo_f:
        cp.wait_recv()

    def last_block(b, carry):
        project_out(b)
        return carry

    lax.fori_loop(0, N_BLOCK, last_block, 0)

    def wait_out(b, carry):
        rows = pl.ds(pl.multiple_of(b * QB, QB), QB)
        pltpu.make_async_copy(out_buf.at[rows], out_hbm.at[rows], out_sem.at[b]).wait()
        return carry

    lax.fori_loop(0, N_BLOCK, wait_out, 0)
    for cp in sent:
        cp.wait_send()

    def wait_sent(i, carry):
        ctx_copy(i).wait_send()
        return carry

    lax.fori_loop(0, TILES, wait_sent, 0)
    assert next(number) <= N_SEM


def solution(mesh):
    def local_block(tokens, w_qkv, w_out, doc_ids):
        bf16, f32 = jnp.bfloat16, jnp.float32
        dma = pltpu.SemaphoreType.DMA
        any_spec = pl.BlockSpec(memory_space=pl.ANY)
        return pl.pallas_call(
            kernel,
            out_shape=jax.ShapeDtypeStruct(tokens.shape, bf16),
            in_specs=[any_spec] * 4,
            out_specs=any_spec,
            scratch_shapes=[
                pltpu.VMEM((ROWS, HID), bf16),
                pltpu.VMEM((ROWS, HID), bf16),
                pltpu.VMEM((2 * HID, QKV), bf16),
                pltpu.VMEM((2 * HID, HID), bf16),
                pltpu.VMEM((4, 8, 128), jnp.int32),
                pltpu.VMEM((ROWS, HID), bf16),
                pltpu.VMEM((ROWS, 128), bf16),
                pltpu.VMEM((SEQ, HEAD_DIM), bf16),
                pltpu.VMEM((SEQ, HEAD_DIM), bf16),
                pltpu.VMEM((12, HEAD_DIM, 256), bf16),
                pltpu.VMEM((8, HEAD_DIM, 128), bf16),
                pltpu.VMEM((SLOTS, SEQ, QB), f32),
                pltpu.VMEM((SLOTS, SEQ // GROUP, 8, QB), f32),
                pltpu.VMEM((SLOTS, 2, 8, QB), f32),
                pltpu.VMEM((TILES, QB, HEAD_DIM), bf16),
                pltpu.VMEM((TILES, QB, HEAD_DIM), bf16),
                dma((4,)),
                dma((N_SEM,)),
                dma((N_SEM,)),
                dma((TILES,)),
                dma((TILES,)),
                dma((N_BLOCK,)),
            ],
            compiler_params=pltpu.CompilerParams(
                collective_id=0, has_side_effects=True, vmem_limit_bytes=67043328
            ),
        )(tokens, w_qkv, w_out, doc_ids.reshape(8, 128))

    row_spec = P(("data", "row"), "col")
    weight_spec = P("row", "col")
    return jax.shard_map(
        local_block,
        mesh=mesh,
        in_specs=(row_spec, weight_spec, weight_spec, P(("data", "row"))),
        out_specs=row_spec,
        check_vma=False,
    )
```

```python
import itertools
import math

import jax
import jax.numpy as jnp
from jax import lax
from jax.experimental import pallas as pl
from jax.experimental.pallas import tpu as pltpu
from jax.sharding import PartitionSpec as P

HEAD_DIM = 128
MESH = pl.DeviceIdType.MESH

ROWS = 1024
HID = 1024
SEQ = 4096
HEADS = 8
QKV = 1280
SHARD = 512
QB = 256
KC = 1024
GROUP = 128
N_GROUP = KC // GROUP
N_STEP = SEQ // KC
CHUNKS = ((0, 256), (256, 256), (512, 256), (768, 128), (896, 128))
W_PIECES = 4
W_ROWS = SHARD // W_PIECES
N_BLOCK = ROWS // QB
TILES = HEADS * N_BLOCK
SLOTS = 8
N_SEM = 64
CORE, XP, DIAG = 0, 1, 2
EXP_SCALE = math.log2(math.e) / math.sqrt(HEAD_DIM)
NT = (((1,), (1,)), ((), ()))
BF16_MAX = float(jnp.finfo(jnp.bfloat16).max)
F32_MIN = float(jnp.finfo(jnp.float32).min)


def kernel(
    tok_hbm, w_hbm, wo_hbm, doc_hbm, out_hbm,
    tok_own, tok_peer, w_buf, wo_buf, doc_buf, q_buf, qx_buf, k_buf, kx_buf, vw_buf, vn_buf, p_buf, top_buf, state_buf,
    ctx_own, ctx_peer, loc_sem, send_sem, recv_sem, ctx_send, ctx_recv, out_sem,
):
    d, y, r = lax.axis_index("data"), lax.axis_index("col"), lax.axis_index("row")
    x, core = r // 2, r % 2
    row_of = {CORE: x * 2 + (1 - core), XP: (1 - x) * 2 + core, DIAG: (1 - x) * 2 + (1 - core)}
    y_peer = (d, 1 - y, r)
    peer = {k: (d, y, v) for k, v in row_of.items()}
    out_buf = tok_own

    barrier = pltpu.get_barrier_semaphore()
    for p in (y_peer, peer[CORE], peer[XP], peer[DIAG]):
        pl.semaphore_signal(barrier, inc=1, device_id=p, device_id_type=MESH)
    pl.semaphore_wait(barrier, 4)

    number = itertools.count()
    sent = []

    def send(src, dst, device):
        i = next(number)
        cp = pltpu.make_async_remote_copy(
            src_ref=src, dst_ref=dst, send_sem=send_sem.at[i], recv_sem=recv_sem.at[i], device_id=device, device_id_type=MESH
        )
        cp.start()
        sent.append(cp)
        return cp

    def local(src, dst, i):
        cp = pltpu.make_async_copy(src, dst, loc_sem.at[i])
        cp.start()
        return cp

    def shard(row, piece=0, size=SHARD):
        return pl.ds(pl.multiple_of(row * SHARD + piece * size, size), size)

    kv_cols, q_cols = pl.ds(HID, 2 * HEAD_DIM), pl.ds(0, HID)

    tok_in = []
    for first, size in CHUNKS:
        rows = pl.ds(first, size)
        tok_in.append(send(tok_hbm.at[rows], tok_peer.at[rows], y_peer))
    wkv_x = send(w_hbm.at[:, kv_cols], w_buf.at[shard(r), kv_cols], peer[XP])
    doc_in = [send(doc_hbm, doc_buf.at[r], peer[k]) for k in (CORE, XP, DIAG)]
    wq_x = [
        send(w_hbm.at[pl.ds(p * W_ROWS, W_ROWS), q_cols], w_buf.at[shard(r, p, W_ROWS), q_cols], peer[XP])
        for p in range(W_PIECES)
    ]
    w_core = send(w_hbm, w_buf.at[shard(r)], peer[CORE])
    wo_core = send(wo_hbm, wo_buf.at[shard(r)], peer[CORE])
    doc_local = local(doc_hbm, doc_buf.at[r], 0)
    w_local = local(w_hbm, w_buf.at[shard(r)], 1)
    tok_local = local(tok_hbm, tok_own, 2)
    wo_local = local(wo_hbm, wo_buf.at[shard(r)], 3)

    doc_local.wait()
    for cp in doc_in:
        cp.wait_recv()
    lane = lax.broadcasted_iota(jnp.int32, (128, 128), 1)

    def as_column(line):
        return jnp.transpose(jnp.broadcast_to(line, (128, 128)))

    def key_mask(place):
        def line_mask(i, carry):
            part, line, first = place(i)
            ids = as_column(doc_buf[part, pl.ds(line, 1), :])
            hit = jnp.where(lane < 3, 1 - ids, jnp.where(lane < 6, ids, 0))
            kx_buf[pl.ds(pl.multiple_of(first, 128), 128), :] = hit.astype(jnp.float32).astype(jnp.bfloat16)
            return carry

        return line_mask

    def query_mask(i, carry):
        ids = as_column(doc_buf[r, pl.ds(i, 1), :])
        hit = jnp.where(lane < 3, ids, jnp.where(lane < 6, 1 - ids, 0))
        qx_buf[pl.ds(pl.multiple_of(i * 128, 128), 128), :] = jnp.where(hit == 1, -BF16_MAX, 0.0).astype(jnp.bfloat16)
        return carry

    wide = key_mask(lambda i: (i // 6, i % 6, (i % 6) // 2 * 1024 + i // 6 * 256 + i % 2 * 128))
    lax.fori_loop(0, 24, wide, 0)
    narrow = key_mask(lambda i: (i // 2, 6 + i % 2, 3072 + i % 2 * 512 + i // 2 * 128))
    lax.fori_loop(0, 8, narrow, 0)
    lax.fori_loop(0, ROWS // 128, query_mask, 0)

    own_half = pl.ds(pl.multiple_of(y * HID, HID), HID)
    peer_half = pl.ds(pl.multiple_of((1 - y) * HID, HID), HID)

    def project(rows, cols):
        return jnp.dot(tok_own[rows, :], w_buf[own_half, cols], preferred_element_type=jnp.float32) + jnp.dot(
            tok_peer[rows, :], w_buf[peer_half, cols], preferred_element_type=jnp.float32
        )

    def forward(ref, *index):
        return send(ref.at[index], ref.at[index], peer[CORE])

    k_in, kv_core = [], [[] for _ in CHUNKS]

    def keys_of(row, c):
        first, size = CHUNKS[c]
        values = vw_buf.at[c * 4 + row] if size == 256 else vn_buf.at[(c - N_STEP + 1) * 4 + row]
        return k_buf.at[pl.ds(pl.multiple_of(first * 4 + row * size, size), size)], values

    def project_kv(c):
        tok_in[c].wait_recv()
        kv = project(pl.ds(*CHUNKS[c]), kv_cols).astype(jnp.bfloat16)
        keys, values = keys_of(r, c)
        keys[...] = kv[:, :HEAD_DIM]
        values[...] = jnp.transpose(kv[:, HEAD_DIM:])

    def send_kv(c):
        refs = keys_of(r, c)
        k_in.append([send(ref, ref, peer[XP]) for ref in refs])
        kv_core[c].extend(send(ref, ref, peer[CORE]) for ref in refs)

    def forward_kv(c):
        for ref, cp in zip(keys_of(row_of[XP], c), k_in[c]):
            cp.wait_recv()
            kv_core[c].append(send(ref, ref, peer[CORE]))

    def wait_kv(c):
        for cp in kv_core[c]:
            cp.wait_recv()

    def project_q(c):
        rows = pl.ds(c * QB, QB)

        def q_tile(n, carry):
            cols = pl.ds(pl.multiple_of(n * 256, 256), 256)
            q_buf[rows, cols] = project(rows, cols).astype(jnp.bfloat16)
            return carry

        lax.fori_loop(0, HID // 256, q_tile, 0)

    wkv_x.wait_recv()
    wkv_f = forward(w_buf, shard(row_of[XP]), kv_cols)
    w_local.wait()
    tok_local.wait()
    w_core.wait_recv()
    wkv_f.wait_recv()
    wq_f = []

    def forward_wq(p):
        wq_x[p].wait_recv()
        wq_f.append(forward(w_buf, shard(row_of[XP], p, W_ROWS), q_cols))

    half = SHARD // 2

    def send_wo(p):
        return send(wo_hbm.at[pl.ds(p * half, half)], wo_buf.at[shard(r, p, half)], peer[XP])

    def tile_of(i):
        return (
            pl.ds(pl.multiple_of((i // HEADS) * QB, QB), QB),
            pl.ds(pl.multiple_of((i % HEADS) * HEAD_DIM, HEAD_DIM), HEAD_DIM),
        )

    def over_keys(f, a):
        return f(a.reshape(a.shape[0] // 8, 8, QB), axis=0)

    def to_keys(a):
        return jnp.concatenate([a] * (GROUP // 8), axis=0)

    def score_step(i, slot, j, state):
        top, total = state
        rows, cols = tile_of(i)
        q = jnp.concatenate([q_buf[rows, cols], qx_buf[rows, :]], axis=1)
        k = jnp.concatenate([k_buf[pl.ds(j * KC, KC), :], kx_buf[pl.ds(j * KC, KC), :]], axis=1)
        s = lax.dot_general(k, q, NT, preferred_element_type=jnp.float32)
        for g in range(N_GROUP):
            part = s[g * GROUP : (g + 1) * GROUP]
            new_top = jnp.maximum(top, over_keys(jnp.max, part))
            scaled = new_top * EXP_SCALE
            top_buf[slot, j * N_GROUP + g] = scaled
            p = jnp.exp2(part * EXP_SCALE - to_keys(scaled))
            p_buf[slot, pl.ds(j * KC + g * GROUP, GROUP), :] = p
            total = total * jnp.exp2(top * EXP_SCALE - scaled) + over_keys(jnp.sum, p)
            top = new_top
        return top, total

    def value_step(slot, j, lse, acc):
        keys = pl.ds(j * KC, KC)
        factor = [to_keys(jnp.exp2(top_buf[slot, j * N_GROUP + g] - lse)) for g in range(N_GROUP)]
        weights = p_buf[slot, keys, :] * jnp.concatenate(factor, axis=0)
        parts = [vw_buf[j * 4 + i] for i in range(4)] if j + 1 < N_STEP else [vn_buf[i] for i in range(8)]
        o = jnp.dot(jnp.concatenate(parts, axis=1), weights.astype(jnp.bfloat16), preferred_element_type=jnp.float32)
        return o if acc is None else acc + o

    def ctx_copy(i):
        return pltpu.make_async_remote_copy(
            src_ref=ctx_own.at[i], dst_ref=ctx_peer.at[i], send_sem=ctx_send.at[i], recv_sem=ctx_recv.at[i],
            device_id=y_peer, device_id_type=MESH,
        )

    empty = (jnp.full((8, QB), F32_MIN, jnp.float32), jnp.zeros((8, QB), jnp.float32))

    def load_state(slot):
        return state_buf[slot, 0], state_buf[slot, 1]

    def prefetch(*steps):
        def one(slot, carry):
            state = load_state(slot) if steps[0] else empty
            for j in steps:
                state = score_step(slot, slot, j, state)
            state_buf[slot, 0], state_buf[slot, 1] = state
            return carry

        lax.fori_loop(0, SLOTS, one, 0)

    def tile(i, slot, state, nxt=None, nxt_slot=None, nxt_state=None, nxt_steps=()):
        top, total = state
        best = jnp.max(top, axis=0, keepdims=True)
        whole = jnp.sum(total * jnp.exp2((top - best) * EXP_SCALE), axis=0, keepdims=True)
        lse = best * EXP_SCALE + jnp.log2(whole)
        acc = None
        steps = list(nxt_steps)
        for j in range(N_STEP):
            if steps:
                nxt_state = score_step(nxt, nxt_slot, steps.pop(0), nxt_state)
            acc = value_step(slot, j, lse, acc)
        ctx_own[i] = jnp.transpose(acc).astype(jnp.bfloat16)
        return nxt_state

    every = range(N_STEP)

    def two_tiles(t, state):
        i = t * 2
        state = tile(i, 0, state, i + 1, 1, empty, every)
        state = tile(i + 1, 1, state, i + 2, 0, empty, every)
        ctx_copy(i).start()
        ctx_copy(i + 1).start()
        return state

    def wait_pieces(first, end):
        def wait_piece(i, carry):
            ctx_copy(i).wait_recv()
            return carry

        lax.fori_loop(first, end, wait_piece, 0)

    def heads(ref, b, first, end):
        return jnp.concatenate([ref[b * HEADS + h] for h in range(first, end)], axis=1)

    def out_rows(half_index, first, end):
        size = (end - first) * HEAD_DIM
        return pl.ds(pl.multiple_of(half_index * HID + first * HEAD_DIM, HEAD_DIM), size)

    def out_copy(b, n):
        at = (pl.ds(pl.multiple_of(b * QB, QB), QB), pl.ds(pl.multiple_of(n * 256, 256), 256))
        return pltpu.make_async_copy(out_buf.at[at], out_hbm.at[at], out_sem.at[b * 4 + n])

    def store_out(b, n, o):
        out_buf[pl.ds(pl.multiple_of(b * QB, QB), QB), pl.ds(pl.multiple_of(n * 256, 256), 256)] = o.astype(jnp.bfloat16)
        out_copy(b, n).start()

    def out_product(b, n, end):
        cols = pl.ds(pl.multiple_of(n * 256, 256), 256)
        own = jnp.dot(heads(ctx_own, b, 0, HEADS), wo_buf[own_half, cols], preferred_element_type=jnp.float32)
        rows = out_rows(1 - y, 0, end)
        return own + jnp.dot(heads(ctx_peer, b, 0, end), wo_buf[rows, cols], preferred_element_type=jnp.float32)

    def project_out(b, carry):
        wait_pieces(b * HEADS, (b + 1) * HEADS)

        def out_tile(n, carry):
            store_out(b, n, out_product(b, n, HEADS))
            return carry

        return lax.fori_loop(0, 4, out_tile, carry)

    def project_last():
        b, most = N_BLOCK - 1, HEADS - 2
        wait_pieces(b * HEADS, b * HEADS + most)

        def first_part(n, carry):
            p_buf[2, pl.ds(pl.multiple_of(n * QB, QB), QB), :] = out_product(b, n, most)
            return carry

        lax.fori_loop(0, 4, first_part, 0)
        wait_pieces(b * HEADS + most, TILES)
        for n in range(4):
            cols, rows = pl.ds(n * 256, 256), out_rows(1 - y, most, HEADS)
            o = jnp.dot(heads(ctx_peer, b, most, HEADS), wo_buf[rows, cols], preferred_element_type=jnp.float32)
            store_out(b, n, p_buf[2, pl.ds(n * QB, QB), :] + o)

    project_kv(0)
    forward_wq(0)
    forward_wq(1)
    project_kv(1)
    forward_wq(2)
    forward_wq(3)
    send_kv(0)
    send_kv(1)
    for cp in wq_f:
        cp.wait_recv()
    project_q(0)
    project_q(1)
    project_kv(2)
    send_kv(2)
    forward_kv(0)
    forward_kv(1)
    project_q(2)
    for c in (0, 1):
        wait_kv(c)
    prefetch(0, 1)
    project_kv(3)
    send_kv(3)
    project_kv(4)
    send_kv(4)
    wo_x = [send_wo(0), send_wo(1)]
    forward_kv(2)
    wait_kv(2)
    prefetch(2)
    forward_kv(3)
    forward_kv(4)
    project_q(3)
    for c in (3, 4):
        wait_kv(c)

    last = N_STEP - 1
    state = score_step(0, 0, last, load_state(0))
    for i in range(SLOTS):
        if i + 1 < SLOTS:
            state = tile(i, i, state, i + 1, i + 1, load_state(i + 1), (last,))
        else:
            state = tile(i, i, state, i + 1, 0, empty, every)
        if i % 2:
            for n in range(max(i - 1, 1), i + 1):
                ctx_copy(n).start()
        elif i == 0:
            ctx_copy(0).start()

    pairs = HEADS // 2
    state = lax.fori_loop(pairs, 2 * pairs, two_tiles, state)
    wo_f = []

    def forward_wo(p):
        wo_x[p].wait_recv()
        wo_f.append(forward(wo_buf, shard(row_of[XP], p, half)))

    forward_wo(0)
    state = lax.fori_loop(2 * pairs, 3 * pairs, two_tiles, state)
    forward_wo(1)
    state = lax.fori_loop(3 * pairs, 4 * pairs - 1, two_tiles, state)
    state = tile(TILES - 2, 0, state, TILES - 1, 1, empty, every)
    ctx_copy(TILES - 2).start()
    tile(TILES - 1, 1, state)
    ctx_copy(TILES - 1).start()

    wo_local.wait()
    wo_core.wait_recv()
    for cp in wo_f:
        cp.wait_recv()

    lax.fori_loop(0, N_BLOCK - 1, project_out, 0)
    project_last()

    def wait_out(i, carry):
        out_copy(i // 4, i % 4).wait()
        return carry

    lax.fori_loop(0, N_BLOCK * 4, wait_out, 0)
    for cp in sent:
        cp.wait_send()

    def wait_sent(i, carry):
        ctx_copy(i).wait_send()
        return carry

    lax.fori_loop(0, TILES, wait_sent, 0)
    assert next(number) <= N_SEM


def solution(mesh):
    def local_block(tokens, w_qkv, w_out, doc_ids):
        bf16, f32 = jnp.bfloat16, jnp.float32
        dma = pltpu.SemaphoreType.DMA
        any_spec = pl.BlockSpec(memory_space=pl.ANY)
        return pl.pallas_call(
            kernel,
            out_shape=jax.ShapeDtypeStruct(tokens.shape, bf16),
            in_specs=[any_spec] * 4,
            out_specs=any_spec,
            scratch_shapes=[
                pltpu.VMEM((ROWS, HID), bf16),
                pltpu.VMEM((ROWS, HID), bf16),
                pltpu.VMEM((2 * HID, QKV), bf16),
                pltpu.VMEM((2 * HID, HID), bf16),
                pltpu.VMEM((4, 8, 128), jnp.int32),
                pltpu.VMEM((ROWS, HID), bf16),
                pltpu.VMEM((ROWS, 128), bf16),
                pltpu.VMEM((SEQ, HEAD_DIM), bf16),
                pltpu.VMEM((SEQ, HEAD_DIM), bf16),
                pltpu.VMEM((12, HEAD_DIM, 256), bf16),
                pltpu.VMEM((8, HEAD_DIM, 128), bf16),
                pltpu.VMEM((SLOTS, SEQ, QB), f32),
                pltpu.VMEM((SLOTS, SEQ // GROUP, 8, QB), f32),
                pltpu.VMEM((SLOTS, 2, 8, QB), f32),
                pltpu.VMEM((TILES, QB, HEAD_DIM), bf16),
                pltpu.VMEM((TILES, QB, HEAD_DIM), bf16),
                dma((4,)),
                dma((N_SEM,)),
                dma((N_SEM,)),
                dma((TILES,)),
                dma((TILES,)),
                dma((N_BLOCK * 4,)),
            ],
            compiler_params=pltpu.CompilerParams(
                collective_id=0, has_side_effects=True, vmem_limit_bytes=67043328
            ),
        )(tokens, w_qkv, w_out, doc_ids.reshape(8, 128))

    row_spec = P(("data", "row"), "col")
    weight_spec = P("row", "col")
    return jax.shard_map(
        local_block,
        mesh=mesh,
        in_specs=(row_spec, weight_spec, weight_spec, P(("data", "row"))),
        out_specs=row_spec,
        check_vma=False,
    )
```

```python
import itertools
import math

import jax
import jax.numpy as jnp
from jax import lax
from jax.experimental import pallas as pl
from jax.experimental.pallas import tpu as pltpu
from jax.sharding import PartitionSpec as P

HEAD_DIM = 128
MESH = pl.DeviceIdType.MESH

ROWS = 1024
HID = 1024
SEQ = 4096
HEADS = 8
QKV = 1280
SHARD = 512
QB = 256
KC = 1024
GROUP = 128
N_GROUP = KC // GROUP
N_STEP = SEQ // KC
CHUNKS = ((0, 256), (256, 256), (512, 256), (768, 128), (896, 128))
W_PIECES = 4
W_ROWS = SHARD // W_PIECES
N_BLOCK = ROWS // QB
TILES = HEADS * N_BLOCK
SLOTS = 8
N_SEM = 64
CORE, XP, DIAG = 0, 1, 2
EXP_SCALE = math.log2(math.e) / math.sqrt(HEAD_DIM)
NT = (((1,), (1,)), ((), ()))
BF16_MAX = float(jnp.finfo(jnp.bfloat16).max)
F32_MIN = float(jnp.finfo(jnp.float32).min)


def kernel(
    tok_hbm, w_hbm, wo_hbm, doc_hbm, out_ref,
    tok_own, tok_peer, w_buf, wo_buf, doc_buf, q_buf, qx_buf, k_buf, kx_buf, vw_buf, vn_buf, p_buf, top_buf, state_buf,
    ctx_own, ctx_peer, loc_sem, send_sem, recv_sem, ctx_send, ctx_recv,
):
    d, y, r = lax.axis_index("data"), lax.axis_index("col"), lax.axis_index("row")
    x, core = r // 2, r % 2
    row_of = {CORE: x * 2 + (1 - core), XP: (1 - x) * 2 + core, DIAG: (1 - x) * 2 + (1 - core)}
    y_peer = (d, 1 - y, r)
    peer = {k: (d, y, v) for k, v in row_of.items()}

    barrier = pltpu.get_barrier_semaphore()
    for p in (y_peer, peer[CORE], peer[XP], peer[DIAG]):
        pl.semaphore_signal(barrier, inc=1, device_id=p, device_id_type=MESH)
    pl.semaphore_wait(barrier, 4)

    number = itertools.count()
    sent = []

    def send(src, dst, device):
        i = next(number)
        cp = pltpu.make_async_remote_copy(
            src_ref=src, dst_ref=dst, send_sem=send_sem.at[i], recv_sem=recv_sem.at[i], device_id=device, device_id_type=MESH
        )
        cp.start()
        sent.append(cp)
        return cp

    def local(src, dst, i):
        cp = pltpu.make_async_copy(src, dst, loc_sem.at[i])
        cp.start()
        return cp

    def shard(row, piece=0, size=SHARD):
        return pl.ds(pl.multiple_of(row * SHARD + piece * size, size), size)

    kv_cols, q_cols = pl.ds(HID, 2 * HEAD_DIM), pl.ds(0, HID)

    tok_in = []
    for first, size in CHUNKS:
        rows = pl.ds(first, size)
        tok_in.append(send(tok_hbm.at[rows], tok_peer.at[rows], y_peer))
    wkv_x = send(w_hbm.at[:, kv_cols], w_buf.at[shard(r), kv_cols], peer[XP])
    doc_in = [send(doc_hbm, doc_buf.at[r], peer[k]) for k in (CORE, XP, DIAG)]
    wq_x = [
        send(w_hbm.at[pl.ds(p * W_ROWS, W_ROWS), q_cols], w_buf.at[shard(r, p, W_ROWS), q_cols], peer[XP])
        for p in range(W_PIECES)
    ]
    w_core = send(w_hbm, w_buf.at[shard(r)], peer[CORE])
    wo_core = send(wo_hbm, wo_buf.at[shard(r)], peer[CORE])
    doc_local = local(doc_hbm, doc_buf.at[r], 0)
    w_local = local(w_hbm, w_buf.at[shard(r)], 1)
    tok_local = local(tok_hbm, tok_own, 2)
    wo_local = local(wo_hbm, wo_buf.at[shard(r)], 3)

    doc_local.wait()
    for cp in doc_in:
        cp.wait_recv()
    lane = lax.broadcasted_iota(jnp.int32, (128, 128), 1)

    def as_column(line):
        return jnp.transpose(jnp.broadcast_to(line, (128, 128)))

    def key_mask(place):
        def line_mask(i, carry):
            part, line, first = place(i)
            ids = as_column(doc_buf[part, pl.ds(line, 1), :])
            hit = jnp.where(lane < 3, 1 - ids, jnp.where(lane < 6, ids, 0))
            kx_buf[pl.ds(pl.multiple_of(first, 128), 128), :] = hit.astype(jnp.float32).astype(jnp.bfloat16)
            return carry

        return line_mask

    def query_mask(i, carry):
        ids = as_column(doc_buf[r, pl.ds(i, 1), :])
        hit = jnp.where(lane < 3, ids, jnp.where(lane < 6, 1 - ids, 0))
        qx_buf[pl.ds(pl.multiple_of(i * 128, 128), 128), :] = jnp.where(hit == 1, -BF16_MAX, 0.0).astype(jnp.bfloat16)
        return carry

    wide = key_mask(lambda i: (i // 6, i % 6, (i % 6) // 2 * 1024 + i // 6 * 256 + i % 2 * 128))
    lax.fori_loop(0, 24, wide, 0)
    narrow = key_mask(lambda i: (i // 2, 6 + i % 2, 3072 + i % 2 * 512 + i // 2 * 128))
    lax.fori_loop(0, 8, narrow, 0)
    lax.fori_loop(0, ROWS // 128, query_mask, 0)

    own_half = pl.ds(pl.multiple_of(y * HID, HID), HID)
    peer_half = pl.ds(pl.multiple_of((1 - y) * HID, HID), HID)

    def project(rows, cols):
        return jnp.dot(tok_own[rows, :], w_buf[own_half, cols], preferred_element_type=jnp.float32) + jnp.dot(
            tok_peer[rows, :], w_buf[peer_half, cols], preferred_element_type=jnp.float32
        )

    def forward(ref, *index):
        return send(ref.at[index], ref.at[index], peer[CORE])

    k_in, kv_core = [], [[] for _ in CHUNKS]

    def keys_of(row, c):
        first, size = CHUNKS[c]
        values = vw_buf.at[c * 4 + row] if size == 256 else vn_buf.at[(c - N_STEP + 1) * 4 + row]
        return k_buf.at[pl.ds(pl.multiple_of(first * 4 + row * size, size), size)], values

    def project_kv(c):
        tok_in[c].wait_recv()
        kv = project(pl.ds(*CHUNKS[c]), kv_cols).astype(jnp.bfloat16)
        keys, values = keys_of(r, c)
        keys[...] = kv[:, :HEAD_DIM]
        values[...] = jnp.transpose(kv[:, HEAD_DIM:])

    def send_kv(c):
        refs = keys_of(r, c)
        k_in.append([send(ref, ref, peer[XP]) for ref in refs])
        kv_core[c].extend(send(ref, ref, peer[CORE]) for ref in refs)

    def forward_kv(c):
        for ref, cp in zip(keys_of(row_of[XP], c), k_in[c]):
            cp.wait_recv()
            kv_core[c].append(send(ref, ref, peer[CORE]))

    def wait_kv(c):
        for cp in kv_core[c]:
            cp.wait_recv()

    def project_q(c):
        rows = pl.ds(c * QB, QB)

        def q_tile(n, carry):
            cols = pl.ds(pl.multiple_of(n * 256, 256), 256)
            q_buf[rows, cols] = project(rows, cols).astype(jnp.bfloat16)
            return carry

        lax.fori_loop(0, HID // 256, q_tile, 0)

    wkv_x.wait_recv()
    wkv_f = forward(w_buf, shard(row_of[XP]), kv_cols)
    w_local.wait()
    tok_local.wait()
    w_core.wait_recv()
    wkv_f.wait_recv()
    wq_f = []

    def forward_wq(p):
        wq_x[p].wait_recv()
        wq_f.append(forward(w_buf, shard(row_of[XP], p, W_ROWS), q_cols))

    half = SHARD // 2

    def send_wo(p):
        return send(wo_hbm.at[pl.ds(p * half, half)], wo_buf.at[shard(r, p, half)], peer[XP])

    def tile_of(i):
        return (
            pl.ds(pl.multiple_of((i // HEADS) * QB, QB), QB),
            pl.ds(pl.multiple_of((i % HEADS) * HEAD_DIM, HEAD_DIM), HEAD_DIM),
        )

    def over_keys(f, a):
        return f(a.reshape(a.shape[0] // 8, 8, QB), axis=0)

    def to_keys(a):
        return jnp.concatenate([a] * (GROUP // 8), axis=0)

    def score_step(i, slot, j, state):
        top, total = state
        rows, cols = tile_of(i)
        q = jnp.concatenate([q_buf[rows, cols], qx_buf[rows, :]], axis=1)
        k = jnp.concatenate([k_buf[pl.ds(j * KC, KC), :], kx_buf[pl.ds(j * KC, KC), :]], axis=1)
        s = lax.dot_general(k, q, NT, preferred_element_type=jnp.float32)
        for g in range(N_GROUP):
            part = s[g * GROUP : (g + 1) * GROUP]
            new_top = jnp.maximum(top, over_keys(jnp.max, part))
            scaled = new_top * EXP_SCALE
            top_buf[slot, j * N_GROUP + g] = scaled
            p = jnp.exp2(part * EXP_SCALE - to_keys(scaled))
            p_buf[slot, pl.ds(j * KC + g * GROUP, GROUP), :] = p
            total = total * jnp.exp2(top * EXP_SCALE - scaled) + over_keys(jnp.sum, p)
            top = new_top
        return top, total

    def value_step(slot, j, lse, acc):
        keys = pl.ds(j * KC, KC)
        factor = [to_keys(jnp.exp2(top_buf[slot, j * N_GROUP + g] - lse)) for g in range(N_GROUP)]
        weights = p_buf[slot, keys, :] * jnp.concatenate(factor, axis=0)
        parts = [vw_buf[j * 4 + i] for i in range(4)] if j + 1 < N_STEP else [vn_buf[i] for i in range(8)]
        o = jnp.dot(jnp.concatenate(parts, axis=1), weights.astype(jnp.bfloat16), preferred_element_type=jnp.float32)
        return o if acc is None else acc + o

    def ctx_copy(i):
        return pltpu.make_async_remote_copy(
            src_ref=ctx_own.at[i], dst_ref=ctx_peer.at[i], send_sem=ctx_send.at[i], recv_sem=ctx_recv.at[i],
            device_id=y_peer, device_id_type=MESH,
        )

    empty = (jnp.full((8, QB), F32_MIN, jnp.float32), jnp.zeros((8, QB), jnp.float32))

    def load_state(slot):
        return state_buf[slot, 0], state_buf[slot, 1]

    def prefetch(*steps):
        def one(slot, carry):
            state = load_state(slot) if steps[0] else empty
            for j in steps:
                state = score_step(slot, slot, j, state)
            state_buf[slot, 0], state_buf[slot, 1] = state
            return carry

        lax.fori_loop(0, SLOTS, one, 0)

    def tile(i, slot, state, nxt=None, nxt_slot=None, nxt_state=None, nxt_steps=()):
        top, total = state
        best = jnp.max(top, axis=0, keepdims=True)
        whole = jnp.sum(total * jnp.exp2((top - best) * EXP_SCALE), axis=0, keepdims=True)
        lse = best * EXP_SCALE + jnp.log2(whole)
        acc = None
        steps = list(nxt_steps)
        for j in range(N_STEP):
            if steps:
                nxt_state = score_step(nxt, nxt_slot, steps.pop(0), nxt_state)
            acc = value_step(slot, j, lse, acc)
        ctx_own[i] = jnp.transpose(acc).astype(jnp.bfloat16)
        return nxt_state

    every = range(N_STEP)

    def two_tiles(t, state):
        i = t * 2
        state = tile(i, 0, state, i + 1, 1, empty, every)
        state = tile(i + 1, 1, state, i + 2, 0, empty, every)
        ctx_copy(i).start()
        ctx_copy(i + 1).start()
        return state

    def wait_pieces(first, end):
        def wait_piece(i, carry):
            ctx_copy(i).wait_recv()
            return carry

        lax.fori_loop(first, end, wait_piece, 0)

    def heads(ref, b, first, end):
        return jnp.concatenate([ref[b * HEADS + h] for h in range(first, end)], axis=1)

    def out_rows(half_index, first, end):
        size = (end - first) * HEAD_DIM
        return pl.ds(pl.multiple_of(half_index * HID + first * HEAD_DIM, HEAD_DIM), size)

    def store_out(b, n, o):
        out_ref[pl.ds(pl.multiple_of(b * QB, QB), QB), pl.ds(pl.multiple_of(n * 256, 256), 256)] = o.astype(jnp.bfloat16)

    def out_product(b, n, end):
        cols = pl.ds(pl.multiple_of(n * 256, 256), 256)
        own = jnp.dot(heads(ctx_own, b, 0, HEADS), wo_buf[own_half, cols], preferred_element_type=jnp.float32)
        rows = out_rows(1 - y, 0, end)
        return own + jnp.dot(heads(ctx_peer, b, 0, end), wo_buf[rows, cols], preferred_element_type=jnp.float32)

    def project_out(b, carry):
        wait_pieces(b * HEADS, (b + 1) * HEADS)

        def out_tile(n, carry):
            store_out(b, n, out_product(b, n, HEADS))
            return carry

        return lax.fori_loop(0, 4, out_tile, carry)

    def project_last():
        b, most = N_BLOCK - 1, HEADS - 2
        wait_pieces(b * HEADS, b * HEADS + most)

        def first_part(n, carry):
            p_buf[2, pl.ds(pl.multiple_of(n * QB, QB), QB), :] = out_product(b, n, most)
            return carry

        lax.fori_loop(0, 4, first_part, 0)
        wait_pieces(b * HEADS + most, TILES)
        for n in range(4):
            cols, rows = pl.ds(n * 256, 256), out_rows(1 - y, most, HEADS)
            o = jnp.dot(heads(ctx_peer, b, most, HEADS), wo_buf[rows, cols], preferred_element_type=jnp.float32)
            store_out(b, n, p_buf[2, pl.ds(n * QB, QB), :] + o)

    project_kv(0)
    forward_wq(0)
    forward_wq(1)
    project_kv(1)
    forward_wq(2)
    forward_wq(3)
    send_kv(0)
    send_kv(1)
    for cp in wq_f:
        cp.wait_recv()
    project_q(0)
    project_q(1)
    project_kv(2)
    send_kv(2)
    forward_kv(0)
    forward_kv(1)
    project_q(2)
    for c in (0, 1):
        wait_kv(c)
    prefetch(0, 1)
    project_kv(3)
    send_kv(3)
    forward_kv(2)
    project_kv(4)
    send_kv(4)
    wo_x = [send_wo(0), send_wo(1)]
    wait_kv(2)
    prefetch(2)
    forward_kv(3)
    forward_kv(4)
    for c in (3, 4):
        wait_kv(c)

    last = N_STEP - 1
    state = score_step(0, 0, last, load_state(0))
    for i in range(SLOTS):
        if i == 0:
            tile(0, 0, state)
            ctx_copy(0).start()
            state = score_step(1, 1, last, load_state(1))
        elif i + 1 < SLOTS:
            state = tile(i, i, state, i + 1, i + 1, load_state(i + 1), (last,))
        else:
            state = tile(i, i, state, i + 1, 0, empty, every)
        if i % 2:
            for n in range(max(i - 1, 1), i + 1):
                ctx_copy(n).start()

    pairs = HEADS // 2
    state = lax.fori_loop(pairs, 2 * pairs, two_tiles, state)
    wo_f = []

    def forward_wo(p):
        wo_x[p].wait_recv()
        wo_f.append(forward(wo_buf, shard(row_of[XP], p, half)))

    forward_wo(0)
    project_q(3)
    state = lax.fori_loop(2 * pairs, 3 * pairs, two_tiles, state)
    forward_wo(1)
    state = lax.fori_loop(3 * pairs, 4 * pairs - 1, two_tiles, state)
    state = tile(TILES - 2, 0, state, TILES - 1, 1, empty, every)
    ctx_copy(TILES - 2).start()
    tile(TILES - 1, 1, state)
    ctx_copy(TILES - 1).start()

    wo_local.wait()
    wo_core.wait_recv()
    for cp in wo_f:
        cp.wait_recv()

    lax.fori_loop(0, N_BLOCK - 1, project_out, 0)
    project_last()

    for cp in sent:
        cp.wait_send()

    def wait_sent(i, carry):
        ctx_copy(i).wait_send()
        return carry

    lax.fori_loop(0, TILES, wait_sent, 0)
    assert next(number) <= N_SEM


def solution(mesh):
    def local_block(tokens, w_qkv, w_out, doc_ids):
        bf16, f32 = jnp.bfloat16, jnp.float32
        dma = pltpu.SemaphoreType.DMA
        any_spec = pl.BlockSpec(memory_space=pl.ANY)
        return pl.pallas_call(
            kernel,
            out_shape=pltpu.VMEM(tokens.shape, bf16),
            in_specs=[any_spec] * 4,
            out_specs=pl.BlockSpec(memory_space=pltpu.VMEM),
            scratch_shapes=[
                pltpu.VMEM((ROWS, HID), bf16),
                pltpu.VMEM((ROWS, HID), bf16),
                pltpu.VMEM((2 * HID, QKV), bf16),
                pltpu.VMEM((2 * HID, HID), bf16),
                pltpu.VMEM((4, 8, 128), jnp.int32),
                pltpu.VMEM((ROWS, HID), bf16),
                pltpu.VMEM((ROWS, 128), bf16),
                pltpu.VMEM((SEQ, HEAD_DIM), bf16),
                pltpu.VMEM((SEQ, HEAD_DIM), bf16),
                pltpu.VMEM((12, HEAD_DIM, 256), bf16),
                pltpu.VMEM((8, HEAD_DIM, 128), bf16),
                pltpu.VMEM((SLOTS, SEQ, QB), f32),
                pltpu.VMEM((SLOTS, SEQ // GROUP, 8, QB), f32),
                pltpu.VMEM((SLOTS, 2, 8, QB), f32),
                pltpu.VMEM((TILES, QB, HEAD_DIM), bf16),
                pltpu.VMEM((TILES, QB, HEAD_DIM), bf16),
                dma((4,)),
                dma((N_SEM,)),
                dma((N_SEM,)),
                dma((TILES,)),
                dma((TILES,)),
            ],
            compiler_params=pltpu.CompilerParams(
                collective_id=0, has_side_effects=True, vmem_limit_bytes=59 * 1024 * 1024
            ),
        )(tokens, w_qkv, w_out, doc_ids.reshape(8, 128))

    row_spec = P(("data", "row"), "col")
    weight_spec = P("row", "col")
    return jax.shard_map(
        local_block,
        mesh=mesh,
        in_specs=(row_spec, weight_spec, weight_spec, P(("data", "row"))),
        out_specs=row_spec,
        check_vma=False,
    )
```

```python
import itertools
import math

import jax
import jax.numpy as jnp
from jax import lax
from jax.experimental import pallas as pl
from jax.experimental.pallas import tpu as pltpu
from jax.sharding import PartitionSpec as P

HEAD_DIM = 128
MESH = pl.DeviceIdType.MESH

ROWS = 1024
HID = 1024
SEQ = 4096
HEADS = 8
QKV = 1280
SHARD = 512
QB = 256
KC = 1024
GROUP = 128
N_GROUP = KC // GROUP
N_STEP = SEQ // KC
CHUNKS = ((0, 256), (256, 256), (512, 256), (768, 128), (896, 64), (960, 64))
W_PIECES = 4
W_ROWS = SHARD // W_PIECES
N_BLOCK = ROWS // QB
TILES = HEADS * N_BLOCK
SLOTS = 8
N_SEM = 72
CORE, XP, DIAG = 0, 1, 2
EXP_SCALE = math.log2(math.e) / math.sqrt(HEAD_DIM)
NT = (((1,), (1,)), ((), ()))
BF16_MAX = float(jnp.finfo(jnp.bfloat16).max)
F32_MIN = float(jnp.finfo(jnp.float32).min)


def kernel(
    tok_hbm, w_hbm, wo_hbm, doc_hbm, out_ref,
    tok_own, tok_peer, w_buf, wo_buf, doc_buf, q_buf, qx_buf, k_buf, kx_buf, vw_buf, vn_buf, vr_buf, vl_buf, p_buf, top_buf, state_buf,
    ctx_own, ctx_peer, loc_sem, send_sem, recv_sem, ctx_send, ctx_recv,
):
    d, y, r = lax.axis_index("data"), lax.axis_index("col"), lax.axis_index("row")
    x, core = r // 2, r % 2
    row_of = {CORE: x * 2 + (1 - core), XP: (1 - x) * 2 + core, DIAG: (1 - x) * 2 + (1 - core)}
    y_peer = (d, 1 - y, r)
    peer = {k: (d, y, v) for k, v in row_of.items()}

    barrier = pltpu.get_barrier_semaphore()
    for p in (y_peer, peer[CORE], peer[XP], peer[DIAG]):
        pl.semaphore_signal(barrier, inc=1, device_id=p, device_id_type=MESH)
    pl.semaphore_wait(barrier, 4)

    number = itertools.count()
    sent = []

    def send(src, dst, device):
        i = next(number)
        cp = pltpu.make_async_remote_copy(
            src_ref=src, dst_ref=dst, send_sem=send_sem.at[i], recv_sem=recv_sem.at[i], device_id=device, device_id_type=MESH
        )
        cp.start()
        sent.append(cp)
        return cp

    def local(src, dst, i):
        cp = pltpu.make_async_copy(src, dst, loc_sem.at[i])
        cp.start()
        return cp

    def shard(row, piece=0, size=SHARD):
        return pl.ds(pl.multiple_of(row * SHARD + piece * size, size), size)

    kv_cols, q_cols = pl.ds(HID, 2 * HEAD_DIM), pl.ds(0, HID)

    tok_in = []
    for first, size in CHUNKS:
        rows = pl.ds(first, size)
        tok_in.append(send(tok_hbm.at[rows], tok_peer.at[rows], y_peer))
    wkv_x = send(w_hbm.at[:, kv_cols], w_buf.at[shard(r), kv_cols], peer[XP])
    doc_in = [send(doc_hbm, doc_buf.at[r], peer[k]) for k in (CORE, XP, DIAG)]
    wq_x = [
        send(w_hbm.at[pl.ds(p * W_ROWS, W_ROWS), q_cols], w_buf.at[shard(r, p, W_ROWS), q_cols], peer[XP])
        for p in range(W_PIECES)
    ]
    w_core = send(w_hbm, w_buf.at[shard(r)], peer[CORE])
    wo_core = send(wo_hbm, wo_buf.at[shard(r)], peer[CORE])
    doc_local = local(doc_hbm, doc_buf.at[r], 0)
    w_local = local(w_hbm, w_buf.at[shard(r)], 1)
    tok_local = local(tok_hbm, tok_own, 2)
    wo_local = local(wo_hbm, wo_buf.at[shard(r)], 3)

    doc_local.wait()
    for cp in doc_in:
        cp.wait_recv()
    lane = lax.broadcasted_iota(jnp.int32, (128, 128), 1)

    def as_column(line):
        return jnp.transpose(jnp.broadcast_to(line, (128, 128)))

    def key_mask(place):
        def line_mask(i, carry):
            part, line, first = place(i)
            ids = as_column(doc_buf[part, pl.ds(line, 1), :])
            hit = jnp.where(lane < 3, 1 - ids, jnp.where(lane < 6, ids, 0)).astype(jnp.float32).astype(jnp.bfloat16)
            for n, at in enumerate(first):
                size = 128 // len(first)
                kx_buf[pl.ds(pl.multiple_of(at, size), size), :] = hit[n * size : (n + 1) * size]
            return carry

        return line_mask

    def query_mask(i, carry):
        ids = as_column(doc_buf[r, pl.ds(i, 1), :])
        hit = jnp.where(lane < 3, ids, jnp.where(lane < 6, 1 - ids, 0))
        qx_buf[pl.ds(pl.multiple_of(i * 128, 128), 128), :] = jnp.where(hit == 1, -BF16_MAX, 0.0).astype(jnp.bfloat16)
        return carry

    wide = key_mask(lambda i: (i // 6, i % 6, [(i % 6) // 2 * 1024 + i // 6 * 256 + i % 2 * 128]))
    lax.fori_loop(0, 24, wide, 0)
    lax.fori_loop(0, 4, key_mask(lambda i: (i, 6, [3072 + i * 128])), 0)
    lax.fori_loop(0, 4, key_mask(lambda i: (i, 7, [3584 + i * 64, 3840 + i * 64])), 0)
    lax.fori_loop(0, ROWS // 128, query_mask, 0)

    own_half = pl.ds(pl.multiple_of(y * HID, HID), HID)
    peer_half = pl.ds(pl.multiple_of((1 - y) * HID, HID), HID)

    def project(rows, cols):
        return jnp.dot(tok_own[rows, :], w_buf[own_half, cols], preferred_element_type=jnp.float32) + jnp.dot(
            tok_peer[rows, :], w_buf[peer_half, cols], preferred_element_type=jnp.float32
        )

    def forward(ref, *index):
        return send(ref.at[index], ref.at[index], peer[CORE])

    k_in, kv_core = [], [[] for _ in CHUNKS]

    def keys_of(row, c):
        first, size = CHUNKS[c]
        if size == 64:
            values = vr_buf.at[c - 4, pl.ds(pl.multiple_of(row * size, size), size)]
        else:
            values = vw_buf.at[c * 4 + row] if size == 256 else vn_buf.at[row]
        return k_buf.at[pl.ds(pl.multiple_of(first * 4 + row * size, size), size)], values

    def project_kv(c):
        tok_in[c].wait_recv()
        kv = project(pl.ds(*CHUNKS[c]), kv_cols).astype(jnp.bfloat16)
        keys, values = keys_of(r, c)
        keys[...] = kv[:, :HEAD_DIM]
        values[...] = kv[:, HEAD_DIM:] if c >= 4 else jnp.transpose(kv[:, HEAD_DIM:])

    def send_kv(c):
        refs = keys_of(r, c)
        if c >= 4:
            kv_core[c] += [send(ref, ref, peer[k]) for k in (XP, DIAG, CORE) for ref in refs]
            return
        k_in.append([send(ref, ref, peer[XP]) for ref in refs])
        kv_core[c].extend(send(ref, ref, peer[CORE]) for ref in refs)

    def forward_kv(c):
        for ref, cp in zip(keys_of(row_of[XP], c), k_in[c]):
            cp.wait_recv()
            kv_core[c].append(send(ref, ref, peer[CORE]))

    def wait_kv(c):
        for cp in kv_core[c]:
            cp.wait_recv()

    def project_q(c):
        rows = pl.ds(c * QB, QB)

        def q_tile(n, carry):
            cols = pl.ds(pl.multiple_of(n * 256, 256), 256)
            q_buf[rows, cols] = project(rows, cols).astype(jnp.bfloat16)
            return carry

        lax.fori_loop(0, HID // 256, q_tile, 0)

    wkv_x.wait_recv()
    wkv_f = forward(w_buf, shard(row_of[XP]), kv_cols)
    w_local.wait()
    tok_local.wait()
    w_core.wait_recv()
    wkv_f.wait_recv()
    wq_f = []

    def forward_wq(p):
        wq_x[p].wait_recv()
        wq_f.append(forward(w_buf, shard(row_of[XP], p, W_ROWS), q_cols))

    half = SHARD // 2

    def send_wo(p):
        return send(wo_hbm.at[pl.ds(p * half, half)], wo_buf.at[shard(r, p, half)], peer[XP])

    def tile_of(i):
        return (
            pl.ds(pl.multiple_of((i // HEADS) * QB, QB), QB),
            pl.ds(pl.multiple_of((i % HEADS) * HEAD_DIM, HEAD_DIM), HEAD_DIM),
        )

    def over_keys(f, a):
        return f(a.reshape(a.shape[0] // 8, 8, QB), axis=0)

    def to_keys(a):
        return jnp.concatenate([a] * (GROUP // 8), axis=0)

    def score_step(i, slot, j, state):
        top, total = state
        rows, cols = tile_of(i)
        q = jnp.concatenate([q_buf[rows, cols], qx_buf[rows, :]], axis=1)
        k = jnp.concatenate([k_buf[pl.ds(j * KC, KC), :], kx_buf[pl.ds(j * KC, KC), :]], axis=1)
        s = lax.dot_general(k, q, NT, preferred_element_type=jnp.float32)
        for g in range(N_GROUP):
            part = s[g * GROUP : (g + 1) * GROUP]
            new_top = jnp.maximum(top, over_keys(jnp.max, part))
            scaled = new_top * EXP_SCALE
            top_buf[slot, j * N_GROUP + g] = scaled
            p = jnp.exp2(part * EXP_SCALE - to_keys(scaled))
            p_buf[slot, pl.ds(j * KC + g * GROUP, GROUP), :] = p
            total = total * jnp.exp2(top * EXP_SCALE - scaled) + over_keys(jnp.sum, p)
            top = new_top
        return top, total

    def value_step(slot, j, lse, acc):
        keys = pl.ds(j * KC, KC)
        factor = [to_keys(jnp.exp2(top_buf[slot, j * N_GROUP + g] - lse)) for g in range(N_GROUP)]
        weights = p_buf[slot, keys, :] * jnp.concatenate(factor, axis=0)
        parts = [vw_buf[j * 4 + i] for i in range(4)] if j + 1 < N_STEP else [*(vn_buf[i] for i in range(4)), vl_buf[0], vl_buf[1]]
        o = jnp.dot(jnp.concatenate(parts, axis=1), weights.astype(jnp.bfloat16), preferred_element_type=jnp.float32)
        return o if acc is None else acc + o

    def ctx_copy(i):
        return pltpu.make_async_remote_copy(
            src_ref=ctx_own.at[i], dst_ref=ctx_peer.at[i], send_sem=ctx_send.at[i], recv_sem=ctx_recv.at[i],
            device_id=y_peer, device_id_type=MESH,
        )

    empty = (jnp.full((8, QB), F32_MIN, jnp.float32), jnp.zeros((8, QB), jnp.float32))

    def load_state(slot):
        return state_buf[slot, 0], state_buf[slot, 1]

    def prefetch(*steps):
        def one(slot, carry):
            state = load_state(slot) if steps[0] else empty
            for j in steps:
                state = score_step(slot, slot, j, state)
            state_buf[slot, 0], state_buf[slot, 1] = state
            return carry

        lax.fori_loop(0, SLOTS, one, 0)

    def tile(i, slot, state, nxt=None, nxt_slot=None, nxt_state=None, nxt_steps=()):
        top, total = state
        best = jnp.max(top, axis=0, keepdims=True)
        whole = jnp.sum(total * jnp.exp2((top - best) * EXP_SCALE), axis=0, keepdims=True)
        lse = best * EXP_SCALE + jnp.log2(whole)
        acc = None
        steps = list(nxt_steps)
        for j in range(N_STEP):
            if steps:
                nxt_state = score_step(nxt, nxt_slot, steps.pop(0), nxt_state)
            acc = value_step(slot, j, lse, acc)
        ctx_own[i] = jnp.transpose(acc).astype(jnp.bfloat16)
        return nxt_state

    every = range(N_STEP)

    def two_tiles(t, state):
        i = t * 2
        state = tile(i, 0, state, i + 1, 1, empty, every)
        state = tile(i + 1, 1, state, i + 2, 0, empty, every)
        ctx_copy(i).start()
        ctx_copy(i + 1).start()
        return state

    def wait_pieces(first, end):
        def wait_piece(i, carry):
            ctx_copy(i).wait_recv()
            return carry

        lax.fori_loop(first, end, wait_piece, 0)

    def heads(ref, b, first, end):
        return jnp.concatenate([ref[b * HEADS + h] for h in range(first, end)], axis=1)

    def out_rows(half_index, first, end):
        size = (end - first) * HEAD_DIM
        return pl.ds(pl.multiple_of(half_index * HID + first * HEAD_DIM, HEAD_DIM), size)

    def store_out(b, n, o):
        out_ref[pl.ds(pl.multiple_of(b * QB, QB), QB), pl.ds(pl.multiple_of(n * 256, 256), 256)] = o.astype(jnp.bfloat16)

    def out_product(b, n, end):
        cols = pl.ds(pl.multiple_of(n * 256, 256), 256)
        own = jnp.dot(heads(ctx_own, b, 0, HEADS), wo_buf[own_half, cols], preferred_element_type=jnp.float32)
        rows = out_rows(1 - y, 0, end)
        return own + jnp.dot(heads(ctx_peer, b, 0, end), wo_buf[rows, cols], preferred_element_type=jnp.float32)

    def project_out(b, carry):
        wait_pieces(b * HEADS, (b + 1) * HEADS)

        def out_tile(n, carry):
            store_out(b, n, out_product(b, n, HEADS))
            return carry

        return lax.fori_loop(0, 4, out_tile, carry)

    def project_last():
        b, most = N_BLOCK - 1, HEADS - 2
        wait_pieces(b * HEADS, b * HEADS + most)

        def first_part(n, carry):
            p_buf[2, pl.ds(pl.multiple_of(n * QB, QB), QB), :] = out_product(b, n, most)
            return carry

        lax.fori_loop(0, 4, first_part, 0)
        wait_pieces(b * HEADS + most, TILES)
        for n in range(4):
            cols, rows = pl.ds(n * 256, 256), out_rows(1 - y, most, HEADS)
            o = jnp.dot(heads(ctx_peer, b, most, HEADS), wo_buf[rows, cols], preferred_element_type=jnp.float32)
            store_out(b, n, p_buf[2, pl.ds(n * QB, QB), :] + o)

    project_kv(0)
    forward_wq(0)
    forward_wq(1)
    project_kv(1)
    forward_wq(2)
    forward_wq(3)
    send_kv(0)
    send_kv(1)
    for cp in wq_f:
        cp.wait_recv()
    project_q(0)
    project_q(1)
    project_kv(2)
    send_kv(2)
    forward_kv(0)
    forward_kv(1)
    project_q(2)
    for c in (0, 1):
        wait_kv(c)
    prefetch(0, 1)
    project_kv(3)
    send_kv(3)
    forward_kv(2)
    project_kv(4)
    send_kv(4)
    project_kv(5)
    send_kv(5)
    wo_x = [send_wo(0), send_wo(1)]
    wait_kv(2)
    forward_kv(3)
    prefetch(2)
    for c in (3, 4, 5):
        wait_kv(c)
        if c >= 4:
            vl_buf[c - 4] = jnp.transpose(vr_buf[c - 4])

    last = N_STEP - 1
    state = score_step(0, 0, last, load_state(0))
    for i in range(SLOTS):
        if i == 0:
            tile(0, 0, state)
            ctx_copy(0).start()
            state = score_step(1, 1, last, load_state(1))
        elif i + 1 < SLOTS:
            state = tile(i, i, state, i + 1, i + 1, load_state(i + 1), (last,))
        else:
            state = tile(i, i, state, i + 1, 0, empty, every)
        if i % 2:
            for n in range(max(i - 1, 1), i + 1):
                ctx_copy(n).start()

    pairs = HEADS // 2
    state = lax.fori_loop(pairs, 2 * pairs, two_tiles, state)
    wo_f = []

    def forward_wo(p):
        wo_x[p].wait_recv()
        wo_f.append(forward(wo_buf, shard(row_of[XP], p, half)))

    forward_wo(0)
    project_q(3)
    state = lax.fori_loop(2 * pairs, 3 * pairs, two_tiles, state)
    forward_wo(1)
    state = lax.fori_loop(3 * pairs, 4 * pairs - 1, two_tiles, state)
    state = tile(TILES - 2, 0, state, TILES - 1, 1, empty, every)
    ctx_copy(TILES - 2).start()
    tile(TILES - 1, 1, state)
    ctx_copy(TILES - 1).start()

    wo_local.wait()
    wo_core.wait_recv()
    for cp in wo_f:
        cp.wait_recv()

    lax.fori_loop(0, N_BLOCK - 1, project_out, 0)
    project_last()

    for cp in sent:
        cp.wait_send()

    def wait_sent(i, carry):
        ctx_copy(i).wait_send()
        return carry

    lax.fori_loop(0, TILES, wait_sent, 0)
    assert next(number) <= N_SEM


def solution(mesh):
    def local_block(tokens, w_qkv, w_out, doc_ids):
        bf16, f32 = jnp.bfloat16, jnp.float32
        dma = pltpu.SemaphoreType.DMA
        any_spec = pl.BlockSpec(memory_space=pl.ANY)
        return pl.pallas_call(
            kernel,
            out_shape=pltpu.VMEM(tokens.shape, bf16),
            in_specs=[any_spec] * 4,
            out_specs=pl.BlockSpec(memory_space=pltpu.VMEM),
            scratch_shapes=[
                pltpu.VMEM((ROWS, HID), bf16),
                pltpu.VMEM((ROWS, HID), bf16),
                pltpu.VMEM((2 * HID, QKV), bf16),
                pltpu.VMEM((2 * HID, HID), bf16),
                pltpu.VMEM((4, 8, 128), jnp.int32),
                pltpu.VMEM((ROWS, HID), bf16),
                pltpu.VMEM((ROWS, 128), bf16),
                pltpu.VMEM((SEQ, HEAD_DIM), bf16),
                pltpu.VMEM((SEQ, HEAD_DIM), bf16),
                pltpu.VMEM((12, HEAD_DIM, 256), bf16),
                pltpu.VMEM((4, HEAD_DIM, 128), bf16),
                pltpu.VMEM((2, 256, HEAD_DIM), bf16),
                pltpu.VMEM((2, HEAD_DIM, 256), bf16),
                pltpu.VMEM((SLOTS, SEQ, QB), f32),
                pltpu.VMEM((SLOTS, SEQ // GROUP, 8, QB), f32),
                pltpu.VMEM((SLOTS, 2, 8, QB), f32),
                pltpu.VMEM((TILES, QB, HEAD_DIM), bf16),
                pltpu.VMEM((TILES, QB, HEAD_DIM), bf16),
                dma((4,)),
                dma((N_SEM,)),
                dma((N_SEM,)),
                dma((TILES,)),
                dma((TILES,)),
            ],
            compiler_params=pltpu.CompilerParams(
                collective_id=0, has_side_effects=True, vmem_limit_bytes=61 * 1024 * 1024
            ),
        )(tokens, w_qkv, w_out, doc_ids.reshape(8, 128))

    row_spec = P(("data", "row"), "col")
    weight_spec = P("row", "col")
    return jax.shard_map(
        local_block,
        mesh=mesh,
        in_specs=(row_spec, weight_spec, weight_spec, P(("data", "row"))),
        out_specs=row_spec,
        check_vma=False,
    )
```

```python
import itertools
import math

import jax
import jax.numpy as jnp
from jax import lax
from jax.experimental import pallas as pl
from jax.experimental.pallas import tpu as pltpu
from jax.sharding import PartitionSpec as P

HEAD_DIM = 128
MESH = pl.DeviceIdType.MESH

ROWS = 1024
HID = 1024
SEQ = 4096
HEADS = 8
QKV = 1280
SHARD = 512
QB = 256
KC = 1024
GROUP = 128
N_GROUP = KC // GROUP
N_STEP = SEQ // KC
CHUNKS = ((0, 256), (256, 256), (512, 256), (768, 128), (896, 64), (960, 64))
W_PIECES = 4
W_ROWS = SHARD // W_PIECES
N_BLOCK = ROWS // QB
TILES = HEADS * N_BLOCK
SLOTS = 8
N_SEM = 72
CORE, XP, DIAG = 0, 1, 2
EXP_SCALE = math.log2(math.e) / math.sqrt(HEAD_DIM)
NT = (((1,), (1,)), ((), ()))
BF16_MAX = float(jnp.finfo(jnp.bfloat16).max)
F32_MIN = float(jnp.finfo(jnp.float32).min)


def kernel(
    tok_hbm, w_hbm, wo_hbm, doc_hbm, out_ref,
    tok_own, tok_peer, w_buf, wo_buf, doc_buf, q_buf, qx_buf, k_buf, kx_buf, vw_buf, vn_buf, vr_buf, vl_buf, p_buf, top_buf, state_buf,
    ctx_own, ctx_peer, loc_sem, send_sem, recv_sem, ctx_send, ctx_recv,
):
    d, y, r = lax.axis_index("data"), lax.axis_index("col"), lax.axis_index("row")
    x, core = r // 2, r % 2
    row_of = {CORE: x * 2 + (1 - core), XP: (1 - x) * 2 + core, DIAG: (1 - x) * 2 + (1 - core)}
    y_peer = (d, 1 - y, r)
    peer = {k: (d, y, v) for k, v in row_of.items()}

    barrier = pltpu.get_barrier_semaphore()
    for p in (y_peer, peer[CORE], peer[XP], peer[DIAG]):
        pl.semaphore_signal(barrier, inc=1, device_id=p, device_id_type=MESH)
    pl.semaphore_wait(barrier, 4)

    number = itertools.count()
    sent = []

    def send(src, dst, device):
        i = next(number)
        cp = pltpu.make_async_remote_copy(
            src_ref=src, dst_ref=dst, send_sem=send_sem.at[i], recv_sem=recv_sem.at[i], device_id=device, device_id_type=MESH
        )
        cp.start()
        sent.append(cp)
        return cp

    def local(src, dst, i):
        cp = pltpu.make_async_copy(src, dst, loc_sem.at[i])
        cp.start()
        return cp

    def shard(row, piece=0, size=SHARD):
        return pl.ds(pl.multiple_of(row * SHARD + piece * size, size), size)

    kv_cols, q_cols = pl.ds(HID, 2 * HEAD_DIM), pl.ds(0, HID)

    tok_in = []
    for first, size in CHUNKS:
        rows = pl.ds(first, size)
        tok_in.append(send(tok_hbm.at[rows], tok_peer.at[rows], y_peer))
    wkv_x = send(w_hbm.at[:, kv_cols], w_buf.at[shard(r), kv_cols], peer[XP])
    doc_in = [send(doc_hbm, doc_buf.at[r], peer[k]) for k in (CORE, XP, DIAG)]
    wq_x = [
        send(w_hbm.at[pl.ds(p * W_ROWS, W_ROWS), q_cols], w_buf.at[shard(r, p, W_ROWS), q_cols], peer[XP])
        for p in range(W_PIECES)
    ]
    w_core = send(w_hbm, w_buf.at[shard(r)], peer[CORE])
    wo_core = send(wo_hbm, wo_buf.at[shard(r)], peer[CORE])
    doc_local = local(doc_hbm, doc_buf.at[r], 0)
    w_local = local(w_hbm, w_buf.at[shard(r)], 1)
    tok_local = local(tok_hbm, tok_own, 2)
    wo_local = local(wo_hbm, wo_buf.at[shard(r)], 3)

    doc_local.wait()
    for cp in doc_in:
        cp.wait_recv()
    lane = lax.broadcasted_iota(jnp.int32, (128, 128), 1)

    def as_column(line):
        return jnp.transpose(jnp.broadcast_to(line, (128, 128)))

    def key_mask(place):
        def line_mask(i, carry):
            part, line, first = place(i)
            ids = as_column(doc_buf[part, pl.ds(line, 1), :])
            hit = jnp.where(lane < 3, 1 - ids, jnp.where(lane < 6, ids, 0)).astype(jnp.float32).astype(jnp.bfloat16)
            for n, at in enumerate(first):
                size = 128 // len(first)
                kx_buf[pl.ds(pl.multiple_of(at, size), size), :] = hit[n * size : (n + 1) * size]
            return carry

        return line_mask

    def query_mask(i, carry):
        ids = as_column(doc_buf[r, pl.ds(i, 1), :])
        hit = jnp.where(lane < 3, ids, jnp.where(lane < 6, 1 - ids, 0))
        qx_buf[pl.ds(pl.multiple_of(i * 128, 128), 128), :] = jnp.where(hit == 1, -BF16_MAX, 0.0).astype(jnp.bfloat16)
        return carry

    wide = key_mask(lambda i: (i // 6, i % 6, [(i % 6) // 2 * 1024 + i // 6 * 256 + i % 2 * 128]))
    lax.fori_loop(0, 24, wide, 0)
    lax.fori_loop(0, 4, key_mask(lambda i: (i, 6, [3072 + i * 128])), 0)
    lax.fori_loop(0, 4, key_mask(lambda i: (i, 7, [3584 + i * 64, 3840 + i * 64])), 0)
    lax.fori_loop(0, ROWS // 128, query_mask, 0)

    own_half = pl.ds(pl.multiple_of(y * HID, HID), HID)
    peer_half = pl.ds(pl.multiple_of((1 - y) * HID, HID), HID)

    def project(rows, cols):
        return jnp.dot(tok_own[rows, :], w_buf[own_half, cols], preferred_element_type=jnp.float32) + jnp.dot(
            tok_peer[rows, :], w_buf[peer_half, cols], preferred_element_type=jnp.float32
        )

    def forward(ref, *index):
        return send(ref.at[index], ref.at[index], peer[CORE])

    k_in, kv_core = [], [[] for _ in CHUNKS]

    def keys_of(row, c):
        first, size = CHUNKS[c]
        if size == 64:
            values = vr_buf.at[c - 4, pl.ds(pl.multiple_of(row * size, size), size)]
        else:
            values = vw_buf.at[c * 4 + row] if size == 256 else vn_buf.at[row]
        return k_buf.at[pl.ds(pl.multiple_of(first * 4 + row * size, size), size)], values

    def project_kv(c):
        tok_in[c].wait_recv()
        kv = project(pl.ds(*CHUNKS[c]), kv_cols).astype(jnp.bfloat16)
        keys, values = keys_of(r, c)
        keys[...] = kv[:, :HEAD_DIM]
        values[...] = kv[:, HEAD_DIM:] if c >= 4 else jnp.transpose(kv[:, HEAD_DIM:])

    def send_kv(c):
        refs = keys_of(r, c)
        if c >= 4:
            kv_core[c] += [send(ref, ref, peer[k]) for k in (XP, DIAG, CORE) for ref in refs]
            return
        k_in.append([send(ref, ref, peer[XP]) for ref in refs])
        kv_core[c].extend(send(ref, ref, peer[CORE]) for ref in refs)

    def forward_kv(c):
        for ref, cp in zip(keys_of(row_of[XP], c), k_in[c]):
            cp.wait_recv()
            kv_core[c].append(send(ref, ref, peer[CORE]))

    def wait_kv(c):
        for cp in kv_core[c]:
            cp.wait_recv()

    def project_q(c):
        rows = pl.ds(c * QB, QB)

        def q_tile(n, carry):
            cols = pl.ds(pl.multiple_of(n * 256, 256), 256)
            q_buf[rows, cols] = project(rows, cols).astype(jnp.bfloat16)
            return carry

        lax.fori_loop(0, HID // 256, q_tile, 0)

    wkv_x.wait_recv()
    wkv_f = forward(w_buf, shard(row_of[XP]), kv_cols)
    w_local.wait()
    tok_local.wait()
    w_core.wait_recv()
    wkv_f.wait_recv()
    wq_f = []

    def forward_wq(p):
        wq_x[p].wait_recv()
        wq_f.append(forward(w_buf, shard(row_of[XP], p, W_ROWS), q_cols))

    half = SHARD // 2

    def send_wo(p):
        return send(wo_hbm.at[pl.ds(p * half, half)], wo_buf.at[shard(r, p, half)], peer[XP])

    def tile_of(i):
        return (
            pl.ds(pl.multiple_of((i // HEADS) * QB, QB), QB),
            pl.ds(pl.multiple_of((i % HEADS) * HEAD_DIM, HEAD_DIM), HEAD_DIM),
        )

    def over_keys(f, a):
        return f(a.reshape(a.shape[0] // 8, 8, QB), axis=0)

    def to_keys(a):
        return jnp.concatenate([a] * (GROUP // 8), axis=0)

    def score_step(i, slot, j, state):
        top, total = state
        rows, cols = tile_of(i)
        q = jnp.concatenate([q_buf[rows, cols], qx_buf[rows, :]], axis=1)
        k = jnp.concatenate([k_buf[pl.ds(j * KC, KC), :], kx_buf[pl.ds(j * KC, KC), :]], axis=1)
        s = lax.dot_general(k, q, NT, preferred_element_type=jnp.float32)
        for g in range(N_GROUP):
            part = s[g * GROUP : (g + 1) * GROUP]
            new_top = jnp.maximum(top, over_keys(jnp.max, part))
            scaled = new_top * EXP_SCALE
            top_buf[slot, j * N_GROUP + g] = scaled
            p = jnp.exp2(part * EXP_SCALE - to_keys(scaled))
            p_buf[slot, pl.ds(j * KC + g * GROUP, GROUP), :] = p
            total = total * jnp.exp2(top * EXP_SCALE - scaled) + over_keys(jnp.sum, p)
            top = new_top
        return top, total

    def value_step(slot, j, lse, acc):
        keys = pl.ds(j * KC, KC)
        factor = [to_keys(jnp.exp2(top_buf[slot, j * N_GROUP + g] - lse)) for g in range(N_GROUP)]
        weights = p_buf[slot, keys, :] * jnp.concatenate(factor, axis=0)
        parts = [vw_buf[j * 4 + i] for i in range(4)] if j + 1 < N_STEP else [*(vn_buf[i] for i in range(4)), vl_buf[0], vl_buf[1]]
        o = jnp.dot(jnp.concatenate(parts, axis=1), weights.astype(jnp.bfloat16), preferred_element_type=jnp.float32)
        return o if acc is None else acc + o

    def ctx_copy(i):
        return pltpu.make_async_remote_copy(
            src_ref=ctx_own.at[i], dst_ref=ctx_peer.at[i], send_sem=ctx_send.at[i], recv_sem=ctx_recv.at[i],
            device_id=y_peer, device_id_type=MESH,
        )

    empty = (jnp.full((8, QB), F32_MIN, jnp.float32), jnp.zeros((8, QB), jnp.float32))

    def load_state(slot):
        return state_buf[slot, 0], state_buf[slot, 1]

    def prefetch(*steps):
        def one(slot, carry):
            state = load_state(slot) if steps[0] else empty
            for j in steps:
                state = score_step(slot, slot, j, state)
            state_buf[slot, 0], state_buf[slot, 1] = state
            return carry

        lax.fori_loop(0, SLOTS, one, 0)

    def tile(i, slot, state, nxt=None, nxt_slot=None, nxt_state=None, nxt_steps=()):
        top, total = state
        best = jnp.max(top, axis=0, keepdims=True)
        whole = jnp.sum(total * jnp.exp2((top - best) * EXP_SCALE), axis=0, keepdims=True)
        lse = best * EXP_SCALE + jnp.log2(whole)
        acc = None
        steps = list(nxt_steps)
        for j in range(N_STEP):
            if steps:
                nxt_state = score_step(nxt, nxt_slot, steps.pop(0), nxt_state)
            acc = value_step(slot, j, lse, acc)
        ctx_own[i] = jnp.transpose(acc).astype(jnp.bfloat16)
        return nxt_state

    every = range(N_STEP)

    def two_tiles(t, state):
        i = t * 2
        state = tile(i, 0, state, i + 1, 1, empty, every)
        state = tile(i + 1, 1, state, i + 2, 0, empty, every)
        ctx_copy(i).start()
        ctx_copy(i + 1).start()
        return state

    def wait_pieces(first, end):
        def wait_piece(i, carry):
            ctx_copy(i).wait_recv()
            return carry

        lax.fori_loop(first, end, wait_piece, 0)

    def heads(ref, b, first, end):
        return jnp.concatenate([ref[b * HEADS + h] for h in range(first, end)], axis=1)

    def out_rows(half_index, first, end):
        size = (end - first) * HEAD_DIM
        return pl.ds(pl.multiple_of(half_index * HID + first * HEAD_DIM, HEAD_DIM), size)

    def store_out(b, n, o):
        out_ref[pl.ds(pl.multiple_of(b * QB, QB), QB), pl.ds(pl.multiple_of(n * 256, 256), 256)] = o.astype(jnp.bfloat16)

    def out_product(b, n, end):
        cols = pl.ds(pl.multiple_of(n * 256, 256), 256)
        own = jnp.dot(heads(ctx_own, b, 0, HEADS), wo_buf[own_half, cols], preferred_element_type=jnp.float32)
        rows = out_rows(1 - y, 0, end)
        return own + jnp.dot(heads(ctx_peer, b, 0, end), wo_buf[rows, cols], preferred_element_type=jnp.float32)

    def project_out(b, carry):
        wait_pieces(b * HEADS, (b + 1) * HEADS)

        def out_tile(n, carry):
            store_out(b, n, out_product(b, n, HEADS))
            return carry

        return lax.fori_loop(0, 4, out_tile, carry)

    def project_last():
        b, most = N_BLOCK - 1, HEADS - 2
        wait_pieces(b * HEADS, b * HEADS + most)

        def first_part(n, carry):
            p_buf[2, pl.ds(pl.multiple_of(n * QB, QB), QB), :] = out_product(b, n, most)
            return carry

        lax.fori_loop(0, 4, first_part, 0)
        wait_pieces(b * HEADS + most, TILES)
        for n in range(4):
            cols, rows = pl.ds(n * 256, 256), out_rows(1 - y, most, HEADS)
            o = jnp.dot(heads(ctx_peer, b, most, HEADS), wo_buf[rows, cols], preferred_element_type=jnp.float32)
            store_out(b, n, p_buf[2, pl.ds(n * QB, QB), :] + o)

    def new_kv(c):
        project_kv(c)
        send_kv(c)

    new_kv(0)
    forward_wq(0)
    forward_wq(1)
    new_kv(1)
    forward_wq(2)
    forward_kv(0)
    forward_wq(3)
    forward_kv(1)
    new_kv(2)
    for cp in wq_f:
        cp.wait_recv()
    project_q(0)
    for c in (0, 1):
        wait_kv(c)
    prefetch(0, 1)
    new_kv(3)
    forward_kv(2)
    project_q(1)
    wait_kv(2)
    prefetch(2)
    new_kv(4)
    new_kv(5)
    wo_x = [send_wo(0), send_wo(1)]
    forward_kv(3)
    project_q(2)
    project_q(3)
    for c in (3, 4, 5):
        wait_kv(c)
        if c >= 4:
            vl_buf[c - 4] = jnp.transpose(vr_buf[c - 4])

    last = N_STEP - 1
    state = score_step(0, 0, last, load_state(0))
    for i in range(SLOTS):
        if i == 0:
            tile(0, 0, state)
            ctx_copy(0).start()
            state = score_step(1, 1, last, load_state(1))
        elif i + 1 < SLOTS:
            state = tile(i, i, state, i + 1, i + 1, load_state(i + 1), (last,))
        else:
            state = tile(i, i, state, i + 1, 0, empty, every)
        if i % 2:
            for n in range(max(i - 1, 1), i + 1):
                ctx_copy(n).start()

    pairs = HEADS // 2
    state = lax.fori_loop(pairs, 2 * pairs, two_tiles, state)
    wo_f = []

    def forward_wo(p):
        wo_x[p].wait_recv()
        wo_f.append(forward(wo_buf, shard(row_of[XP], p, half)))

    forward_wo(0)
    state = lax.fori_loop(2 * pairs, 3 * pairs, two_tiles, state)
    forward_wo(1)
    state = lax.fori_loop(3 * pairs, 4 * pairs - 1, two_tiles, state)
    state = tile(TILES - 2, 0, state, TILES - 1, 1, empty, every)
    ctx_copy(TILES - 2).start()
    tile(TILES - 1, 1, state)
    ctx_copy(TILES - 1).start()

    wo_local.wait()
    wo_core.wait_recv()
    for cp in wo_f:
        cp.wait_recv()

    lax.fori_loop(0, N_BLOCK - 1, project_out, 0)
    project_last()

    for cp in sent:
        cp.wait_send()

    def wait_sent(i, carry):
        ctx_copy(i).wait_send()
        return carry

    lax.fori_loop(0, TILES, wait_sent, 0)
    assert next(number) <= N_SEM


def solution(mesh):
    def local_block(tokens, w_qkv, w_out, doc_ids):
        bf16, f32 = jnp.bfloat16, jnp.float32
        dma = pltpu.SemaphoreType.DMA
        any_spec = pl.BlockSpec(memory_space=pl.ANY)
        return pl.pallas_call(
            kernel,
            out_shape=pltpu.VMEM(tokens.shape, bf16),
            in_specs=[any_spec] * 4,
            out_specs=pl.BlockSpec(memory_space=pltpu.VMEM),
            scratch_shapes=[
                pltpu.VMEM((ROWS, HID), bf16),
                pltpu.VMEM((ROWS, HID), bf16),
                pltpu.VMEM((2 * HID, QKV), bf16),
                pltpu.VMEM((2 * HID, HID), bf16),
                pltpu.VMEM((4, 8, 128), jnp.int32),
                pltpu.VMEM((ROWS, HID), bf16),
                pltpu.VMEM((ROWS, 128), bf16),
                pltpu.VMEM((SEQ, HEAD_DIM), bf16),
                pltpu.VMEM((SEQ, HEAD_DIM), bf16),
                pltpu.VMEM((12, HEAD_DIM, 256), bf16),
                pltpu.VMEM((4, HEAD_DIM, 128), bf16),
                pltpu.VMEM((2, 256, HEAD_DIM), bf16),
                pltpu.VMEM((2, HEAD_DIM, 256), bf16),
                pltpu.VMEM((SLOTS, SEQ, QB), f32),
                pltpu.VMEM((SLOTS, SEQ // GROUP, 8, QB), f32),
                pltpu.VMEM((SLOTS, 2, 8, QB), f32),
                pltpu.VMEM((TILES, QB, HEAD_DIM), bf16),
                pltpu.VMEM((TILES, QB, HEAD_DIM), bf16),
                dma((4,)),
                dma((N_SEM,)),
                dma((N_SEM,)),
                dma((TILES,)),
                dma((TILES,)),
            ],
            compiler_params=pltpu.CompilerParams(
                collective_id=0, has_side_effects=True, vmem_limit_bytes=61 * 1024 * 1024
            ),
        )(tokens, w_qkv, w_out, doc_ids.reshape(8, 128))

    row_spec = P(("data", "row"), "col")
    weight_spec = P("row", "col")
    return jax.shard_map(
        local_block,
        mesh=mesh,
        in_specs=(row_spec, weight_spec, weight_spec, P(("data", "row"))),
        out_specs=row_spec,
        check_vma=False,
    )
```

```python
import itertools
import math

import jax
import jax.numpy as jnp
from jax import lax
from jax.experimental import pallas as pl
from jax.experimental.pallas import tpu as pltpu
from jax.sharding import PartitionSpec as P

HEAD_DIM = 128
MESH = pl.DeviceIdType.MESH

ROWS = 1024
HID = 1024
SEQ = 4096
HEADS = 8
QKV = 1280
SHARD = 512
QB = 256
KC = 1024
GROUP = 128
N_GROUP = KC // GROUP
N_STEP = SEQ // KC
CHUNKS = ((0, 256), (256, 256), (512, 256), (768, 128), (896, 64), (960, 64))
HALF_COLS = HID // 2
N_BLOCK = ROWS // QB
TILES = HEADS * N_BLOCK
SLOTS = 8
N_SEM = 72
CORE, XP, DIAG = 0, 1, 2
EXP_SCALE = math.log2(math.e) / math.sqrt(HEAD_DIM)
NT = (((1,), (1,)), ((), ()))
BF16_MAX = float(jnp.finfo(jnp.bfloat16).max)
F32_MIN = float(jnp.finfo(jnp.float32).min)


def kernel(
    tok_hbm, w_hbm, wo_hbm, doc_hbm, out_ref,
    tok_own, tok_peer, w_buf, wo_buf, doc_buf, q_buf, qx_buf, k_buf, kx_buf, vw_buf, vn_buf, vr_buf, vl_buf, p_buf, top_buf, state_buf,
    ctx_own, ctx_peer, loc_sem, send_sem, recv_sem, ctx_send, ctx_recv,
):
    d, y, r = lax.axis_index("data"), lax.axis_index("col"), lax.axis_index("row")
    x, core = r // 2, r % 2
    row_of = {CORE: x * 2 + (1 - core), XP: (1 - x) * 2 + core, DIAG: (1 - x) * 2 + (1 - core)}
    y_peer = (d, 1 - y, r)
    peer = {k: (d, y, v) for k, v in row_of.items()}

    barrier = pltpu.get_barrier_semaphore()
    for p in (y_peer, peer[CORE], peer[XP], peer[DIAG]):
        pl.semaphore_signal(barrier, inc=1, device_id=p, device_id_type=MESH)
    pl.semaphore_wait(barrier, 4)

    number = itertools.count()
    sent = []

    def send(src, dst, device):
        i = next(number)
        cp = pltpu.make_async_remote_copy(
            src_ref=src, dst_ref=dst, send_sem=send_sem.at[i], recv_sem=recv_sem.at[i], device_id=device, device_id_type=MESH
        )
        cp.start()
        sent.append(cp)
        return cp

    def local(src, dst, i):
        cp = pltpu.make_async_copy(src, dst, loc_sem.at[i])
        cp.start()
        return cp

    def shard(row, piece=0, size=SHARD):
        return pl.ds(pl.multiple_of(row * SHARD + piece * size, size), size)

    kv_cols, half = pl.ds(HID, 2 * HEAD_DIM), SHARD // 2

    def send_wq(cols):
        at = pl.ds(cols * HALF_COLS, HALF_COLS)
        return [
            send(w_hbm.at[pl.ds(p * half, half), at], w_buf.at[shard(r, p, half), at], peer[XP]) for p in (0, 1)
        ]

    tok_in = []
    for first, size in CHUNKS:
        rows = pl.ds(first, size)
        tok_in.append(send(tok_hbm.at[rows], tok_peer.at[rows], y_peer))
    wkv_x = send(w_hbm.at[:, kv_cols], w_buf.at[shard(r), kv_cols], peer[XP])
    doc_in = [send(doc_hbm, doc_buf.at[r], peer[k]) for k in (CORE, XP, DIAG)]
    wq_x = [send_wq(0)]
    w_core = send(w_hbm, w_buf.at[shard(r)], peer[CORE])
    wo_core = send(wo_hbm, wo_buf.at[shard(r)], peer[CORE])
    doc_local = local(doc_hbm, doc_buf.at[r], 0)
    w_local = local(w_hbm, w_buf.at[shard(r)], 1)
    tok_local = local(tok_hbm, tok_own, 2)
    wo_local = local(wo_hbm, wo_buf.at[shard(r)], 3)

    doc_local.wait()
    for cp in doc_in:
        cp.wait_recv()
    lane = lax.broadcasted_iota(jnp.int32, (128, 128), 1)

    def as_column(line):
        return jnp.transpose(jnp.broadcast_to(line, (128, 128)))

    def key_mask(place):
        def line_mask(i, carry):
            part, line, first = place(i)
            ids = as_column(doc_buf[part, pl.ds(line, 1), :])
            hit = jnp.where(lane < 3, 1 - ids, jnp.where(lane < 6, ids, 0)).astype(jnp.float32).astype(jnp.bfloat16)
            for n, at in enumerate(first):
                size = 128 // len(first)
                kx_buf[pl.ds(pl.multiple_of(at, size), size), :] = hit[n * size : (n + 1) * size]
            return carry

        return line_mask

    def query_mask(i, carry):
        ids = as_column(doc_buf[r, pl.ds(i, 1), :])
        hit = jnp.where(lane < 3, ids, jnp.where(lane < 6, 1 - ids, 0))
        qx_buf[pl.ds(pl.multiple_of(i * 128, 128), 128), :] = jnp.where(hit == 1, -BF16_MAX, 0.0).astype(jnp.bfloat16)
        return carry

    wide = key_mask(lambda i: (i // 6, i % 6, [(i % 6) // 2 * 1024 + i // 6 * 256 + i % 2 * 128]))
    lax.fori_loop(0, 24, wide, 0)
    lax.fori_loop(0, 4, key_mask(lambda i: (i, 6, [3072 + i * 128])), 0)
    lax.fori_loop(0, 4, key_mask(lambda i: (i, 7, [3584 + i * 64, 3840 + i * 64])), 0)
    lax.fori_loop(0, ROWS // 128, query_mask, 0)

    own_half = pl.ds(pl.multiple_of(y * HID, HID), HID)
    peer_half = pl.ds(pl.multiple_of((1 - y) * HID, HID), HID)

    def project(rows, cols):
        return jnp.dot(tok_own[rows, :], w_buf[own_half, cols], preferred_element_type=jnp.float32) + jnp.dot(
            tok_peer[rows, :], w_buf[peer_half, cols], preferred_element_type=jnp.float32
        )

    def forward(ref, *index):
        return send(ref.at[index], ref.at[index], peer[CORE])

    k_in, kv_core = [], [[] for _ in CHUNKS]

    def keys_of(row, c):
        first, size = CHUNKS[c]
        if size == 64:
            values = vr_buf.at[c - 4, pl.ds(pl.multiple_of(row * size, size), size)]
        else:
            values = vw_buf.at[c * 4 + row] if size == 256 else vn_buf.at[row]
        return k_buf.at[pl.ds(pl.multiple_of(first * 4 + row * size, size), size)], values

    def project_kv(c):
        tok_in[c].wait_recv()
        kv = project(pl.ds(*CHUNKS[c]), kv_cols).astype(jnp.bfloat16)
        keys, values = keys_of(r, c)
        keys[...] = kv[:, :HEAD_DIM]
        values[...] = kv[:, HEAD_DIM:] if c >= 4 else jnp.transpose(kv[:, HEAD_DIM:])

    def send_kv(c):
        refs = keys_of(r, c)
        if c >= 4:
            kv_core[c] += [send(ref, ref, peer[k]) for k in (XP, DIAG, CORE) for ref in refs]
            return
        k_in.append([send(ref, ref, peer[XP]) for ref in refs])
        kv_core[c].extend(send(ref, ref, peer[CORE]) for ref in refs)

    def forward_kv(c):
        for ref, cp in zip(keys_of(row_of[XP], c), k_in[c]):
            cp.wait_recv()
            kv_core[c].append(send(ref, ref, peer[CORE]))

    def wait_kv(c):
        for cp in kv_core[c]:
            cp.wait_recv()

    def project_q(c, first=0, end=4):
        rows = pl.ds(c * QB, QB)

        def q_tile(n, carry):
            cols = pl.ds(pl.multiple_of(n * 256, 256), 256)
            q_buf[rows, cols] = project(rows, cols).astype(jnp.bfloat16)
            return carry

        lax.fori_loop(first, end, q_tile, 0)

    wkv_x.wait_recv()
    wkv_f = forward(w_buf, shard(row_of[XP]), kv_cols)
    w_local.wait()
    tok_local.wait()
    w_core.wait_recv()
    wkv_f.wait_recv()
    wq_f = [[], []]

    def forward_wq(cols, p):
        wq_x[cols][p].wait_recv()
        wq_f[cols].append(forward(w_buf, shard(row_of[XP], p, half), pl.ds(cols * HALF_COLS, HALF_COLS)))

    def wait_wq(cols):
        for cp in wq_f[cols]:
            cp.wait_recv()

    def send_wo(p):
        return send(wo_hbm.at[pl.ds(p * half, half)], wo_buf.at[shard(r, p, half)], peer[XP])

    def tile_of(i):
        block, head = i // 16 * 2 + i // 4 % 2, i // 8 % 2 * 4 + i % 4
        return (
            pl.ds(pl.multiple_of(block * QB, QB), QB),
            pl.ds(pl.multiple_of(head * HEAD_DIM, HEAD_DIM), HEAD_DIM),
        )

    def tile_at(block, head):
        return block // 2 * 16 + head // 4 * 8 + block % 2 * 4 + head % 4

    def over_keys(f, a):
        return f(a.reshape(a.shape[0] // 8, 8, QB), axis=0)

    def to_keys(a):
        return jnp.concatenate([a] * (GROUP // 8), axis=0)

    def score_step(i, slot, j, state):
        top, total = state
        rows, cols = tile_of(i)
        q = jnp.concatenate([q_buf[rows, cols], qx_buf[rows, :]], axis=1)
        k = jnp.concatenate([k_buf[pl.ds(j * KC, KC), :], kx_buf[pl.ds(j * KC, KC), :]], axis=1)
        s = lax.dot_general(k, q, NT, preferred_element_type=jnp.float32)
        for g in range(N_GROUP):
            part = s[g * GROUP : (g + 1) * GROUP]
            new_top = jnp.maximum(top, over_keys(jnp.max, part))
            scaled = new_top * EXP_SCALE
            top_buf[slot, j * N_GROUP + g] = scaled
            p = jnp.exp2(part * EXP_SCALE - to_keys(scaled))
            p_buf[slot, pl.ds(j * KC + g * GROUP, GROUP), :] = p
            total = total * jnp.exp2(top * EXP_SCALE - scaled) + over_keys(jnp.sum, p)
            top = new_top
        return top, total

    def value_step(slot, j, lse, acc):
        keys = pl.ds(j * KC, KC)
        factor = [to_keys(jnp.exp2(top_buf[slot, j * N_GROUP + g] - lse)) for g in range(N_GROUP)]
        weights = p_buf[slot, keys, :] * jnp.concatenate(factor, axis=0)
        parts = [vw_buf[j * 4 + i] for i in range(4)] if j + 1 < N_STEP else [*(vn_buf[i] for i in range(4)), vl_buf[0], vl_buf[1]]
        o = jnp.dot(jnp.concatenate(parts, axis=1), weights.astype(jnp.bfloat16), preferred_element_type=jnp.float32)
        return o if acc is None else acc + o

    def ctx_copy(i):
        return pltpu.make_async_remote_copy(
            src_ref=ctx_own.at[i], dst_ref=ctx_peer.at[i], send_sem=ctx_send.at[i], recv_sem=ctx_recv.at[i],
            device_id=y_peer, device_id_type=MESH,
        )

    empty = (jnp.full((8, QB), F32_MIN, jnp.float32), jnp.zeros((8, QB), jnp.float32))

    def load_state(slot):
        return state_buf[slot, 0], state_buf[slot, 1]

    def prefetch(*steps):
        def one(slot, carry):
            state = load_state(slot) if steps[0] else empty
            for j in steps:
                state = score_step(slot, slot, j, state)
            state_buf[slot, 0], state_buf[slot, 1] = state
            return carry

        lax.fori_loop(0, SLOTS, one, 0)

    def tile(i, slot, state, nxt=None, nxt_slot=None, nxt_state=None, nxt_steps=()):
        top, total = state
        best = jnp.max(top, axis=0, keepdims=True)
        whole = jnp.sum(total * jnp.exp2((top - best) * EXP_SCALE), axis=0, keepdims=True)
        lse = best * EXP_SCALE + jnp.log2(whole)
        acc = None
        steps = list(nxt_steps)
        for j in range(N_STEP):
            if steps:
                nxt_state = score_step(nxt, nxt_slot, steps.pop(0), nxt_state)
            acc = value_step(slot, j, lse, acc)
        ctx_own[i] = jnp.transpose(acc).astype(jnp.bfloat16)
        return nxt_state

    every = range(N_STEP)

    def two_tiles(t, state):
        i = t * 2
        state = tile(i, 0, state, i + 1, 1, empty, every)
        state = tile(i + 1, 1, state, i + 2, 0, empty, every)
        ctx_copy(i).start()
        ctx_copy(i + 1).start()
        return state

    def wait_pieces(b, first, end):
        def wait_piece(h, carry):
            ctx_copy(tile_at(b, h)).wait_recv()
            return carry

        lax.fori_loop(first, end, wait_piece, 0)

    def heads(ref, b, first, end):
        return jnp.concatenate([ref[tile_at(b, h)] for h in range(first, end)], axis=1)

    def out_rows(half_index, first, end):
        size = (end - first) * HEAD_DIM
        return pl.ds(pl.multiple_of(half_index * HID + first * HEAD_DIM, HEAD_DIM), size)

    def store_out(b, n, o):
        out_ref[pl.ds(pl.multiple_of(b * QB, QB), QB), pl.ds(pl.multiple_of(n * 256, 256), 256)] = o.astype(jnp.bfloat16)

    def out_product(b, n, end):
        cols = pl.ds(pl.multiple_of(n * 256, 256), 256)
        own = jnp.dot(heads(ctx_own, b, 0, HEADS), wo_buf[own_half, cols], preferred_element_type=jnp.float32)
        rows = out_rows(1 - y, 0, end)
        return own + jnp.dot(heads(ctx_peer, b, 0, end), wo_buf[rows, cols], preferred_element_type=jnp.float32)

    def project_out(b, carry):
        wait_pieces(b, 0, HEADS)

        def out_tile(n, carry):
            store_out(b, n, out_product(b, n, HEADS))
            return carry

        return lax.fori_loop(0, 4, out_tile, carry)

    def project_last():
        b, most = N_BLOCK - 1, HEADS - 2
        wait_pieces(b, 0, most)

        def first_part(n, carry):
            p_buf[2, pl.ds(pl.multiple_of(n * QB, QB), QB), :] = out_product(b, n, most)
            return carry

        lax.fori_loop(0, 4, first_part, 0)
        wait_pieces(b, most, HEADS)
        for n in range(4):
            cols, rows = pl.ds(n * 256, 256), out_rows(1 - y, most, HEADS)
            o = jnp.dot(heads(ctx_peer, b, most, HEADS), wo_buf[rows, cols], preferred_element_type=jnp.float32)
            store_out(b, n, p_buf[2, pl.ds(n * QB, QB), :] + o)

    def new_kv(c):
        project_kv(c)
        send_kv(c)

    new_kv(0)
    forward_wq(0, 0)
    forward_wq(0, 1)
    forward_kv(0)
    wait_wq(0)
    project_q(0, 0, 2)
    new_kv(1)
    wq_x.append(send_wq(1))
    project_q(1, 0, 2)
    wait_kv(0)
    prefetch(0)
    forward_kv(1)
    wait_kv(1)
    prefetch(1)
    forward_wq(1, 0)
    new_kv(2)
    forward_wq(1, 1)
    wait_wq(1)
    project_q(0, 2, 4)
    project_q(1, 2, 4)
    forward_kv(2)
    wait_kv(2)
    prefetch(2)
    new_kv(3)
    project_q(2)
    new_kv(4)
    new_kv(5)
    wo_x = [send_wo(0), send_wo(1)]
    forward_kv(3)
    project_q(3)
    for c in (3, 4, 5):
        wait_kv(c)
        if c >= 4:
            vl_buf[c - 4] = jnp.transpose(vr_buf[c - 4])

    last = N_STEP - 1
    state = score_step(0, 0, last, load_state(0))
    for i in range(SLOTS):
        if i == 0:
            tile(0, 0, state)
            ctx_copy(0).start()
            state = score_step(1, 1, last, load_state(1))
        elif i + 1 < SLOTS:
            state = tile(i, i, state, i + 1, i + 1, load_state(i + 1), (last,))
        else:
            state = tile(i, i, state, i + 1, 0, empty, every)
        if i % 2:
            for n in range(max(i - 1, 1), i + 1):
                ctx_copy(n).start()

    pairs = HEADS // 2
    state = lax.fori_loop(pairs, 2 * pairs, two_tiles, state)
    wo_f = []

    def forward_wo(p):
        wo_x[p].wait_recv()
        wo_f.append(forward(wo_buf, shard(row_of[XP], p, half)))

    forward_wo(0)
    state = lax.fori_loop(2 * pairs, 3 * pairs, two_tiles, state)
    forward_wo(1)
    state = lax.fori_loop(3 * pairs, 4 * pairs - 1, two_tiles, state)
    state = tile(TILES - 2, 0, state, TILES - 1, 1, empty, every)
    ctx_copy(TILES - 2).start()
    tile(TILES - 1, 1, state)
    ctx_copy(TILES - 1).start()

    wo_local.wait()
    wo_core.wait_recv()
    for cp in wo_f:
        cp.wait_recv()

    lax.fori_loop(0, N_BLOCK - 1, project_out, 0)
    project_last()

    for cp in sent:
        cp.wait_send()

    def wait_sent(i, carry):
        ctx_copy(i).wait_send()
        return carry

    lax.fori_loop(0, TILES, wait_sent, 0)
    assert next(number) <= N_SEM


def solution(mesh):
    def local_block(tokens, w_qkv, w_out, doc_ids):
        bf16, f32 = jnp.bfloat16, jnp.float32
        dma = pltpu.SemaphoreType.DMA
        any_spec = pl.BlockSpec(memory_space=pl.ANY)
        return pl.pallas_call(
            kernel,
            out_shape=pltpu.VMEM(tokens.shape, bf16),
            in_specs=[any_spec] * 4,
            out_specs=pl.BlockSpec(memory_space=pltpu.VMEM),
            scratch_shapes=[
                pltpu.VMEM((ROWS, HID), bf16),
                pltpu.VMEM((ROWS, HID), bf16),
                pltpu.VMEM((2 * HID, QKV), bf16),
                pltpu.VMEM((2 * HID, HID), bf16),
                pltpu.VMEM((4, 8, 128), jnp.int32),
                pltpu.VMEM((ROWS, HID), bf16),
                pltpu.VMEM((ROWS, 128), bf16),
                pltpu.VMEM((SEQ, HEAD_DIM), bf16),
                pltpu.VMEM((SEQ, HEAD_DIM), bf16),
                pltpu.VMEM((12, HEAD_DIM, 256), bf16),
                pltpu.VMEM((4, HEAD_DIM, 128), bf16),
                pltpu.VMEM((2, 256, HEAD_DIM), bf16),
                pltpu.VMEM((2, HEAD_DIM, 256), bf16),
                pltpu.VMEM((SLOTS, SEQ, QB), f32),
                pltpu.VMEM((SLOTS, SEQ // GROUP, 8, QB), f32),
                pltpu.VMEM((SLOTS, 2, 8, QB), f32),
                pltpu.VMEM((TILES, QB, HEAD_DIM), bf16),
                pltpu.VMEM((TILES, QB, HEAD_DIM), bf16),
                dma((4,)),
                dma((N_SEM,)),
                dma((N_SEM,)),
                dma((TILES,)),
                dma((TILES,)),
            ],
            compiler_params=pltpu.CompilerParams(
                collective_id=0, has_side_effects=True, vmem_limit_bytes=61 * 1024 * 1024
            ),
        )(tokens, w_qkv, w_out, doc_ids.reshape(8, 128))

    row_spec = P(("data", "row"), "col")
    weight_spec = P("row", "col")
    return jax.shard_map(
        local_block,
        mesh=mesh,
        in_specs=(row_spec, weight_spec, weight_spec, P(("data", "row"))),
        out_specs=row_spec,
        check_vma=False,
    )
```

```python
import itertools
import math

import jax
import jax.numpy as jnp
from jax import lax
from jax.experimental import pallas as pl
from jax.experimental.pallas import tpu as pltpu
from jax.sharding import PartitionSpec as P

HEAD_DIM = 128
MESH = pl.DeviceIdType.MESH

ROWS = 1024
HID = 1024
SEQ = 4096
HEADS = 8
QKV = 1280
SHARD = 512
QB = 256
KC = 1024
GROUP = 128
N_GROUP = KC // GROUP
N_STEP = SEQ // KC
CHUNKS = ((0, 256), (256, 256), (512, 256), (768, 128), (896, 64), (960, 64))
HALF_COLS = HID // 2
N_BLOCK = ROWS // QB
TILES = HEADS * N_BLOCK
SLOTS = 8
N_SEM = 72
CORE, XP, DIAG = 0, 1, 2
EXP_SCALE = math.log2(math.e) / math.sqrt(HEAD_DIM)
NT = (((1,), (1,)), ((), ()))
BF16_MAX = float(jnp.finfo(jnp.bfloat16).max)
F32_MIN = float(jnp.finfo(jnp.float32).min)


def kernel(
    tok_hbm, w_hbm, wo_hbm, doc_hbm, out_ref,
    tok_own, tok_peer, w_buf, wo_buf, doc_buf, q_buf, qx_buf, k_buf, kx_buf, vw_buf, vn_buf, vr_buf, vl_buf, p_buf, top_buf, state_buf,
    ctx_own, ctx_peer, loc_sem, send_sem, recv_sem, ctx_send, ctx_recv,
):
    d, y, r = lax.axis_index("data"), lax.axis_index("col"), lax.axis_index("row")
    x, core = r // 2, r % 2
    row_of = {CORE: x * 2 + (1 - core), XP: (1 - x) * 2 + core, DIAG: (1 - x) * 2 + (1 - core)}
    y_peer = (d, 1 - y, r)
    peer = {k: (d, y, v) for k, v in row_of.items()}

    barrier = pltpu.get_barrier_semaphore()
    for p in (y_peer, peer[CORE], peer[XP], peer[DIAG]):
        pl.semaphore_signal(barrier, inc=1, device_id=p, device_id_type=MESH)
    pl.semaphore_wait(barrier, 4)

    number = itertools.count()
    sent = []

    def send(src, dst, device):
        i = next(number)
        cp = pltpu.make_async_remote_copy(
            src_ref=src, dst_ref=dst, send_sem=send_sem.at[i], recv_sem=recv_sem.at[i], device_id=device, device_id_type=MESH
        )
        cp.start()
        sent.append(cp)
        return cp

    def local(src, dst, i):
        cp = pltpu.make_async_copy(src, dst, loc_sem.at[i])
        cp.start()
        return cp

    def shard(row, piece=0, size=SHARD):
        return pl.ds(pl.multiple_of(row * SHARD + piece * size, size), size)

    kv_cols, half = pl.ds(HID, 2 * HEAD_DIM), SHARD // 2

    def send_wq(cols):
        at = pl.ds(cols * HALF_COLS, HALF_COLS)
        return [
            send(w_hbm.at[pl.ds(p * half, half), at], w_buf.at[shard(r, p, half), at], peer[XP]) for p in (0, 1)
        ]

    tok_in = []

    def send_tokens(source, *chunks):
        for c in chunks:
            rows = pl.ds(*CHUNKS[c])
            tok_in.append(send(source.at[rows], tok_peer.at[rows], y_peer))

    send_tokens(tok_hbm, 0, 1)
    wkv_x = send(w_hbm.at[:, kv_cols], w_buf.at[shard(r), kv_cols], peer[XP])
    doc_in = [send(doc_hbm, doc_buf.at[r], peer[k]) for k in (CORE, XP, DIAG)]
    wq_x = []
    w_core = send(w_hbm, w_buf.at[shard(r)], peer[CORE])
    wo_core = send(wo_hbm, wo_buf.at[shard(r)], peer[CORE])
    doc_local = local(doc_hbm, doc_buf.at[r], 0)
    w_local = local(w_hbm, w_buf.at[shard(r)], 1)
    tok_local = local(tok_hbm, tok_own, 2)
    wo_local = local(wo_hbm, wo_buf.at[shard(r)], 3)

    doc_local.wait()
    for cp in doc_in:
        cp.wait_recv()
    lane = lax.broadcasted_iota(jnp.int32, (128, 128), 1)

    def as_column(line):
        return jnp.transpose(jnp.broadcast_to(line, (128, 128)))

    def key_mask(place):
        def line_mask(i, carry):
            part, line, first = place(i)
            ids = as_column(doc_buf[part, pl.ds(line, 1), :])
            hit = jnp.where(lane < 3, 1 - ids, jnp.where(lane < 6, ids, 0)).astype(jnp.float32).astype(jnp.bfloat16)
            for n, at in enumerate(first):
                size = 128 // len(first)
                kx_buf[pl.ds(pl.multiple_of(at, size), size), :] = hit[n * size : (n + 1) * size]
            return carry

        return line_mask

    def query_mask(i, carry):
        ids = as_column(doc_buf[r, pl.ds(i, 1), :])
        hit = jnp.where(lane < 3, ids, jnp.where(lane < 6, 1 - ids, 0))
        qx_buf[pl.ds(pl.multiple_of(i * 128, 128), 128), :] = jnp.where(hit == 1, -BF16_MAX, 0.0).astype(jnp.bfloat16)
        return carry

    wide = key_mask(lambda i: (i // 6, i % 6, [(i % 6) // 2 * 1024 + i // 6 * 256 + i % 2 * 128]))
    lax.fori_loop(0, 24, wide, 0)
    lax.fori_loop(0, 4, key_mask(lambda i: (i, 6, [3072 + i * 128])), 0)
    lax.fori_loop(0, 4, key_mask(lambda i: (i, 7, [3584 + i * 64, 3840 + i * 64])), 0)
    lax.fori_loop(0, ROWS // 128, query_mask, 0)

    own_half = pl.ds(pl.multiple_of(y * HID, HID), HID)
    peer_half = pl.ds(pl.multiple_of((1 - y) * HID, HID), HID)

    def project(rows, cols):
        return jnp.dot(tok_own[rows, :], w_buf[own_half, cols], preferred_element_type=jnp.float32) + jnp.dot(
            tok_peer[rows, :], w_buf[peer_half, cols], preferred_element_type=jnp.float32
        )

    def forward(ref, *index):
        return send(ref.at[index], ref.at[index], peer[CORE])

    k_in, kv_core = {}, [[] for _ in CHUNKS]

    def keys_of(row, c):
        first, size = CHUNKS[c]
        if size == 64:
            values = vr_buf.at[c - 4, pl.ds(pl.multiple_of(row * size, size), size)]
        else:
            values = vw_buf.at[c * 4 + row] if size == 256 else vn_buf.at[row]
        return k_buf.at[pl.ds(pl.multiple_of(first * 4 + row * size, size), size)], values

    def project_kv(c):
        tok_in[c].wait_recv()
        kv = project(pl.ds(*CHUNKS[c]), kv_cols).astype(jnp.bfloat16)
        keys, values = keys_of(r, c)
        keys[...] = kv[:, :HEAD_DIM]
        values[...] = kv[:, HEAD_DIM:] if c >= 4 else jnp.transpose(kv[:, HEAD_DIM:])

    def send_kv(c):
        refs = keys_of(r, c)
        if c >= 4:
            kv_core[c] += [send(ref, ref, peer[k]) for k in (XP, DIAG, CORE) for ref in refs]
            return
        k_in[c] = [send(ref, ref, peer[XP]) for ref in refs]
        kv_core[c].extend(send(ref, ref, peer[CORE]) for ref in refs)

    def forward_kv(c):
        for ref, cp in zip(keys_of(row_of[XP], c), k_in[c]):
            cp.wait_recv()
            kv_core[c].append(send(ref, ref, peer[CORE]))

    def wait_kv(c):
        for cp in kv_core[c]:
            cp.wait_recv()

    def project_q(c, first=0, end=4):
        rows = pl.ds(c * QB, QB)

        def q_tile(n, carry):
            cols = pl.ds(pl.multiple_of(n * 256, 256), 256)
            q_buf[rows, cols] = project(rows, cols).astype(jnp.bfloat16)
            return carry

        lax.fori_loop(first, end, q_tile, 0)

    left = []

    def gone(*copies):
        for cp in copies:
            cp.wait_send()
            left.append(id(cp))

    gone(wkv_x)
    wq_x.append(send_wq(0))
    wkv_x.wait_recv()
    wkv_f = forward(w_buf, shard(row_of[XP]), kv_cols)
    w_local.wait()
    tok_local.wait()
    w_core.wait_recv()
    wkv_f.wait_recv()
    wq_f = [[], []]

    def forward_wq(cols, p):
        wq_x[cols][p].wait_recv()
        wq_f[cols].append(forward(w_buf, shard(row_of[XP], p, half), pl.ds(cols * HALF_COLS, HALF_COLS)))

    def wait_wq(cols):
        for cp in wq_f[cols]:
            cp.wait_recv()

    def send_wo(p):
        return send(wo_hbm.at[pl.ds(p * half, half)], wo_buf.at[shard(r, p, half)], peer[XP])

    def tile_of(i):
        block, head = i // 16 * 2 + i // 4 % 2, i // 8 % 2 * 4 + i % 4
        return (
            pl.ds(pl.multiple_of(block * QB, QB), QB),
            pl.ds(pl.multiple_of(head * HEAD_DIM, HEAD_DIM), HEAD_DIM),
        )

    def tile_at(block, head):
        return block // 2 * 16 + head // 4 * 8 + block % 2 * 4 + head % 4

    def over_keys(f, a):
        return f(a.reshape(a.shape[0] // 8, 8, QB), axis=0)

    def to_keys(a):
        return jnp.concatenate([a] * (GROUP // 8), axis=0)

    def score_step(i, slot, j, state):
        top, total = state
        rows, cols = tile_of(i)
        q = jnp.concatenate([q_buf[rows, cols], qx_buf[rows, :]], axis=1)
        k = jnp.concatenate([k_buf[pl.ds(j * KC, KC), :], kx_buf[pl.ds(j * KC, KC), :]], axis=1)
        s = lax.dot_general(k, q, NT, preferred_element_type=jnp.float32)
        for g in range(N_GROUP):
            part = s[g * GROUP : (g + 1) * GROUP]
            new_top = jnp.maximum(top, over_keys(jnp.max, part))
            scaled = new_top * EXP_SCALE
            top_buf[slot, j * N_GROUP + g] = scaled
            p = jnp.exp2(part * EXP_SCALE - to_keys(scaled))
            p_buf[slot, pl.ds(j * KC + g * GROUP, GROUP), :] = p
            total = total * jnp.exp2(top * EXP_SCALE - scaled) + over_keys(jnp.sum, p)
            top = new_top
        return top, total

    def value_step(slot, j, lse, acc):
        keys = pl.ds(j * KC, KC)
        factor = [to_keys(jnp.exp2(top_buf[slot, j * N_GROUP + g] - lse)) for g in range(N_GROUP)]
        weights = p_buf[slot, keys, :] * jnp.concatenate(factor, axis=0)
        parts = [vw_buf[j * 4 + i] for i in range(4)] if j + 1 < N_STEP else [*(vn_buf[i] for i in range(4)), vl_buf[0], vl_buf[1]]
        o = jnp.dot(jnp.concatenate(parts, axis=1), weights.astype(jnp.bfloat16), preferred_element_type=jnp.float32)
        return o if acc is None else acc + o

    def ctx_copy(i):
        return pltpu.make_async_remote_copy(
            src_ref=ctx_own.at[i], dst_ref=ctx_peer.at[i], send_sem=ctx_send.at[i], recv_sem=ctx_recv.at[i],
            device_id=y_peer, device_id_type=MESH,
        )

    empty = (jnp.full((8, QB), F32_MIN, jnp.float32), jnp.zeros((8, QB), jnp.float32))

    def load_state(slot):
        return state_buf[slot, 0], state_buf[slot, 1]

    def prefetch(*steps):
        def one(slot, carry):
            state = load_state(slot) if steps[0] else empty
            for j in steps:
                state = score_step(slot, slot, j, state)
            state_buf[slot, 0], state_buf[slot, 1] = state
            return carry

        lax.fori_loop(0, SLOTS, one, 0)

    def tile(i, slot, state, nxt=None, nxt_slot=None, nxt_state=None, nxt_steps=()):
        top, total = state
        best = jnp.max(top, axis=0, keepdims=True)
        whole = jnp.sum(total * jnp.exp2((top - best) * EXP_SCALE), axis=0, keepdims=True)
        lse = best * EXP_SCALE + jnp.log2(whole)
        acc = None
        steps = list(nxt_steps)
        for j in range(N_STEP):
            if steps:
                nxt_state = score_step(nxt, nxt_slot, steps.pop(0), nxt_state)
            acc = value_step(slot, j, lse, acc)
        ctx_own[i] = jnp.transpose(acc).astype(jnp.bfloat16)
        return nxt_state

    every = range(N_STEP)

    def two_tiles(t, state):
        i = t * 2
        state = tile(i, 0, state, i + 1, 1, empty, every)
        state = tile(i + 1, 1, state, i + 2, 0, empty, every)
        ctx_copy(i).start()
        ctx_copy(i + 1).start()
        return state

    def wait_pieces(b, first, end):
        def wait_piece(h, carry):
            ctx_copy(tile_at(b, h)).wait_recv()
            return carry

        lax.fori_loop(first, end, wait_piece, 0)

    def heads(ref, b, first, end):
        return jnp.concatenate([ref[tile_at(b, h)] for h in range(first, end)], axis=1)

    def out_rows(half_index, first, end):
        size = (end - first) * HEAD_DIM
        return pl.ds(pl.multiple_of(half_index * HID + first * HEAD_DIM, HEAD_DIM), size)

    def store_out(b, n, o):
        out_ref[pl.ds(pl.multiple_of(b * QB, QB), QB), pl.ds(pl.multiple_of(n * 256, 256), 256)] = o.astype(jnp.bfloat16)

    def out_product(b, n, end):
        cols = pl.ds(pl.multiple_of(n * 256, 256), 256)
        own = jnp.dot(heads(ctx_own, b, 0, HEADS), wo_buf[own_half, cols], preferred_element_type=jnp.float32)
        rows = out_rows(1 - y, 0, end)
        return own + jnp.dot(heads(ctx_peer, b, 0, end), wo_buf[rows, cols], preferred_element_type=jnp.float32)

    def project_out(b, carry):
        wait_pieces(b, 0, HEADS)

        def out_tile(n, carry):
            store_out(b, n, out_product(b, n, HEADS))
            return carry

        return lax.fori_loop(0, 4, out_tile, carry)

    def project_last():
        b, most = N_BLOCK - 1, HEADS - 2
        wait_pieces(b, 0, most)

        def first_part(n, carry):
            p_buf[2, pl.ds(pl.multiple_of(n * QB, QB), QB), :] = out_product(b, n, most)
            return carry

        lax.fori_loop(0, 4, first_part, 0)
        wait_pieces(b, most, HEADS)
        for n in range(4):
            cols, rows = pl.ds(n * 256, 256), out_rows(1 - y, most, HEADS)
            o = jnp.dot(heads(ctx_peer, b, most, HEADS), wo_buf[rows, cols], preferred_element_type=jnp.float32)
            store_out(b, n, p_buf[2, pl.ds(n * QB, QB), :] + o)

    def new_kv(c):
        project_kv(c)
        send_kv(c)

    forward_wq(0, 0)
    forward_wq(0, 1)
    gone(*wq_x[0])
    wq_x.append(send_wq(1))
    wait_wq(0)
    gone(tok_in[0], tok_in[1])
    send_tokens(tok_own, 2)
    new_kv(0)
    new_kv(1)
    project_q(0, 0, 2)
    project_q(1, 0, 2)
    forward_kv(0)
    forward_kv(1)
    forward_wq(1, 0)
    forward_wq(1, 1)
    wait_kv(0)
    prefetch(0)
    gone(tok_in[2])
    send_tokens(tok_own, 3, 4, 5)
    wait_kv(1)
    prefetch(1)
    new_kv(2)
    wait_wq(1)
    project_q(0, 2, 4)
    project_q(1, 2, 4)
    forward_kv(2)
    wait_kv(2)
    prefetch(2)
    project_q(2)
    new_kv(4)
    new_kv(5)
    new_kv(3)
    project_q(3)
    forward_kv(3)
    for c in (4, 5, 3):
        wait_kv(c)
        if c >= 4:
            vl_buf[c - 4] = jnp.transpose(vr_buf[c - 4])
    wo_x = [send_wo(0)]

    last = N_STEP - 1
    state = score_step(0, 0, last, load_state(0))
    for i in range(SLOTS):
        if i == 0:
            tile(0, 0, state)
            ctx_copy(0).start()
            state = score_step(1, 1, last, load_state(1))
        elif i + 1 < SLOTS:
            state = tile(i, i, state, i + 1, i + 1, load_state(i + 1), (last,))
        else:
            state = tile(i, i, state, i + 1, 0, empty, every)
        if i % 2:
            for n in range(max(i - 1, 1), i + 1):
                ctx_copy(n).start()

    pairs = HEADS // 2
    state = lax.fori_loop(pairs, 2 * pairs, two_tiles, state)
    wo_f = []

    def forward_wo(p):
        wo_x[p].wait_recv()
        wo_f.append(forward(wo_buf, shard(row_of[XP], p, half)))

    gone(wo_x[0])
    wo_x.append(send_wo(1))
    forward_wo(0)
    state = lax.fori_loop(2 * pairs, 3 * pairs, two_tiles, state)
    forward_wo(1)
    state = lax.fori_loop(3 * pairs, 4 * pairs - 1, two_tiles, state)
    state = tile(TILES - 2, 0, state, TILES - 1, 1, empty, every)
    ctx_copy(TILES - 2).start()
    tile(TILES - 1, 1, state)
    ctx_copy(TILES - 1).start()

    wo_local.wait()
    wo_core.wait_recv()
    for cp in wo_f:
        cp.wait_recv()

    lax.fori_loop(0, N_BLOCK - 1, project_out, 0)
    project_last()

    for cp in sent:
        if id(cp) not in left:
            cp.wait_send()

    def wait_sent(i, carry):
        ctx_copy(i).wait_send()
        return carry

    lax.fori_loop(0, TILES, wait_sent, 0)
    assert next(number) <= N_SEM


def solution(mesh):
    def local_block(tokens, w_qkv, w_out, doc_ids):
        bf16, f32 = jnp.bfloat16, jnp.float32
        dma = pltpu.SemaphoreType.DMA
        any_spec = pl.BlockSpec(memory_space=pl.ANY)
        return pl.pallas_call(
            kernel,
            out_shape=pltpu.VMEM(tokens.shape, bf16),
            in_specs=[any_spec] * 4,
            out_specs=pl.BlockSpec(memory_space=pltpu.VMEM),
            scratch_shapes=[
                pltpu.VMEM((ROWS, HID), bf16),
                pltpu.VMEM((ROWS, HID), bf16),
                pltpu.VMEM((2 * HID, QKV), bf16),
                pltpu.VMEM((2 * HID, HID), bf16),
                pltpu.VMEM((4, 8, 128), jnp.int32),
                pltpu.VMEM((ROWS, HID), bf16),
                pltpu.VMEM((ROWS, 128), bf16),
                pltpu.VMEM((SEQ, HEAD_DIM), bf16),
                pltpu.VMEM((SEQ, HEAD_DIM), bf16),
                pltpu.VMEM((12, HEAD_DIM, 256), bf16),
                pltpu.VMEM((4, HEAD_DIM, 128), bf16),
                pltpu.VMEM((2, 256, HEAD_DIM), bf16),
                pltpu.VMEM((2, HEAD_DIM, 256), bf16),
                pltpu.VMEM((SLOTS, SEQ, QB), f32),
                pltpu.VMEM((SLOTS, SEQ // GROUP, 8, QB), f32),
                pltpu.VMEM((SLOTS, 2, 8, QB), f32),
                pltpu.VMEM((TILES, QB, HEAD_DIM), bf16),
                pltpu.VMEM((TILES, QB, HEAD_DIM), bf16),
                dma((4,)),
                dma((N_SEM,)),
                dma((N_SEM,)),
                dma((TILES,)),
                dma((TILES,)),
            ],
            compiler_params=pltpu.CompilerParams(
                collective_id=0, has_side_effects=True, vmem_limit_bytes=61 * 1024 * 1024
            ),
        )(tokens, w_qkv, w_out, doc_ids.reshape(8, 128))

    row_spec = P(("data", "row"), "col")
    weight_spec = P("row", "col")
    return jax.shard_map(
        local_block,
        mesh=mesh,
        in_specs=(row_spec, weight_spec, weight_spec, P(("data", "row"))),
        out_specs=row_spec,
        check_vma=False,
    )
```

```python
import itertools
import math

import jax
import jax.numpy as jnp
from jax import lax
from jax.experimental import pallas as pl
from jax.experimental.pallas import tpu as pltpu
from jax.sharding import PartitionSpec as P

HEAD_DIM = 128
MESH = pl.DeviceIdType.MESH

ROWS = 1024
HID = 1024
SEQ = 4096
HEADS = 8
QKV = 1280
SHARD = 512
QB = 256
KC = 1024
GROUP = 128
N_GROUP = KC // GROUP
N_STEP = SEQ // KC
CHUNKS = ((0, 256), (256, 256), (512, 256), (768, 128), (896, 128))
W_PIECES = 4
W_ROWS = SHARD // W_PIECES
N_BLOCK = ROWS // QB
TILES = HEADS * N_BLOCK
SLOTS = 8
N_SEM = 64
CORE, XP, DIAG = 0, 1, 2
EXP_SCALE = math.log2(math.e) / math.sqrt(HEAD_DIM)
NT = (((1,), (1,)), ((), ()))
BF16_MAX = float(jnp.finfo(jnp.bfloat16).max)
F32_MIN = float(jnp.finfo(jnp.float32).min)


def kernel(
    tok_hbm, w_hbm, wo_hbm, doc_hbm, out_ref,
    tok_own, tok_peer, w_buf, wo_buf, doc_buf, q_buf, qx_buf, k_buf, kx_buf, vw_buf, vn_buf, p_buf, top_buf, state_buf,
    ctx_own, ctx_peer, loc_sem, send_sem, recv_sem, ctx_send, ctx_recv,
):
    d, y, r = lax.axis_index("data"), lax.axis_index("col"), lax.axis_index("row")
    x, core = r // 2, r % 2
    row_of = {CORE: x * 2 + (1 - core), XP: (1 - x) * 2 + core, DIAG: (1 - x) * 2 + (1 - core)}
    y_peer = (d, 1 - y, r)
    peer = {k: (d, y, v) for k, v in row_of.items()}

    barrier = pltpu.get_barrier_semaphore()
    for p in (y_peer, peer[CORE], peer[XP], peer[DIAG]):
        pl.semaphore_signal(barrier, inc=1, device_id=p, device_id_type=MESH)
    pl.semaphore_wait(barrier, 4)

    number = itertools.count()
    sent = []

    def send(src, dst, device):
        i = next(number)
        cp = pltpu.make_async_remote_copy(
            src_ref=src, dst_ref=dst, send_sem=send_sem.at[i], recv_sem=recv_sem.at[i], device_id=device, device_id_type=MESH
        )
        cp.start()
        sent.append(cp)
        return cp

    def local(src, dst, i):
        cp = pltpu.make_async_copy(src, dst, loc_sem.at[i])
        cp.start()
        return cp

    def shard(row, piece=0, size=SHARD):
        return pl.ds(pl.multiple_of(row * SHARD + piece * size, size), size)

    kv_cols, q_cols = pl.ds(HID, 2 * HEAD_DIM), pl.ds(0, HID)

    tok_in = []
    for first, size in CHUNKS:
        rows = pl.ds(first, size)
        tok_in.append(send(tok_hbm.at[rows], tok_peer.at[rows], y_peer))
    wkv_x = send(w_hbm.at[:, kv_cols], w_buf.at[shard(r), kv_cols], peer[XP])
    doc_in = [send(doc_hbm, doc_buf.at[r], peer[k]) for k in (CORE, XP, DIAG)]
    wq_x = [
        send(w_hbm.at[pl.ds(p * W_ROWS, W_ROWS), q_cols], w_buf.at[shard(r, p, W_ROWS), q_cols], peer[XP])
        for p in range(W_PIECES)
    ]
    w_core = send(w_hbm, w_buf.at[shard(r)], peer[CORE])
    wo_core = send(wo_hbm, wo_buf.at[shard(r)], peer[CORE])
    doc_local = local(doc_hbm, doc_buf.at[r], 0)
    w_local = local(w_hbm, w_buf.at[shard(r)], 1)
    tok_local = local(tok_hbm, tok_own, 2)
    wo_local = local(wo_hbm, wo_buf.at[shard(r)], 3)

    doc_local.wait()
    for cp in doc_in:
        cp.wait_recv()
    lane = lax.broadcasted_iota(jnp.int32, (128, 128), 1)

    def as_column(line):
        return jnp.transpose(jnp.broadcast_to(line, (128, 128)))

    def key_mask(place):
        def line_mask(i, carry):
            part, line, first = place(i)
            ids = as_column(doc_buf[part, pl.ds(line, 1), :])
            hit = jnp.where(lane < 3, 1 - ids, jnp.where(lane < 6, ids, 0))
            kx_buf[pl.ds(pl.multiple_of(first, 128), 128), :] = hit.astype(jnp.float32).astype(jnp.bfloat16)
            return carry

        return line_mask

    def query_mask(i, carry):
        ids = as_column(doc_buf[r, pl.ds(i, 1), :])
        hit = jnp.where(lane < 3, ids, jnp.where(lane < 6, 1 - ids, 0))
        qx_buf[pl.ds(pl.multiple_of(i * 128, 128), 128), :] = jnp.where(hit == 1, -BF16_MAX, 0.0).astype(jnp.bfloat16)
        return carry

    wide = key_mask(lambda i: (i // 6, i % 6, (i % 6) // 2 * 1024 + i // 6 * 256 + i % 2 * 128))
    lax.fori_loop(0, 24, wide, 0)
    narrow = key_mask(lambda i: (i // 2, 6 + i % 2, 3072 + i % 2 * 512 + i // 2 * 128))
    lax.fori_loop(0, 8, narrow, 0)
    lax.fori_loop(0, ROWS // 128, query_mask, 0)

    own_half = pl.ds(pl.multiple_of(y * HID, HID), HID)
    peer_half = pl.ds(pl.multiple_of((1 - y) * HID, HID), HID)

    def project(rows, cols):
        return jnp.dot(tok_own[rows, :], w_buf[own_half, cols], preferred_element_type=jnp.float32) + jnp.dot(
            tok_peer[rows, :], w_buf[peer_half, cols], preferred_element_type=jnp.float32
        )

    def forward(ref, *index):
        return send(ref.at[index], ref.at[index], peer[CORE])

    k_in, kv_core = [], [[] for _ in CHUNKS]

    def keys_of(row, c):
        first, size = CHUNKS[c]
        values = vw_buf.at[c * 4 + row] if size == 256 else vn_buf.at[(c - N_STEP + 1) * 4 + row]
        return k_buf.at[pl.ds(pl.multiple_of(first * 4 + row * size, size), size)], values

    def project_kv(c):
        tok_in[c].wait_recv()
        kv = project(pl.ds(*CHUNKS[c]), kv_cols).astype(jnp.bfloat16)
        keys, values = keys_of(r, c)
        keys[...] = kv[:, :HEAD_DIM]
        values[...] = jnp.transpose(kv[:, HEAD_DIM:])

    def send_kv(c):
        refs = keys_of(r, c)
        k_in.append([send(ref, ref, peer[XP]) for ref in refs])
        kv_core[c].extend(send(ref, ref, peer[CORE]) for ref in refs)

    def forward_kv(c):
        for ref, cp in zip(keys_of(row_of[XP], c), k_in[c]):
            cp.wait_recv()
            kv_core[c].append(send(ref, ref, peer[CORE]))

    def wait_kv(c):
        for cp in kv_core[c]:
            cp.wait_recv()

    def project_q(c):
        rows = pl.ds(c * QB, QB)

        def q_tile(n, carry):
            cols = pl.ds(pl.multiple_of(n * 256, 256), 256)
            q_buf[rows, cols] = project(rows, cols).astype(jnp.bfloat16)
            return carry

        lax.fori_loop(0, HID // 256, q_tile, 0)

    wkv_x.wait_recv()
    wkv_f = forward(w_buf, shard(row_of[XP]), kv_cols)
    w_local.wait()
    tok_local.wait()
    w_core.wait_recv()
    wkv_f.wait_recv()
    wq_f = []

    def forward_wq(p):
        wq_x[p].wait_recv()
        wq_f.append(forward(w_buf, shard(row_of[XP], p, W_ROWS), q_cols))

    half = SHARD // 2

    def send_wo(p):
        return send(wo_hbm.at[pl.ds(p * half, half)], wo_buf.at[shard(r, p, half)], peer[XP])

    def tile_of(i):
        return (
            pl.ds(pl.multiple_of((i // HEADS) * QB, QB), QB),
            pl.ds(pl.multiple_of((i % HEADS) * HEAD_DIM, HEAD_DIM), HEAD_DIM),
        )

    def over_keys(f, a):
        return f(a.reshape(a.shape[0] // 8, 8, QB), axis=0)

    def to_keys(a):
        return jnp.concatenate([a] * (GROUP // 8), axis=0)

    def score_step(i, slot, j, state):
        top, total = state
        rows, cols = tile_of(i)
        q = jnp.concatenate([q_buf[rows, cols], qx_buf[rows, :]], axis=1)
        k = jnp.concatenate([k_buf[pl.ds(j * KC, KC), :], kx_buf[pl.ds(j * KC, KC), :]], axis=1)
        s = lax.dot_general(k, q, NT, preferred_element_type=jnp.float32)
        for g in range(N_GROUP):
            part = s[g * GROUP : (g + 1) * GROUP]
            new_top = jnp.maximum(top, over_keys(jnp.max, part))
            scaled = new_top * EXP_SCALE
            top_buf[slot, j * N_GROUP + g] = scaled
            p = jnp.exp2(part * EXP_SCALE - to_keys(scaled))
            p_buf[slot, pl.ds(j * KC + g * GROUP, GROUP), :] = p
            total = total * jnp.exp2(top * EXP_SCALE - scaled) + over_keys(jnp.sum, p)
            top = new_top
        return top, total

    def value_step(slot, j, lse, acc):
        keys = pl.ds(j * KC, KC)
        factor = [to_keys(jnp.exp2(top_buf[slot, j * N_GROUP + g] - lse)) for g in range(N_GROUP)]
        weights = p_buf[slot, keys, :] * jnp.concatenate(factor, axis=0)
        parts = [vw_buf[j * 4 + i] for i in range(4)] if j + 1 < N_STEP else [vn_buf[i] for i in range(8)]
        o = jnp.dot(jnp.concatenate(parts, axis=1), weights.astype(jnp.bfloat16), preferred_element_type=jnp.float32)
        return o if acc is None else acc + o

    def ctx_copy(i):
        return pltpu.make_async_remote_copy(
            src_ref=ctx_own.at[i], dst_ref=ctx_peer.at[i], send_sem=ctx_send.at[i], recv_sem=ctx_recv.at[i],
            device_id=y_peer, device_id_type=MESH,
        )

    empty = (jnp.full((8, QB), F32_MIN, jnp.float32), jnp.zeros((8, QB), jnp.float32))

    def load_state(slot):
        return state_buf[slot, 0], state_buf[slot, 1]

    def prefetch(*steps):
        def one(slot, carry):
            state = load_state(slot) if steps[0] else empty
            for j in steps:
                state = score_step(slot, slot, j, state)
            state_buf[slot, 0], state_buf[slot, 1] = state
            return carry

        lax.fori_loop(0, SLOTS, one, 0)

    def tile(i, slot, state, nxt=None, nxt_slot=None, nxt_state=None, nxt_steps=()):
        top, total = state
        best = jnp.max(top, axis=0, keepdims=True)
        whole = jnp.sum(total * jnp.exp2((top - best) * EXP_SCALE), axis=0, keepdims=True)
        lse = best * EXP_SCALE + jnp.log2(whole)
        acc = None
        steps = list(nxt_steps)
        for j in range(N_STEP):
            if steps:
                nxt_state = score_step(nxt, nxt_slot, steps.pop(0), nxt_state)
            acc = value_step(slot, j, lse, acc)
        ctx_own[i] = jnp.transpose(acc).astype(jnp.bfloat16)
        return nxt_state

    every = range(N_STEP)

    def two_tiles(t, state):
        i = t * 2
        state = tile(i, 0, state, i + 1, 1, empty, every)
        state = tile(i + 1, 1, state, i + 2, 0, empty, every)
        ctx_copy(i).start()
        ctx_copy(i + 1).start()
        return state

    def wait_pieces(first, end):
        def wait_piece(i, carry):
            ctx_copy(i).wait_recv()
            return carry

        lax.fori_loop(first, end, wait_piece, 0)

    def heads(ref, b, first, end):
        return jnp.concatenate([ref[b * HEADS + h] for h in range(first, end)], axis=1)

    def out_rows(half_index, first, end):
        size = (end - first) * HEAD_DIM
        return pl.ds(pl.multiple_of(half_index * HID + first * HEAD_DIM, HEAD_DIM), size)

    def store_out(b, n, o):
        out_ref[pl.ds(pl.multiple_of(b * QB, QB), QB), pl.ds(pl.multiple_of(n * 256, 256), 256)] = o.astype(jnp.bfloat16)

    def out_product(b, n, end):
        cols = pl.ds(pl.multiple_of(n * 256, 256), 256)
        own = jnp.dot(heads(ctx_own, b, 0, HEADS), wo_buf[own_half, cols], preferred_element_type=jnp.float32)
        rows = out_rows(1 - y, 0, end)
        return own + jnp.dot(heads(ctx_peer, b, 0, end), wo_buf[rows, cols], preferred_element_type=jnp.float32)

    def project_out(b, carry):
        wait_pieces(b * HEADS, (b + 1) * HEADS)

        def out_tile(n, carry):
            store_out(b, n, out_product(b, n, HEADS))
            return carry

        return lax.fori_loop(0, 4, out_tile, carry)

    def project_last():
        b, most = N_BLOCK - 1, HEADS - 2
        wait_pieces(b * HEADS, b * HEADS + most)

        def first_part(n, carry):
            p_buf[2, pl.ds(pl.multiple_of(n * QB, QB), QB), :] = out_product(b, n, most)
            return carry

        lax.fori_loop(0, 4, first_part, 0)
        wait_pieces(b * HEADS + most, TILES)
        for n in range(4):
            cols, rows = pl.ds(n * 256, 256), out_rows(1 - y, most, HEADS)
            o = jnp.dot(heads(ctx_peer, b, most, HEADS), wo_buf[rows, cols], preferred_element_type=jnp.float32)
            store_out(b, n, p_buf[2, pl.ds(n * QB, QB), :] + o)

    project_kv(0)
    forward_wq(0)
    forward_wq(1)
    project_kv(1)
    forward_wq(2)
    forward_wq(3)
    send_kv(0)
    send_kv(1)
    for cp in wq_f:
        cp.wait_recv()
    project_q(0)
    project_kv(2)
    send_kv(2)
    forward_kv(0)
    forward_kv(1)
    for c in (0, 1):
        wait_kv(c)
    prefetch(0, 1)
    project_kv(3)
    send_kv(3)
    forward_kv(2)
    project_kv(4)
    send_kv(4)
    wo_x = [send_wo(0), send_wo(1)]
    wait_kv(2)
    prefetch(2)
    forward_kv(3)
    forward_kv(4)
    for c in (3, 4):
        wait_kv(c)

    last = N_STEP - 1
    state = score_step(0, 0, last, load_state(0))
    for i in range(SLOTS):
        if i == 4:
            project_q(1)
        if i == 0:
            tile(0, 0, state)
            ctx_copy(0).start()
            state = score_step(1, 1, last, load_state(1))
        elif i + 1 < SLOTS:
            state = tile(i, i, state, i + 1, i + 1, load_state(i + 1), (last,))
        else:
            state = tile(i, i, state, i + 1, 0, empty, every)
        if i % 2:
            for n in range(max(i - 1, 1), i + 1):
                ctx_copy(n).start()

    project_q(2)
    pairs = HEADS // 2
    state = lax.fori_loop(pairs, 2 * pairs, two_tiles, state)
    wo_f = []

    def forward_wo(p):
        wo_x[p].wait_recv()
        wo_f.append(forward(wo_buf, shard(row_of[XP], p, half)))

    forward_wo(0)
    project_q(3)
    state = lax.fori_loop(2 * pairs, 3 * pairs, two_tiles, state)
    forward_wo(1)
    state = lax.fori_loop(3 * pairs, 4 * pairs - 1, two_tiles, state)
    state = tile(TILES - 2, 0, state, TILES - 1, 1, empty, every)
    ctx_copy(TILES - 2).start()
    tile(TILES - 1, 1, state)
    ctx_copy(TILES - 1).start()

    wo_local.wait()
    wo_core.wait_recv()
    for cp in wo_f:
        cp.wait_recv()

    lax.fori_loop(0, N_BLOCK - 1, project_out, 0)
    project_last()

    for cp in sent:
        cp.wait_send()

    def wait_sent(i, carry):
        ctx_copy(i).wait_send()
        return carry

    lax.fori_loop(0, TILES, wait_sent, 0)
    assert next(number) <= N_SEM


def solution(mesh):
    def local_block(tokens, w_qkv, w_out, doc_ids):
        bf16, f32 = jnp.bfloat16, jnp.float32
        dma = pltpu.SemaphoreType.DMA
        any_spec = pl.BlockSpec(memory_space=pl.ANY)
        return pl.pallas_call(
            kernel,
            out_shape=pltpu.VMEM(tokens.shape, bf16),
            in_specs=[any_spec] * 4,
            out_specs=pl.BlockSpec(memory_space=pltpu.VMEM),
            scratch_shapes=[
                pltpu.VMEM((ROWS, HID), bf16),
                pltpu.VMEM((ROWS, HID), bf16),
                pltpu.VMEM((2 * HID, QKV), bf16),
                pltpu.VMEM((2 * HID, HID), bf16),
                pltpu.VMEM((4, 8, 128), jnp.int32),
                pltpu.VMEM((ROWS, HID), bf16),
                pltpu.VMEM((ROWS, 128), bf16),
                pltpu.VMEM((SEQ, HEAD_DIM), bf16),
                pltpu.VMEM((SEQ, HEAD_DIM), bf16),
                pltpu.VMEM((12, HEAD_DIM, 256), bf16),
                pltpu.VMEM((8, HEAD_DIM, 128), bf16),
                pltpu.VMEM((SLOTS, SEQ, QB), f32),
                pltpu.VMEM((SLOTS, SEQ // GROUP, 8, QB), f32),
                pltpu.VMEM((SLOTS, 2, 8, QB), f32),
                pltpu.VMEM((TILES, QB, HEAD_DIM), bf16),
                pltpu.VMEM((TILES, QB, HEAD_DIM), bf16),
                dma((4,)),
                dma((N_SEM,)),
                dma((N_SEM,)),
                dma((TILES,)),
                dma((TILES,)),
            ],
            compiler_params=pltpu.CompilerParams(
                collective_id=0, has_side_effects=True, vmem_limit_bytes=59 * 1024 * 1024
            ),
        )(tokens, w_qkv, w_out, doc_ids.reshape(8, 128))

    row_spec = P(("data", "row"), "col")
    weight_spec = P("row", "col")
    return jax.shard_map(
        local_block,
        mesh=mesh,
        in_specs=(row_spec, weight_spec, weight_spec, P(("data", "row"))),
        out_specs=row_spec,
        check_vma=False,
    )
```

```python
import itertools
import math

import jax
import jax.numpy as jnp
from jax import lax
from jax.experimental import pallas as pl
from jax.experimental.pallas import tpu as pltpu
from jax.sharding import PartitionSpec as P

HEAD_DIM = 128
MESH = pl.DeviceIdType.MESH

ROWS = 1024
HID = 1024
SEQ = 4096
HEADS = 8
QKV = 1280
SHARD = 512
QB = 256
KC = 1024
GROUP = 128
N_GROUP = KC // GROUP
N_STEP = SEQ // KC
CHUNKS = ((0, 256), (256, 256), (512, 256), (768, 128), (896, 128))
W_PIECES = 4
W_ROWS = SHARD // W_PIECES
N_BLOCK = ROWS // QB
TILES = HEADS * N_BLOCK
SLOTS = 8
N_SEM = 64
CORE, XP, DIAG = 0, 1, 2
EXP_SCALE = math.log2(math.e) / math.sqrt(HEAD_DIM)
NT = (((1,), (1,)), ((), ()))
BF16_MAX = float(jnp.finfo(jnp.bfloat16).max)
F32_MIN = float(jnp.finfo(jnp.float32).min)


def kernel(
    tok_hbm, w_hbm, wo_hbm, doc_hbm, out_ref,
    tok_own, tok_peer, w_buf, wo_buf, doc_buf, q_buf, qx_buf, k_buf, kx_buf, vw_buf, vn_buf, p_buf, top_buf, state_buf,
    ctx_own, ctx_peer, loc_sem, send_sem, recv_sem, ctx_send, ctx_recv,
):
    d, y, r = lax.axis_index("data"), lax.axis_index("col"), lax.axis_index("row")
    x, core = r // 2, r % 2
    row_of = {CORE: x * 2 + (1 - core), XP: (1 - x) * 2 + core, DIAG: (1 - x) * 2 + (1 - core)}
    y_peer = (d, 1 - y, r)
    peer = {k: (d, y, v) for k, v in row_of.items()}

    barrier = pltpu.get_barrier_semaphore()
    for p in (y_peer, peer[CORE], peer[XP], peer[DIAG]):
        pl.semaphore_signal(barrier, inc=1, device_id=p, device_id_type=MESH)
    pl.semaphore_wait(barrier, 4)

    number = itertools.count()
    sent = []

    def send(src, dst, device):
        i = next(number)
        cp = pltpu.make_async_remote_copy(
            src_ref=src, dst_ref=dst, send_sem=send_sem.at[i], recv_sem=recv_sem.at[i], device_id=device, device_id_type=MESH
        )
        cp.start()
        sent.append(cp)
        return cp

    def local(src, dst, i):
        cp = pltpu.make_async_copy(src, dst, loc_sem.at[i])
        cp.start()
        return cp

    def shard(row, piece=0, size=SHARD):
        return pl.ds(pl.multiple_of(row * SHARD + piece * size, size), size)

    kv_cols, q_cols = pl.ds(HID, 2 * HEAD_DIM), pl.ds(0, HID)

    tok_in = []
    for first, size in CHUNKS:
        rows = pl.ds(first, size)
        tok_in.append(send(tok_hbm.at[rows], tok_peer.at[rows], y_peer))
    wkv_x = send(w_hbm.at[:, kv_cols], w_buf.at[shard(r), kv_cols], peer[XP])
    doc_in = [send(doc_hbm, doc_buf.at[r], peer[k]) for k in (CORE, XP, DIAG)]
    wq_x = [
        send(w_hbm.at[pl.ds(p * W_ROWS, W_ROWS), q_cols], w_buf.at[shard(r, p, W_ROWS), q_cols], peer[XP])
        for p in range(W_PIECES)
    ]
    w_core = send(w_hbm, w_buf.at[shard(r)], peer[CORE])
    wo_core = send(wo_hbm, wo_buf.at[shard(r)], peer[CORE])
    doc_local = local(doc_hbm, doc_buf.at[r], 0)
    w_local = local(w_hbm, w_buf.at[shard(r)], 1)
    tok_local = local(tok_hbm, tok_own, 2)
    wo_local = local(wo_hbm, wo_buf.at[shard(r)], 3)

    doc_local.wait()
    for cp in doc_in:
        cp.wait_recv()
    lane = lax.broadcasted_iota(jnp.int32, (128, 128), 1)

    def as_column(line):
        return jnp.transpose(jnp.broadcast_to(line, (128, 128)))

    def key_mask(place):
        def line_mask(i, carry):
            part, line, first = place(i)
            ids = as_column(doc_buf[part, pl.ds(line, 1), :])
            hit = jnp.where(lane < 3, 1 - ids, jnp.where(lane < 6, ids, 0))
            kx_buf[pl.ds(pl.multiple_of(first, 128), 128), :] = hit.astype(jnp.float32).astype(jnp.bfloat16)
            return carry

        return line_mask

    def query_mask(i, carry):
        ids = as_column(doc_buf[r, pl.ds(i, 1), :])
        hit = jnp.where(lane < 3, ids, jnp.where(lane < 6, 1 - ids, 0))
        qx_buf[pl.ds(pl.multiple_of(i * 128, 128), 128), :] = jnp.where(hit == 1, -BF16_MAX, 0.0).astype(jnp.bfloat16)
        return carry

    wide = key_mask(lambda i: (i // 6, i % 6, (i % 6) // 2 * 1024 + i // 6 * 256 + i % 2 * 128))
    lax.fori_loop(0, 24, wide, 0)
    narrow = key_mask(lambda i: (i // 2, 6 + i % 2, 3072 + i % 2 * 512 + i // 2 * 128))
    lax.fori_loop(0, 8, narrow, 0)
    lax.fori_loop(0, ROWS // 128, query_mask, 0)

    own_half = pl.ds(pl.multiple_of(y * HID, HID), HID)
    peer_half = pl.ds(pl.multiple_of((1 - y) * HID, HID), HID)

    def project(rows, cols):
        return jnp.dot(tok_own[rows, :], w_buf[own_half, cols], preferred_element_type=jnp.float32) + jnp.dot(
            tok_peer[rows, :], w_buf[peer_half, cols], preferred_element_type=jnp.float32
        )

    def forward(ref, *index):
        return send(ref.at[index], ref.at[index], peer[CORE])

    k_in, kv_core = [], [[] for _ in CHUNKS]

    def keys_of(row, c):
        first, size = CHUNKS[c]
        values = vw_buf.at[c * 4 + row] if size == 256 else vn_buf.at[(c - N_STEP + 1) * 4 + row]
        return k_buf.at[pl.ds(pl.multiple_of(first * 4 + row * size, size), size)], values

    def project_kv(c):
        tok_in[c].wait_recv()
        kv = project(pl.ds(*CHUNKS[c]), kv_cols).astype(jnp.bfloat16)
        keys, values = keys_of(r, c)
        keys[...] = kv[:, :HEAD_DIM]
        values[...] = jnp.transpose(kv[:, HEAD_DIM:])

    def send_kv(c):
        refs = keys_of(r, c)
        k_in.append([send(ref, ref, peer[XP]) for ref in refs])
        kv_core[c].extend(send(ref, ref, peer[CORE]) for ref in refs)

    def forward_kv(c):
        for ref, cp in zip(keys_of(row_of[XP], c), k_in[c]):
            cp.wait_recv()
            kv_core[c].append(send(ref, ref, peer[CORE]))

    def wait_kv(c):
        for cp in kv_core[c]:
            cp.wait_recv()

    def project_q(c):
        rows = pl.ds(c * QB, QB)

        def q_tile(n, carry):
            cols = pl.ds(pl.multiple_of(n * 256, 256), 256)
            q_buf[rows, cols] = project(rows, cols).astype(jnp.bfloat16)
            return carry

        lax.fori_loop(0, HID // 256, q_tile, 0)

    wkv_x.wait_recv()
    wkv_f = forward(w_buf, shard(row_of[XP]), kv_cols)
    w_local.wait()
    tok_local.wait()
    w_core.wait_recv()
    wkv_f.wait_recv()
    wq_f = []

    def forward_wq(p):
        wq_x[p].wait_recv()
        wq_f.append(forward(w_buf, shard(row_of[XP], p, W_ROWS), q_cols))

    half = SHARD // 2

    def send_wo(p):
        return send(wo_hbm.at[pl.ds(p * half, half)], wo_buf.at[shard(r, p, half)], peer[XP])

    def tile_of(i):
        return (
            pl.ds(pl.multiple_of((i // HEADS) * QB, QB), QB),
            pl.ds(pl.multiple_of((i % HEADS) * HEAD_DIM, HEAD_DIM), HEAD_DIM),
        )

    def over_keys(f, a):
        return f(a.reshape(a.shape[0] // 8, 8, QB), axis=0)

    def to_keys(a):
        return jnp.concatenate([a] * (GROUP // 8), axis=0)

    def score_step(i, slot, j, state):
        top, total = state
        rows, cols = tile_of(i)
        q = jnp.concatenate([q_buf[rows, cols], qx_buf[rows, :]], axis=1)
        k = jnp.concatenate([k_buf[pl.ds(j * KC, KC), :], kx_buf[pl.ds(j * KC, KC), :]], axis=1)
        s = lax.dot_general(k, q, NT, preferred_element_type=jnp.float32)
        for g in range(N_GROUP):
            part = s[g * GROUP : (g + 1) * GROUP]
            new_top = jnp.maximum(top, over_keys(jnp.max, part))
            scaled = new_top * EXP_SCALE
            top_buf[slot, j * N_GROUP + g] = scaled
            p = jnp.exp2(part * EXP_SCALE - to_keys(scaled))
            p_buf[slot, pl.ds(j * KC + g * GROUP, GROUP), :] = p
            total = total * jnp.exp2(top * EXP_SCALE - scaled) + over_keys(jnp.sum, p)
            top = new_top
        return top, total

    def value_step(slot, j, lse, acc):
        keys = pl.ds(j * KC, KC)
        factor = [to_keys(jnp.exp2(top_buf[slot, j * N_GROUP + g] - lse)) for g in range(N_GROUP)]
        weights = p_buf[slot, keys, :] * jnp.concatenate(factor, axis=0)
        parts = [vw_buf[j * 4 + i] for i in range(4)] if j + 1 < N_STEP else [vn_buf[i] for i in range(8)]
        o = jnp.dot(jnp.concatenate(parts, axis=1), weights.astype(jnp.bfloat16), preferred_element_type=jnp.float32)
        return o if acc is None else acc + o

    def ctx_copy(i):
        return pltpu.make_async_remote_copy(
            src_ref=ctx_own.at[i], dst_ref=ctx_peer.at[i], send_sem=ctx_send.at[i], recv_sem=ctx_recv.at[i],
            device_id=y_peer, device_id_type=MESH,
        )

    empty = (jnp.full((8, QB), F32_MIN, jnp.float32), jnp.zeros((8, QB), jnp.float32))

    def load_state(slot):
        return state_buf[slot, 0], state_buf[slot, 1]

    def prefetch(*steps):
        def one(slot, carry):
            state = load_state(slot) if steps[0] else empty
            for j in steps:
                state = score_step(slot, slot, j, state)
            state_buf[slot, 0], state_buf[slot, 1] = state
            return carry

        lax.fori_loop(0, SLOTS, one, 0)

    def tile(i, slot, state, nxt=None, nxt_slot=None, nxt_state=None, nxt_steps=()):
        top, total = state
        best = jnp.max(top, axis=0, keepdims=True)
        whole = jnp.sum(total * jnp.exp2((top - best) * EXP_SCALE), axis=0, keepdims=True)
        lse = best * EXP_SCALE + jnp.log2(whole)
        acc = None
        steps = list(nxt_steps)
        for j in range(N_STEP):
            if steps:
                nxt_state = score_step(nxt, nxt_slot, steps.pop(0), nxt_state)
            acc = value_step(slot, j, lse, acc)
        ctx_own[i] = jnp.transpose(acc).astype(jnp.bfloat16)
        return nxt_state

    every = range(N_STEP)

    def two_tiles(t, state):
        i = t * 2
        state = tile(i, 0, state, i + 1, 1, empty, every)
        state = tile(i + 1, 1, state, i + 2, 0, empty, every)
        ctx_copy(i).start()
        ctx_copy(i + 1).start()
        return state

    def wait_pieces(first, end):
        def wait_piece(i, carry):
            ctx_copy(i).wait_recv()
            return carry

        lax.fori_loop(first, end, wait_piece, 0)

    def heads(ref, b, first, end):
        return jnp.concatenate([ref[b * HEADS + h] for h in range(first, end)], axis=1)

    def out_rows(half_index, first, end):
        size = (end - first) * HEAD_DIM
        return pl.ds(pl.multiple_of(half_index * HID + first * HEAD_DIM, HEAD_DIM), size)

    def store_out(b, n, o):
        out_ref[pl.ds(pl.multiple_of(b * QB, QB), QB), pl.ds(pl.multiple_of(n * 256, 256), 256)] = o.astype(jnp.bfloat16)

    def out_product(b, n, end):
        cols = pl.ds(pl.multiple_of(n * 256, 256), 256)
        own = jnp.dot(heads(ctx_own, b, 0, HEADS), wo_buf[own_half, cols], preferred_element_type=jnp.float32)
        rows = out_rows(1 - y, 0, end)
        return own + jnp.dot(heads(ctx_peer, b, 0, end), wo_buf[rows, cols], preferred_element_type=jnp.float32)

    def project_out(b, carry):
        wait_pieces(b * HEADS, (b + 1) * HEADS)

        def out_tile(n, carry):
            store_out(b, n, out_product(b, n, HEADS))
            return carry

        return lax.fori_loop(0, 4, out_tile, carry)

    def project_last():
        b, most = N_BLOCK - 1, HEADS - 2
        wait_pieces(b * HEADS, b * HEADS + most)

        def first_part(n, carry):
            p_buf[2, pl.ds(pl.multiple_of(n * QB, QB), QB), :] = out_product(b, n, most)
            return carry

        lax.fori_loop(0, 4, first_part, 0)
        wait_pieces(b * HEADS + most, TILES)
        for n in range(4):
            cols, rows = pl.ds(n * 256, 256), out_rows(1 - y, most, HEADS)
            o = jnp.dot(heads(ctx_peer, b, most, HEADS), wo_buf[rows, cols], preferred_element_type=jnp.float32)
            store_out(b, n, p_buf[2, pl.ds(n * QB, QB), :] + o)

    project_kv(0)
    forward_wq(0)
    forward_wq(1)
    project_kv(1)
    forward_wq(2)
    forward_wq(3)
    send_kv(0)
    send_kv(1)
    for cp in wq_f:
        cp.wait_recv()
    project_q(0)
    project_q(1)
    project_kv(2)
    send_kv(2)
    forward_kv(0)
    forward_kv(1)
    project_q(2)
    for c in (0, 1):
        wait_kv(c)
    prefetch(0, 1)
    project_kv(3)
    send_kv(3)
    forward_kv(2)
    project_kv(4)
    send_kv(4)
    wo_x = [send_wo(0), send_wo(1)]
    wait_kv(2)
    prefetch(2)
    forward_kv(3)
    forward_kv(4)
    project_q(3)
    for c in (3, 4):
        wait_kv(c)

    last = N_STEP - 1
    state = score_step(0, 0, last, load_state(0))
    for i in range(SLOTS):
        if i == 0:
            tile(0, 0, state)
            ctx_copy(0).start()
            state = score_step(1, 1, last, load_state(1))
        elif i + 1 < SLOTS:
            state = tile(i, i, state, i + 1, i + 1, load_state(i + 1), (last,))
        else:
            state = tile(i, i, state, i + 1, 0, empty, every)
        if i % 2:
            for n in range(max(i - 1, 1), i + 1):
                ctx_copy(n).start()

    pairs = HEADS // 2
    state = lax.fori_loop(pairs, 2 * pairs, two_tiles, state)
    wo_f = []

    def forward_wo(p):
        wo_x[p].wait_recv()
        wo_f.append(forward(wo_buf, shard(row_of[XP], p, half)))

    forward_wo(0)
    state = lax.fori_loop(2 * pairs, 3 * pairs, two_tiles, state)
    forward_wo(1)
    state = lax.fori_loop(3 * pairs, 4 * pairs - 1, two_tiles, state)
    state = tile(TILES - 2, 0, state, TILES - 1, 1, empty, every)
    ctx_copy(TILES - 2).start()
    tile(TILES - 1, 1, state)
    ctx_copy(TILES - 1).start()

    wo_local.wait()
    wo_core.wait_recv()
    for cp in wo_f:
        cp.wait_recv()

    lax.fori_loop(0, N_BLOCK - 1, project_out, 0)
    project_last()

    for cp in sent:
        cp.wait_send()

    def wait_sent(i, carry):
        ctx_copy(i).wait_send()
        return carry

    lax.fori_loop(0, TILES, wait_sent, 0)
    assert next(number) <= N_SEM


def solution(mesh):
    def local_block(tokens, w_qkv, w_out, doc_ids):
        bf16, f32 = jnp.bfloat16, jnp.float32
        dma = pltpu.SemaphoreType.DMA
        any_spec = pl.BlockSpec(memory_space=pl.ANY)
        return pl.pallas_call(
            kernel,
            out_shape=pltpu.VMEM(tokens.shape, bf16),
            in_specs=[any_spec] * 4,
            out_specs=pl.BlockSpec(memory_space=pltpu.VMEM),
            scratch_shapes=[
                pltpu.VMEM((ROWS, HID), bf16),
                pltpu.VMEM((ROWS, HID), bf16),
                pltpu.VMEM((2 * HID, QKV), bf16),
                pltpu.VMEM((2 * HID, HID), bf16),
                pltpu.VMEM((4, 8, 128), jnp.int32),
                pltpu.VMEM((ROWS, HID), bf16),
                pltpu.VMEM((ROWS, 128), bf16),
                pltpu.VMEM((SEQ, HEAD_DIM), bf16),
                pltpu.VMEM((SEQ, HEAD_DIM), bf16),
                pltpu.VMEM((12, HEAD_DIM, 256), bf16),
                pltpu.VMEM((8, HEAD_DIM, 128), bf16),
                pltpu.VMEM((SLOTS, SEQ, QB), f32),
                pltpu.VMEM((SLOTS, SEQ // GROUP, 8, QB), f32),
                pltpu.VMEM((SLOTS, 2, 8, QB), f32),
                pltpu.VMEM((TILES, QB, HEAD_DIM), bf16),
                pltpu.VMEM((TILES, QB, HEAD_DIM), bf16),
                dma((4,)),
                dma((N_SEM,)),
                dma((N_SEM,)),
                dma((TILES,)),
                dma((TILES,)),
            ],
            compiler_params=pltpu.CompilerParams(
                collective_id=0, has_side_effects=True, vmem_limit_bytes=59 * 1024 * 1024
            ),
        )(tokens, w_qkv, w_out, doc_ids.reshape(8, 128))

    row_spec = P(("data", "row"), "col")
    weight_spec = P("row", "col")
    return jax.shard_map(
        local_block,
        mesh=mesh,
        in_specs=(row_spec, weight_spec, weight_spec, P(("data", "row"))),
        out_specs=row_spec,
        check_vma=False,
    )
```
